32 devices in a mesh: gx: 4 (over x, core), gy: 8 (over z, y).
Axes of the slice: x: 2, y: 2, z: 4, core: 2. Of those that a mesh axis runs over, the one named last changes fastest.
Arguments:
- substrate: float32 [16, 64, 1024], P(None, 'gy', 'gx'), may hold values from 0 to 1
- catalyst: float32 [16, 64, 1024], P(None, 'gy', 'gx'), may hold values from 0 to 1
Outputs:
- substrate_next: float32 [16, 64, 1024], P(None, 'gy', 'gx')
- catalyst_next: float32 [16, 64, 1024], P(None, 'gy', 'gx')
- rebuilt: float32 [2, 16, 1024, 64], P(None, None, ('gx', 'gy'))
The draws below stay inside these ranges and needn't reach their ends.
All inputs are finite; a program needn't handle non-finite values.
Results may differ from the reference program's by a relative error of at most 0.00002.
Values sent between devices are 32-bit elements; how exact they have to be, the bound alone decides.
A program may use at most 64 MiB of HBM per device.

```python
import jax
import jax.numpy as jnp

Z = 16
NX = 1024
NY = 64


def block_scale(rng, extent, split, low, largest):
    def one(axis_at, shards_of):
        heights = jax.random.uniform(jax.random.fold_in(jax.random.fold_in(rng, 6), axis_at), (shards_of,), jnp.float32, low / len(split), largest / len(split))
        return jnp.repeat(jnp.exp(heights), extent[axis_at] // shards_of).reshape((-1,) + (1,) * (len(extent) - axis_at - 1))

    gain = one(*split[0])
    for cut in split[1:]:
        gain = gain * one(*cut)
    return gain


def setup_inputs(seed: int = 0) -> dict:
    seeds = jax.random.split(jax.random.key(seed), 3)
    return {
        "substrate": jnp.clip(1.0 * jax.random.uniform(seeds[0], (Z, NY, NX), jnp.float32) ** block_scale(seeds[0], (Z, NY, NX), ((1, 8), (2, 4)), -0.2, 0.2), 0.0, 1.0),
        "catalyst": jnp.clip(1.0 * jax.random.uniform(seeds[1], (Z, NY, NX), jnp.float32) ** block_scale(seeds[1], (Z, NY, NX), ((1, 8), (2, 4)), -0.2, 0.2), 0.0, 1.0),
    }


feed_rate = 0.037
kill_rate = 0.06
substrate_diffusion = 0.15
catalyst_diffusion = 0.08


def react(center, spread):
    substrate = center[0]
    catalyst = center[1]
    reaction = substrate * catalyst * catalyst
    new_substrate = substrate + substrate_diffusion * spread[0] - reaction + feed_rate * (1.0 - substrate)
    new_catalyst = catalyst + catalyst_diffusion * spread[1] + reaction - (feed_rate + kill_rate) * catalyst
    return jnp.stack([new_substrate, new_catalyst])


def neighbours(field):
    total = jnp.roll(field, 1, 1) + jnp.roll(field, -1, 1)
    total = total + jnp.roll(field, 1, 2) + jnp.roll(field, -1, 2)
    total = total + jnp.roll(field, 1, 3) + jnp.roll(field, -1, 3)
    return total - 6.0 * field


def restrict(field):
    shape = field.shape
    blocks = field.reshape(shape[0], shape[1], shape[2] // 2, 2, shape[3] // 2, 2)
    return (blocks[:, :, :, 0, :, 0] + blocks[:, :, :, 0, :, 1] + blocks[:, :, :, 1, :, 0] + blocks[:, :, :, 1, :, 1]) * 0.25


def prolong(field):
    return jnp.repeat(jnp.repeat(field, 2, axis=2), 2, axis=3)


def reference(substrate, catalyst):
    state = jnp.stack([substrate, catalyst])
    state = react(state, neighbours(state))
    state = react(state, neighbours(state))
    level1 = restrict(state)
    level2 = restrict(level1)
    coarse = prolong(level2)
    blend = coarse + 0.5 * (level1 - coarse)
    rebuilt = jnp.swapaxes(prolong(blend), 2, 3)
    return state[0], state[1], rebuilt
```

```python
import functools

import jax
import jax.numpy as jnp
from jax import lax
from jax.experimental import pallas as pl
from jax.experimental.pallas import tpu as pltpu
from jax.sharding import PartitionSpec as P

feed_rate = 0.037
kill_rate = 0.06
substrate_diffusion = 0.15
catalyst_diffusion = 0.08

MESH = pl.DeviceIdType.MESH
LANES = 128


def react(substrate, catalyst, spread_substrate, spread_catalyst):
    reaction = substrate * catalyst * catalyst
    new_substrate = (
        substrate
        + substrate_diffusion * spread_substrate
        - reaction
        + feed_rate * (1.0 - substrate)
    )
    new_catalyst = (
        catalyst
        + catalyst_diffusion * spread_catalyst
        + reaction
        - (feed_rate + kill_rate) * catalyst
    )
    return new_substrate, new_catalyst


def split(value):
    high = value.astype(jnp.bfloat16)
    low = (value - high.astype(jnp.float32)).astype(jnp.bfloat16)
    return high, low


def spread_of(before, here, after):
    planes, extent = here.shape
    total = pltpu.roll(here, 1, 0) + pltpu.roll(here, planes - 1, 0)
    total = total + before + after
    total = total + pltpu.roll(here, 1, 1) + pltpu.roll(here, extent - 1, 1)
    return total - 6.0 * here


def partner_of(me, step, size):
    if size & (size - 1):
        return lax.rem(me + step, size)
    partner = me + step
    for bit in range(size.bit_length() - 1):
        if step >> bit & 1:
            partner = partner - 2 * (1 << bit) * lax.rem(me // (1 << bit), 2)
    return partner


def kernel(dims, *refs):
    planes, columns, extent, owners, slabs_x, slabs_y = dims
    (u_ref, v_ref, u_out, v_out, gathered, loaded, state, edge, packed, got, corner, middle, sums,
     outgoing, load_sem, send_sem, recv_sem, deal_send, deal_recv) = refs
    tiles = extent // LANES
    gx, gy = lax.axis_index("gx"), lax.axis_index("gy")

    barrier = pltpu.get_barrier_semaphore()
    sides = [(lax.rem(gx + shift, slabs_x), gy) for shift in (1, slabs_x - 1)]
    ends = [(gx, lax.rem(gy + shift, owners)) for shift in (1, owners - 1)]
    peers = [(gx, lax.rem(gy + step, owners)) for step in range(1, owners)]
    diagonals = [(side[0], end[1]) for end in ends for side in sides]
    for device in sides + diagonals + peers:
        pl.semaphore_signal(barrier, inc=1, device_id=device, device_id_type=MESH)

    loads = [
        pltpu.make_async_copy(source, loaded.at[field], load_sem.at[field])
        for field, source in enumerate((u_ref, v_ref))
    ]
    for load in loads:
        load.start()
    for load in loads:
        load.wait()

    lane = lax.broadcasted_iota(jnp.int32, (planes, LANES), 1)
    group = lax.rem(lane + 2, LANES) // 4
    pack = jnp.zeros((planes, LANES), jnp.float32)
    for field in range(2):
        for column in range(columns):
            slab = jnp.concatenate(
                [
                    loaded[field, pl.ds(tile * columns + column, planes, stride=tiles * columns), :]
                    for tile in range(tiles)
                ],
                axis=1,
            )
            state[field, 2 + column] = slab
            at = field * columns + column
            tips = jnp.where(lane < LANES // 2, slab[:, :LANES], slab[:, extent - LANES :])
            tips = pltpu.roll(tips, 4 * at, 1) if at else tips
            pack = jnp.where(group == at, tips, pack)
    packed[...] = pack

    pl.semaphore_wait(barrier, len(sides) + len(diagonals) + len(peers))

    def send(number, source, target, device):
        return pltpu.make_async_remote_copy(
            src_ref=source,
            dst_ref=target,
            send_sem=send_sem.at[number],
            recv_sem=recv_sem.at[number],
            device_id=device,
            device_id_type=MESH,
        )

    low_end, high_end = slice(0, 2), slice(columns + 2, columns + 4)
    across = [send(2 + side, packed, got.at[side], sides[side]) for side in range(2)]
    along = [
        send(0, state.at[:, columns : columns + 2], state.at[:, low_end], ends[0]),
        send(1, state.at[:, 2:4], state.at[:, high_end], ends[1]),
    ]
    corners = [send(4 + at, packed, corner.at[at], diagonals[at]) for at in range(4)]
    for copy in across + corners + along:
        copy.start()

    half = extent // 2
    row = lax.broadcasted_iota(jnp.int32, (half, extent), 0)
    fine = lax.broadcasted_iota(jnp.int32, (half, extent), 1)
    to_blend = jnp.concatenate(
        [
            jnp.where(fine // 2 == row, 0.125, 0.0),
            jnp.where(fine // 4 == row // 2, 0.03125, 0.0),
        ],
        axis=1,
    ).astype(jnp.bfloat16)

    for copy in across:
        copy.wait_recv()

    def merged(ref, at):
        return jnp.where(lax.rem(lane, 4) < 2, ref[at + 1], ref[at])

    both = merged(got, 0)

    def place(field, c, tile, column):
        at = field * columns + column
        edge[field, c] = pltpu.roll(tile, LANES - 4 * at, 1) if at else tile

    for field in range(2):
        for c in range(2, columns + 2):
            place(field, c, both, c - 2)
    def wide(field, c):
        if c in (0, columns + 3):
            tail = jnp.zeros((planes, LANES), jnp.float32)
        else:
            tail = edge[field, c]
        return jnp.concatenate([state[field, c], tail], axis=1)

    def first(c):
        u, v = wide(0, c), wide(1, c)
        su = spread_of(wide(0, c - 1), u, wide(0, c + 1))
        sv = spread_of(wide(1, c - 1), v, wide(1, c + 1))
        middle[0, c], middle[1, c] = react(u, v, su, sv)

    level = [{}, {}]

    def second(c):
        u, v = middle[0, c], middle[1, c]
        su = spread_of(middle[0, c - 1], u, middle[0, c + 1])
        sv = spread_of(middle[1, c - 1], v, middle[1, c + 1])
        new = react(u[:, :extent], v[:, :extent], su[:, :extent], sv[:, :extent])
        for field, out in enumerate((u_out, v_out)):
            for tile in range(tiles):
                rows = pl.ds(tile * columns + c - 2, planes, stride=tiles * columns)
                out[rows, :] = new[field][:, tile * LANES : (tile + 1) * LANES]
            level[field][c - 2] = new[field]

    for c in range(3, columns + 1):
        first(c)
    for c in range(4, columns):
        second(c)
    for side, (outer, steps, last) in enumerate(
        ((1, (1, 2), (2, 3)), (columns + 2, (columns + 2, columns + 1), (columns + 1, columns)))
    ):
        along[side].wait_recv()
        for copy in corners[2 * side : 2 * side + 2]:
            copy.wait_recv()
        beyond = merged(corner, 2 * side)
        for field in range(2):
            place(field, outer, beyond, (1 - side) * (columns - 1))
        for c in steps:
            first(c)
        for c in last:
            second(c)

    pairs = columns // 2
    for field in range(2):
        twos = [level[field][2 * k] + level[field][2 * k + 1] for k in range(pairs)]
        fours = [twos[2 * q] + twos[2 * q + 1] for q in range(pairs // 2)]
        for k in range(pairs):
            rows = pl.ds(field * planes * pairs + k, planes, stride=pairs)
            for tile in range(tiles):
                lanes = slice(tile * LANES, (tile + 1) * LANES)
                sums[tile, rows, :] = twos[k][:, lanes]
                sums[tiles + tile, rows, :] = fours[k // 2][:, lanes]

    contract = (((1,), (1,)), ((), ()))
    high, low = split(jnp.concatenate([sums[tile] for tile in range(2 * tiles)], axis=1))
    blend = lax.dot_general(to_blend, high, contract, preferred_element_type=jnp.float32)
    blend += lax.dot_general(to_blend, low, contract, preferred_element_type=jnp.float32)
    portion = half // owners
    for owner in range(owners):
        outgoing[owner] = blend[owner * portion : (owner + 1) * portion]

    deals = []
    for step in range(owners - 1, 0, -1):
        partner = partner_of(gy, step, owners)
        deals.append(
            pltpu.make_async_remote_copy(
                src_ref=outgoing.at[partner],
                dst_ref=gathered.at[gy],
                send_sem=deal_send.at[step - 1],
                recv_sem=deal_recv.at[step - 1],
                device_id=(gx, partner),
                device_id_type=MESH,
            )
        )
        deals[-1].start()
    gathered[gy] = outgoing[gy]

    for deal in deals:
        deal.wait_recv()

    for copy in across + along + corners:
        copy.wait_send()
    for deal in deals:
        deal.wait_send()


def finish(u_ref, v_ref, dealt, u_out, v_out, rebuilt_out, doubled, rebuilt, sems):
    copies = [
        pltpu.make_async_copy(u_ref, u_out, sems.at[0]),
        pltpu.make_async_copy(v_ref, v_out, sems.at[1]),
    ]
    for copy in copies:
        copy.start()

    owners, portion, _ = dealt.shape
    wide_in = lax.broadcasted_iota(jnp.int32, (LANES, 4 * LANES), 0)
    wide_out = lax.broadcasted_iota(jnp.int32, (LANES, 4 * LANES), 1)
    column_of = wide_in // 16 * 4 + wide_in % 4
    spreading = jnp.where(
        (wide_in // 4 % 4 == wide_out // LANES) & (column_of == wide_out % LANES // 2),
        1.0,
        0.0,
    ).astype(jnp.bfloat16)
    lane = lax.broadcasted_iota(jnp.int32, (portion, LANES), 1)
    blocks = [dealt[owner] for owner in range(owners)]
    width, rows = rebuilt.shape[1], 2 * portion
    chunks = 4
    share = 8 // chunks
    for chunk in range(chunks):
        for h in range(chunk * share, (chunk + 1) * share):
            part = jnp.zeros((portion, LANES), jnp.float32)
            for owner in range(8):
                shift = (16 * (owner - h)) % LANES
                moved = pltpu.roll(blocks[owner], shift, 1) if shift else blocks[owner]
                part = jnp.where(lane // 16 == owner, moved, part)
            doubled[pl.ds(h * rows, portion, stride=2), :] = part
            doubled[pl.ds(h * rows + 1, portion, stride=2), :] = part
        high, low = split(doubled[chunk * share * rows : (chunk + 1) * share * rows, :])
        whole = jnp.dot(high, spreading, preferred_element_type=jnp.float32)
        whole += jnp.dot(low, spreading, preferred_element_type=jnp.float32)
        for h in range(share):
            for z in range(4):
                base = ((chunk * share + h) * 4 + z) * rows
                rebuilt[base : base + rows, :] = whole[
                    h * rows : (h + 1) * rows, z * LANES : z * LANES + width
                ]
        size = share * 4 * rows
        copies.append(
            pltpu.make_async_copy(
                rebuilt.at[chunk * size : (chunk + 1) * size],
                rebuilt_out.at[chunk * size : (chunk + 1) * size],
                sems.at[2 + chunk],
            )
        )
        copies[-1].start()
    for copy in copies:
        copy.wait()


def tiled(field):
    planes, columns, extent = field.shape
    field = field.reshape(planes, columns, extent // LANES, LANES)
    return jnp.transpose(field, (0, 2, 1, 3)).reshape(-1, LANES)


def untiled(field, shape):
    planes, columns, extent = shape
    field = field.reshape(planes, extent // LANES, columns, LANES)
    return jnp.transpose(field, (0, 2, 1, 3)).reshape(shape)


def body(substrate, catalyst):
    planes, columns, extent = substrate.shape
    slabs_x, owners = lax.axis_size("gx"), lax.axis_size("gy")
    half, pairs, tiles = extent // 2, columns // 2, extent // LANES
    portion = half // owners
    values = 2 * planes * pairs
    fused = (
        planes == 16 and pairs == 4 and owners == 8 and values == LANES and portion % 8 == 0
    )
    dims = (planes, columns, extent, owners, slabs_x, owners)
    f32 = jnp.float32
    flat = (planes * tiles * columns, LANES)
    vmem = pl.BlockSpec(memory_space=pltpu.VMEM)
    anywhere = pl.BlockSpec(memory_space=pl.ANY)
    u, v, dealt = pl.pallas_call(
        functools.partial(kernel, dims),
        out_shape=(
            pltpu.VMEM(flat, f32),
            pltpu.VMEM(flat, f32),
            pltpu.VMEM((owners, portion, values), f32),
        ),
        in_specs=[anywhere] * 2,
        out_specs=(vmem,) * 3,
        scratch_shapes=[
            pltpu.VMEM((2,) + flat, f32),
            pltpu.VMEM((2, columns + 4, planes, extent), f32),
            pltpu.VMEM((2, columns + 4, planes, LANES), f32),
            pltpu.VMEM((planes, LANES), f32),
            pltpu.VMEM((2, planes, LANES), f32),
            pltpu.VMEM((4, planes, LANES), f32),
            pltpu.VMEM((2, columns + 4, planes, extent + LANES), f32),
            pltpu.VMEM((2 * tiles, values, LANES), f32),
            pltpu.VMEM((owners, portion, values), f32),
            pltpu.SemaphoreType.DMA((2,)),
            pltpu.SemaphoreType.DMA((8,)),
            pltpu.SemaphoreType.DMA((8,)),
            pltpu.SemaphoreType.DMA((owners - 1,)),
            pltpu.SemaphoreType.DMA((owners - 1,)),
        ],
        compiler_params=pltpu.CompilerParams(collective_id=0, has_side_effects=True),
    )(tiled(substrate), tiled(catalyst))
    rows, width = 2 * portion, columns * owners
    if fused:
        u, v, dealt = (
            pltpu.with_memory_space_constraint(x, pltpu.VMEM) for x in (u, v, dealt)
        )
        u, v, rebuilt = pl.pallas_call(
            finish,
            out_shape=(
                jax.ShapeDtypeStruct(flat, f32),
                jax.ShapeDtypeStruct(flat, f32),
                jax.ShapeDtypeStruct((2 * planes * rows, width), f32),
            ),
            in_specs=[vmem] * 3,
            out_specs=(anywhere,) * 3,
            scratch_shapes=[
                pltpu.VMEM((8 * rows, LANES), f32),
                pltpu.VMEM((2 * planes * rows, width), f32),
                pltpu.SemaphoreType.DMA((6,)),
            ],
        )(u, v, dealt)
        rebuilt = rebuilt.reshape(2, planes, rows, width)
    else:
        blend = dealt.reshape(owners, portion, 2, planes, pairs)
        blend = jnp.transpose(blend, (2, 3, 1, 0, 4)).reshape(2, planes, portion, owners * pairs)
        rebuilt = jnp.repeat(jnp.repeat(blend, 2, axis=2), 2, axis=3)
    return untiled(u, substrate.shape), untiled(v, substrate.shape), rebuilt


def solution(mesh):
    in_specs = (P(None, "gy", "gx"), P(None, "gy", "gx"))
    out_specs = (P(None, "gy", "gx"), P(None, "gy", "gx"), P(None, None, ("gx", "gy"), None))
    return jax.shard_map(body, mesh=mesh, in_specs=in_specs, out_specs=out_specs, check_vma=False)
```

```python
import functools

import jax
import jax.numpy as jnp
from jax import lax
from jax.experimental import pallas as pl
from jax.experimental.pallas import tpu as pltpu
from jax.sharding import PartitionSpec as P

feed_rate = 0.037
kill_rate = 0.06
substrate_diffusion = 0.15
catalyst_diffusion = 0.08

MESH = pl.DeviceIdType.MESH
LANES = 128


def react(substrate, catalyst, spread_substrate, spread_catalyst):
    reaction = substrate * catalyst * catalyst
    new_substrate = (
        substrate
        + substrate_diffusion * spread_substrate
        - reaction
        + feed_rate * (1.0 - substrate)
    )
    new_catalyst = (
        catalyst
        + catalyst_diffusion * spread_catalyst
        + reaction
        - (feed_rate + kill_rate) * catalyst
    )
    return new_substrate, new_catalyst


def split(value):
    high = value.astype(jnp.bfloat16)
    low = (value - high.astype(jnp.float32)).astype(jnp.bfloat16)
    return high, low


def spread_of(before, here, after):
    planes, extent = here.shape
    total = pltpu.roll(here, 1, 0) + pltpu.roll(here, planes - 1, 0)
    total = total + before + after
    total = total + pltpu.roll(here, 1, 1) + pltpu.roll(here, extent - 1, 1)
    return total - 6.0 * here


def partner_of(me, step, size):
    if size & (size - 1):
        return lax.rem(me + step, size)
    partner = me + step
    for bit in range(size.bit_length() - 1):
        if step >> bit & 1:
            partner = partner - 2 * (1 << bit) * lax.rem(me // (1 << bit), 2)
    return partner


def kernel(dims, *refs):
    planes, columns, extent, owners, slabs_x = dims
    (u_ref, v_ref, u_out, v_out, gathered, loaded, state, edge, packed, got, corner, middle, sums, outgoing,
     load_sem, send_sem, recv_sem, deal_send, deal_recv, late_send, late_recv, far) = refs
    tiles, pairs, last = extent // LANES, columns // 2, owners - 1
    gx, gy = lax.axis_index("gx"), lax.axis_index("gy")
    at_top, at_bottom = gy // last, (last - gy) // last

    barrier = pltpu.get_barrier_semaphore()
    across_of = [lax.rem(gx + shift, slabs_x) for shift in (1, slabs_x - 1)]
    along_of = [lax.rem(gy + shift, owners) for shift in (1, owners - 1)]

    def greet(semaphore, x, y):
        pl.semaphore_signal(semaphore, inc=1, device_id=(x, y), device_id_type=MESH)

    for x in across_of:
        greet(barrier, x, gy)
        greet(barrier, x, along_of[1])

    @pl.when(gy < last)
    def _():
        for x in across_of:
            greet(barrier, x, gy + 1)

    for peer in range(owners):

        @pl.when((peer > gy) | (peer == gy - 1))
        def _():
            greet(barrier, gx, peer)

    near_count = 4 + gy + (1 - at_top) + 2 * (1 - at_bottom)
    far_count = last - gy - 1 + 2 * at_bottom

    loads = [
        pltpu.make_async_copy(source, loaded.at[field], load_sem.at[field])
        for field, source in enumerate((u_ref, v_ref))
    ]
    for load in loads:
        load.start()
    for load in loads:
        load.wait()

    low = 4
    high = low + columns
    lane = lax.broadcasted_iota(jnp.int32, (planes, LANES), 1)
    group = lax.rem(lane + 2, LANES) // 4
    pack = jnp.zeros((planes, LANES), jnp.float32)
    for field in range(2):
        for column in range(columns):
            slab = jnp.concatenate(
                [
                    loaded[field, pl.ds(tile * columns + column, planes, stride=tiles * columns), :]
                    for tile in range(tiles)
                ],
                axis=1,
            )
            state[field, low + column] = slab
            at = field * columns + column
            tips = jnp.where(lane < LANES // 2, slab[:, :LANES], slab[:, extent - LANES :])
            tips = pltpu.roll(tips, 4 * at, 1) if at else tips
            pack = jnp.where(group == at, tips, pack)
    packed[...] = pack

    pl.semaphore_wait(barrier, near_count)

    def send(number, source, target, x, y):
        return pltpu.make_async_remote_copy(
            src_ref=source,
            dst_ref=target,
            send_sem=send_sem.at[number],
            recv_sem=recv_sem.at[number],
            device_id=(x, y),
            device_id_type=MESH,
        )

    up = send(0, state.at[:, high - 2 : high], state.at[:, low - 2 : low], gx, along_of[0])
    down = send(1, state.at[:, low : low + 2], state.at[:, high : high + 2], gx, along_of[1])
    wrap = send(2, state.at[:, high - 4 : high - 2], state.at[:, low - 4 : low - 2], gx, along_of[0])
    across = [send(3 + side, packed, got.at[side], across_of[side], gy) for side in range(2)]
    corners_up = [send(5 + side, packed, corner.at[0, side], across_of[side], along_of[0]) for side in range(2)]
    corners_down = [send(7 + side, packed, corner.at[1, side], across_of[side], along_of[1]) for side in range(2)]
    for copy in across + corners_up + [up]:
        copy.start()

    @pl.when(gy > 0)
    def _():
        for copy in corners_down + [down]:
            copy.start()

    @pl.when(gy == last)
    def _():
        wrap.start()
        for x in across_of:
            greet(far, x, 0)

    for peer in range(owners - 2):

        @pl.when(peer < gy - 1)
        def _():
            greet(far, gx, peer)

    half = extent // 2
    row = lax.broadcasted_iota(jnp.int32, (half, extent), 0)
    fine = lax.broadcasted_iota(jnp.int32, (half, extent), 1)
    to_level = jnp.where(fine // 2 == row, 0.25, 0.0).astype(jnp.bfloat16)

    for copy in across:
        copy.wait_recv()

    def merged(below, above):
        return jnp.where(lax.rem(lane, 4) < 2, above, below)

    def place(c, tips, column):
        for field in range(2):
            at = field * columns + column
            edge[field, c] = pltpu.roll(tips, LANES - 4 * at, 1) if at else tips

    both = merged(got[0], got[1])
    for column in range(columns):
        place(low + column, both, column)

    def wide(field, c, outer=()):
        tail = jnp.zeros((planes, LANES), jnp.float32) if c in outer else edge[field, c]
        return jnp.concatenate([state[field, c], tail], axis=1)

    def first(c, outer=()):
        u, v = wide(0, c), wide(1, c)
        su = spread_of(wide(0, c - 1, outer), u, wide(0, c + 1, outer))
        sv = spread_of(wide(1, c - 1, outer), v, wide(1, c + 1, outer))
        middle[0, c], middle[1, c] = react(u, v, su, sv)

    def second(c):
        u, v = middle[0, c], middle[1, c]
        su = spread_of(middle[0, c - 1], u, middle[0, c + 1])
        sv = spread_of(middle[1, c - 1], v, middle[1, c + 1])
        return react(u[:, :extent], v[:, :extent], su[:, :extent], sv[:, :extent])

    def pair(k, c, own=True):
        new = [second(c), second(c + 1)]
        for field, out in enumerate((u_out, v_out)):
            for tile in range(tiles):
                lanes = slice(tile * LANES, (tile + 1) * LANES)
                parts = [new[i][field][:, lanes] for i in range(2)]
                if own:
                    for i in range(2):
                        rows = pl.ds(tile * columns + c - low + i, planes, stride=tiles * columns)
                        out[rows, :] = parts[i]
                rows = pl.ds(field * planes * pairs + k, planes, stride=pairs)
                sums[tile, rows, :] = parts[0] + parts[1]

    def low_side(wrapped):
        up.wait_recv()
        for copy in corners_up:
            copy.wait_recv()
        beyond = merged(corner[0, 0], corner[0, 1])
        for step in range(1, 4 if wrapped else 2):
            place(low - step, beyond, columns - step)
        first(low)
        first(low - 1, () if wrapped else (low - 2,))
        pair(0, low)

    def high_side():
        down.wait_recv()
        for copy in corners_down:
            copy.wait_recv()
        place(high, merged(corner[1, 0], corner[1, 1]), 0)
        first(high - 1)
        first(high, (high + 1,))
        pair(pairs - 1, high - 2)

    def level_of():
        contract = (((1,), (1,)), ((), ()))
        upper, lower = split(jnp.concatenate([sums[tile] for tile in range(tiles)], axis=1))
        level = lax.dot_general(to_level, upper, contract, preferred_element_type=jnp.float32)
        return level + lax.dot_general(to_level, lower, contract, preferred_element_type=jnp.float32)

    portion = half // owners

    for c in range(low + 1, high - 1):
        first(c)
    for k in range(1, pairs - 1):
        pair(k, low + 2 * k)

    @pl.when(gy > 0)
    def _():
        low_side(False)

    @pl.when(gy < last)
    def _():
        high_side()

    @pl.when(gy < last - 1)
    def _():
        pl.semaphore_wait(far, far_count)

    @pl.when(gy == 0)
    def _():
        for copy in corners_down + [down]:
            copy.start()
        low_side(True)

    level = level_of()
    for owner in range(owners):
        outgoing[0, owner] = level[owner * portion : (owner + 1) * portion]

    deals = []
    for step in range(owners - 1, 0, -1):
        partner = partner_of(gy, step, owners)
        deals.append(
            pltpu.make_async_remote_copy(
                src_ref=outgoing.at[0, partner],
                dst_ref=gathered.at[gy],
                send_sem=deal_send.at[step - 1],
                recv_sem=deal_recv.at[step - 1],
                device_id=(gx, partner),
                device_id_type=MESH,
            )
        )
        deals[-1].start()
    gathered[gy] = outgoing[0, gy]

    late = [
        pltpu.make_async_remote_copy(
            src_ref=outgoing.at[1, owner],
            dst_ref=gathered.at[owners],
            send_sem=late_send.at[owner - 1],
            recv_sem=late_recv,
            device_id=(gx, owner),
            device_id_type=MESH,
        )
        for owner in range(1, owners)
    ]

    @pl.when(gy == 0)
    def _():
        wrap.wait_recv()
        first(low - 2)
        first(low - 3, (low - 4,))
        pair(pairs - 1, low - 2, own=False)
        level = level_of()
        for owner in range(owners):
            outgoing[1, owner] = level[owner * portion : (owner + 1) * portion]
        for copy in late:
            copy.start()
        gathered[owners] = outgoing[1, 0]

    @pl.when(gy == last)
    def _():
        high_side()

    for deal in deals:
        deal.wait_recv()

    @pl.when(gy > 0)
    def _():
        late[0].wait_recv()

    for copy in across + corners_up + corners_down + [up, down]:
        copy.wait_send()
    for deal in deals:
        deal.wait_send()

    @pl.when(gy == 0)
    def _():
        for copy in late:
            copy.wait_send()

    @pl.when(gy == last)
    def _():
        wrap.wait_send()


def finish(u_ref, v_ref, dealt, u_out, v_out, rebuilt_out, doubled, paired, rebuilt, sems):
    copies = [
        pltpu.make_async_copy(u_ref, u_out, sems.at[0]),
        pltpu.make_async_copy(v_ref, v_out, sems.at[1]),
    ]
    for copy in copies:
        copy.start()

    owners, portion = dealt.shape[0] - 1, dealt.shape[1]
    wide_in = lax.broadcasted_iota(jnp.int32, (LANES, 4 * LANES), 0)
    wide_out = lax.broadcasted_iota(jnp.int32, (LANES, 4 * LANES), 1)
    column_of = wide_in // 16 * 4 + wide_in % 4
    plane = wide_in // 4 % 4 == wide_out // LANES
    spreading = jnp.concatenate(
        [
            jnp.where(plane & (column_of == wide_out % LANES // 2), 0.5, 0.0),
            jnp.where(plane & (column_of // 2 == wide_out % LANES // 4), 0.125, 0.0),
        ],
        axis=0,
    ).astype(jnp.bfloat16)
    lane = lax.broadcasted_iota(jnp.int32, (portion, LANES), 1)
    even = lax.broadcasted_iota(jnp.int32, (portion, LANES), 0) % 2 == 0
    blocks = [dealt[owner] for owner in range(owners)]
    blocks[-1] = jnp.where(lane % 4 == 3, dealt[owners], blocks[-1])
    width, rows = rebuilt.shape[1], 2 * portion
    chunks = 4
    share = 8 // chunks
    for chunk in range(chunks):
        for h in range(chunk * share, (chunk + 1) * share):
            part = jnp.zeros((portion, LANES), jnp.float32)
            for owner in range(8):
                shift = (16 * (owner - h)) % LANES
                moved = pltpu.roll(blocks[owner], shift, 1) if shift else blocks[owner]
                part = jnp.where(lane // 16 == owner, moved, part)
            other = jnp.where(even, pltpu.roll(part, portion - 1, 0), pltpu.roll(part, 1, 0))
            total = part + other
            for twin in range(2):
                doubled[pl.ds(h * rows + twin, portion, stride=2), :] = part
                paired[pl.ds(h * rows + twin, portion, stride=2), :] = total
        span = slice(chunk * share * rows, (chunk + 1) * share * rows)
        high, low = split(jnp.concatenate([doubled[span, :], paired[span, :]], axis=1))
        whole = jnp.dot(high, spreading, preferred_element_type=jnp.float32)
        whole += jnp.dot(low, spreading, preferred_element_type=jnp.float32)
        for h in range(share):
            for z in range(4):
                base = ((chunk * share + h) * 4 + z) * rows
                rebuilt[base : base + rows, :] = whole[
                    h * rows : (h + 1) * rows, z * LANES : z * LANES + width
                ]
        size = share * 4 * rows
        copies.append(
            pltpu.make_async_copy(
                rebuilt.at[chunk * size : (chunk + 1) * size],
                rebuilt_out.at[chunk * size : (chunk + 1) * size],
                sems.at[2 + chunk],
            )
        )
        copies[-1].start()
    for copy in copies:
        copy.wait()


def tiled(field):
    planes, columns, extent = field.shape
    field = field.reshape(planes, columns, extent // LANES, LANES)
    return jnp.transpose(field, (0, 2, 1, 3)).reshape(-1, LANES)


def untiled(field, shape):
    planes, columns, extent = shape
    field = field.reshape(planes, extent // LANES, columns, LANES)
    return jnp.transpose(field, (0, 2, 1, 3)).reshape(shape)


def body(substrate, catalyst):
    planes, columns, extent = substrate.shape
    slabs_x, owners = lax.axis_size("gx"), lax.axis_size("gy")
    half, pairs, tiles = extent // 2, columns // 2, extent // LANES
    portion = half // owners
    values = 2 * planes * pairs
    fused = (
        planes == 16 and pairs == 4 and owners == 8 and values == LANES and portion % 8 == 0
    )
    dims = (planes, columns, extent, owners, slabs_x)
    f32 = jnp.float32
    flat = (planes * tiles * columns, LANES)
    vmem = pl.BlockSpec(memory_space=pltpu.VMEM)
    anywhere = pl.BlockSpec(memory_space=pl.ANY)
    u, v, dealt = pl.pallas_call(
        functools.partial(kernel, dims),
        out_shape=(
            pltpu.VMEM(flat, f32),
            pltpu.VMEM(flat, f32),
            pltpu.VMEM((owners + 1, portion, values), f32),
        ),
        in_specs=[anywhere] * 2,
        out_specs=(vmem,) * 3,
        scratch_shapes=[
            pltpu.VMEM((2,) + flat, f32),
            pltpu.VMEM((2, columns + 6, planes, extent), f32),
            pltpu.VMEM((2, columns + 6, planes, LANES), f32),
            pltpu.VMEM((planes, LANES), f32),
            pltpu.VMEM((2, planes, LANES), f32),
            pltpu.VMEM((2, 2, planes, LANES), f32),
            pltpu.VMEM((2, columns + 6, planes, extent + LANES), f32),
            pltpu.VMEM((tiles, values, LANES), f32),
            pltpu.VMEM((2, owners, portion, values), f32),
            pltpu.SemaphoreType.DMA((2,)),
            pltpu.SemaphoreType.DMA((9,)),
            pltpu.SemaphoreType.DMA((9,)),
            pltpu.SemaphoreType.DMA((owners - 1,)),
            pltpu.SemaphoreType.DMA((owners - 1,)),
            pltpu.SemaphoreType.DMA((owners - 1,)),
            pltpu.SemaphoreType.DMA,
            pltpu.SemaphoreType.REGULAR,
        ],
        compiler_params=pltpu.CompilerParams(collective_id=0, has_side_effects=True),
    )(tiled(substrate), tiled(catalyst))
    rows, width = 2 * portion, columns * owners
    if fused:
        u, v, dealt = (
            pltpu.with_memory_space_constraint(x, pltpu.VMEM) for x in (u, v, dealt)
        )
        u, v, rebuilt = pl.pallas_call(
            finish,
            out_shape=(
                jax.ShapeDtypeStruct(flat, f32),
                jax.ShapeDtypeStruct(flat, f32),
                jax.ShapeDtypeStruct((2 * planes * rows, width), f32),
            ),
            in_specs=[vmem] * 3,
            out_specs=(anywhere,) * 3,
            scratch_shapes=[
                pltpu.VMEM((8 * rows, LANES), f32),
                pltpu.VMEM((8 * rows, LANES), f32),
                pltpu.VMEM((2 * planes * rows, width), f32),
                pltpu.SemaphoreType.DMA((6,)),
            ],
        )(u, v, dealt)
        rebuilt = rebuilt.reshape(2, planes, rows, width)
    else:
        level = dealt.reshape(owners + 1, portion, 2, planes, pairs)
        latest = jnp.concatenate([level[owners - 1, ..., :-1], level[owners, ..., -1:]], axis=-1)
        level = jnp.concatenate([level[: owners - 1], latest[None]], axis=0)
        level = jnp.transpose(level, (2, 3, 1, 0, 4)).reshape(2, planes, portion // 2, 2, columns * owners // 4, 2)
        coarse = 0.25 * jnp.sum(level, axis=(3, 5), keepdims=True)
        blend = (coarse + 0.5 * (level - coarse)).reshape(2, planes, portion, columns * owners // 2)
        rebuilt = jnp.repeat(jnp.repeat(blend, 2, axis=2), 2, axis=3)
    return untiled(u, substrate.shape), untiled(v, substrate.shape), rebuilt


def solution(mesh):
    in_specs = (P(None, "gy", "gx"), P(None, "gy", "gx"))
    out_specs = (P(None, "gy", "gx"), P(None, "gy", "gx"), P(None, None, ("gx", "gy"), None))
    return jax.shard_map(body, mesh=mesh, in_specs=in_specs, out_specs=out_specs, check_vma=False)
```

```python
import functools

import jax
import jax.numpy as jnp
from jax import lax
from jax.experimental import pallas as pl
from jax.experimental.pallas import tpu as pltpu
from jax.sharding import PartitionSpec as P

feed_rate = 0.037
kill_rate = 0.06
substrate_diffusion = 0.15
catalyst_diffusion = 0.08

MESH = pl.DeviceIdType.MESH
LANES = 128


def react(substrate, catalyst, spread_substrate, spread_catalyst):
    reaction = substrate * catalyst * catalyst
    new_substrate = (
        substrate
        + substrate_diffusion * spread_substrate
        - reaction
        + feed_rate * (1.0 - substrate)
    )
    new_catalyst = (
        catalyst
        + catalyst_diffusion * spread_catalyst
        + reaction
        - (feed_rate + kill_rate) * catalyst
    )
    return new_substrate, new_catalyst


def split(value):
    high = value.astype(jnp.bfloat16)
    low = (value - high.astype(jnp.float32)).astype(jnp.bfloat16)
    return high, low


def spread_of(before, here, after):
    planes, extent = here.shape
    total = pltpu.roll(here, 1, 0) + pltpu.roll(here, planes - 1, 0)
    total = total + before + after
    total = total + pltpu.roll(here, 1, 1) + pltpu.roll(here, extent - 1, 1)
    return total - 6.0 * here


def kernel(dims, *refs):
    planes, columns, extent, owners, slabs_x = dims
    (u_ref, v_ref, u_out, v_out, gathered, loaded, state, edge, packed, got, corner, middle, sums, outgoing,
     load_sem, send_sem, recv_sem, deal_send, deal_recv, late_send, late_recv, far) = refs
    tiles, pairs, last = extent // LANES, columns // 2, owners - 1
    half = extent // 2
    portion = half // owners
    widths = (LANES, extent) if tiles > 1 else (extent,)
    dealt_to = [(width - 2) // (2 * portion) for width in widths[:-1]] + [owners]
    spans = list(zip((0,) + widths[:-1], widths))
    shares = list(zip([0] + dealt_to[:-1], dealt_to))
    parts = range(len(widths))
    gx, gy = lax.axis_index("gx"), lax.axis_index("gy")
    at_top, at_bottom = gy // last, (last - gy) // last

    barrier = pltpu.get_barrier_semaphore()
    across_of = [lax.rem(gx + shift, slabs_x) for shift in (1, slabs_x - 1)]
    along_of = [lax.rem(gy + shift, owners) for shift in (1, owners - 1)]

    def greet(semaphore, x, y):
        pl.semaphore_signal(semaphore, inc=1, device_id=(x, y), device_id_type=MESH)

    for x in across_of:
        greet(barrier, x, gy)
        greet(barrier, x, along_of[1])

    @pl.when(gy < last)
    def _():
        for x in across_of:
            greet(barrier, x, gy + 1)

    for peer in range(owners):

        @pl.when((peer > gy) | (peer == gy - 1))
        def _():
            greet(barrier, gx, peer)

    near_count = 4 + gy + (1 - at_top) + 2 * (1 - at_bottom)
    far_count = last - gy - 1 + 2 * at_bottom

    loads = [
        pltpu.make_async_copy(source, loaded.at[field], load_sem.at[field])
        for field, source in enumerate((u_ref, v_ref))
    ]
    for load in loads:
        load.start()
    for load in loads:
        load.wait()

    low = 4
    high = low + columns
    lane = lax.broadcasted_iota(jnp.int32, (planes, LANES), 1)
    group = lax.rem(lane + 2, LANES) // 4
    pack = jnp.zeros((planes, LANES), jnp.float32)
    for field in range(2):
        for column in range(columns):
            slab = jnp.concatenate(
                [
                    loaded[field, pl.ds(tile * columns + column, planes, stride=tiles * columns), :]
                    for tile in range(tiles)
                ],
                axis=1,
            )
            state[field, low + column] = slab
            at = field * columns + column
            tips = jnp.where(lane < LANES // 2, slab[:, :LANES], slab[:, extent - LANES :])
            tips = pltpu.roll(tips, 4 * at, 1) if at else tips
            pack = jnp.where(group == at, tips, pack)
    packed[...] = pack

    pl.semaphore_wait(barrier, near_count)

    def send(number, source, target, x, y):
        return pltpu.make_async_remote_copy(
            src_ref=source,
            dst_ref=target,
            send_sem=send_sem.at[number],
            recv_sem=recv_sem.at[number],
            device_id=(x, y),
            device_id_type=MESH,
        )

    def columns_of(first_column, count, part):
        return state.at[:, first_column : first_column + count, :, slice(*spans[part])]

    across = [send(side, packed, got.at[side], across_of[side], gy) for side in range(2)]
    corners_up = [send(2 + side, packed, corner.at[0, side], across_of[side], along_of[0]) for side in range(2)]
    corners_down = [send(4 + side, packed, corner.at[1, side], across_of[side], along_of[1]) for side in range(2)]
    up, down, wrap = [
        [
            send(6 + 3 * part + kind, columns_of(source, 2, part), columns_of(target, 2, part), gx, along_of[way])
            for part in parts
        ]
        for kind, source, target, way in (
            (0, high - 2, low - 2, 0),
            (1, low, high, 1),
            (2, high - 4, low - 4, 0),
        )
    ]

    @pl.when(gy == last)
    def _():
        for x in across_of:
            greet(far, x, 0)

    for peer in range(owners - 2):

        @pl.when(peer < gy - 1)
        def _():
            greet(far, gx, peer)

    for copy in across + corners_up:
        copy.start()

    @pl.when(gy > 0)
    def _():
        for copy in corners_down:
            copy.start()

    for part in parts:
        up[part].start()

        @pl.when(gy > 0)
        def _():
            down[part].start()

        @pl.when(gy == last)
        def _():
            wrap[part].start()

    row = lax.broadcasted_iota(jnp.int32, (half, extent), 0)
    fine = lax.broadcasted_iota(jnp.int32, (half, extent), 1)
    to_level = jnp.where(fine // 2 == row, 0.25, 0.0).astype(jnp.bfloat16)

    for copy in across:
        copy.wait_recv()

    def merged(below, above):
        return jnp.where(lax.rem(lane, 4) < 2, above, below)

    def place(c, tips, column):
        for field in range(2):
            at = field * columns + column
            edge[field, c] = pltpu.roll(tips, LANES - 4 * at, 1) if at else tips

    both = merged(got[0], got[1])
    for column in range(columns):
        place(low + column, both, column)

    def wide(field, c, width, outer=()):
        tail = jnp.zeros((planes, LANES), jnp.float32) if c in outer else edge[field, c]
        return jnp.concatenate([state[field, c, :, :width], tail], axis=1)

    def first(c, width, outer=()):
        u, v = wide(0, c, width), wide(1, c, width)
        su = spread_of(wide(0, c - 1, width, outer), u, wide(0, c + 1, width, outer))
        sv = spread_of(wide(1, c - 1, width, outer), v, wide(1, c + 1, width, outer))
        for field, new in enumerate(react(u, v, su, sv)):
            middle[field, c, :, :width] = new[:, :width]
            middle[field, c, :, extent:] = new[:, width:]

    def half_way(field, c, width):
        return jnp.concatenate([middle[field, c, :, :width], middle[field, c, :, extent:]], axis=1)

    def second(c, width):
        u, v = half_way(0, c, width), half_way(1, c, width)
        su = spread_of(half_way(0, c - 1, width), u, half_way(0, c + 1, width))
        sv = spread_of(half_way(1, c - 1, width), v, half_way(1, c + 1, width))
        return react(u[:, :width], v[:, :width], su[:, :width], sv[:, :width])

    def pair(k, c, width=extent, own=True):
        new = [second(c, width), second(c + 1, width)]
        for field, out in enumerate((u_out, v_out)):
            for tile in range(width // LANES):
                lanes = slice(tile * LANES, (tile + 1) * LANES)
                both_of = [new[i][field][:, lanes] for i in range(2)]
                if own:
                    for i in range(2):
                        rows = pl.ds(tile * columns + c - low + i, planes, stride=tiles * columns)
                        out[rows, :] = both_of[i]
                rows = pl.ds(field * planes * pairs + k, planes, stride=pairs)
                sums[tile, rows, :] = both_of[0] + both_of[1]

    final = len(widths) - 1

    def low_side(part, wrapped):
        width = widths[part]
        up[part].wait_recv()
        if part == 0:
            for copy in corners_up:
                copy.wait_recv()
            beyond = merged(corner[0, 0], corner[0, 1])
            for step in range(1, 4 if wrapped else 2):
                place(low - step, beyond, columns - step)
        first(low, width)
        first(low - 1, width, () if wrapped else (low - 2,))
        pair(0, low, width, own=part == final)

    def high_side(part):
        width = widths[part]
        down[part].wait_recv()
        if part == 0:
            for copy in corners_down:
                copy.wait_recv()
            place(high, merged(corner[1, 0], corner[1, 1]), 0)
        first(high - 1, width)
        first(high, width, (high + 1,))
        pair(pairs - 1, high - 2, width, own=part == final)

    def level_of(slot, part):
        width = widths[part]
        contract = (((1,), (1,)), ((), ()))
        taking = to_level[: width // 2, :width]
        upper, lower = split(jnp.concatenate([sums[tile] for tile in range(width // LANES)], axis=1))
        level = lax.dot_general(taking, upper, contract, preferred_element_type=jnp.float32)
        level += lax.dot_general(taking, lower, contract, preferred_element_type=jnp.float32)
        for owner in range(*shares[part]):
            outgoing[slot, owner] = level[owner * portion : (owner + 1) * portion]

    def deal(slot, owner, target, sender, receiver):
        return pltpu.make_async_remote_copy(
            src_ref=outgoing.at[slot, owner],
            dst_ref=gathered.at[target],
            send_sem=sender,
            recv_sem=receiver,
            device_id=(gx, owner),
            device_id_type=MESH,
        )

    deals = [deal(0, owner, gy, deal_send.at[owner], deal_recv.at[gy]) for owner in range(owners)]
    late = [None] + [deal(1, owner, owners, late_send.at[owner], late_recv) for owner in range(1, owners)]

    for c in range(low + 1, high - 1):
        first(c, extent)
    for k in range(1, pairs - 1):
        pair(k, low + 2 * k)

    for part in parts:

        @pl.when(gy > 0)
        def _():
            low_side(part, False)

        @pl.when(gy < last)
        def _():
            high_side(part)

        if part == 0:

            @pl.when(gy < last - 1)
            def _():
                pl.semaphore_wait(far, far_count)

        @pl.when(gy == 0)
        def _():
            if part == 0:
                for copy in corners_down + down:
                    copy.start()
            low_side(part, True)

        level_of(0, part)
        for owner in range(*shares[part]):

            @pl.when(owner != gy)
            def _():
                deals[owner].start()

        @pl.when(gy == 0)
        def _():
            wrap[part].wait_recv()
            width = widths[part]
            first(low - 2, width)
            first(low - 3, width, (low - 4,))
            pair(pairs - 1, low - 2, width, own=False)
            level_of(1, part)
            for owner in range(*shares[part]):
                if owner:
                    late[owner].start()

    gathered[gy] = outgoing[0, gy]

    @pl.when(gy == 0)
    def _():
        gathered[owners] = outgoing[1, 0]

    @pl.when(gy == last)
    def _():
        for part in parts:
            if part < final:
                down[part].wait_recv()
        for copy in corners_down:
            copy.wait_recv()
        place(high, merged(corner[1, 0], corner[1, 1]), 0)
        down[final].wait_recv()
        first(high - 1, extent)
        first(high, extent, (high + 1,))
        pair(pairs - 1, high - 2)

    for sender in range(owners):

        @pl.when(sender != gy)
        def _():
            deal(0, sender, sender, deal_send.at[sender], deal_recv.at[sender]).wait_recv()

    @pl.when(gy > 0)
    def _():
        late[1].wait_recv()

    for copy in across + corners_up + corners_down + up + down:
        copy.wait_send()
    for owner in range(owners):

        @pl.when(owner != gy)
        def _():
            deals[owner].wait_send()

    @pl.when(gy == 0)
    def _():
        for copy in late[1:]:
            copy.wait_send()

    @pl.when(gy == last)
    def _():
        for copy in wrap:
            copy.wait_send()


def finish(u_ref, v_ref, dealt, u_out, v_out, rebuilt_out, doubled, paired, rebuilt, sems):
    copies = [
        pltpu.make_async_copy(u_ref, u_out, sems.at[0]),
        pltpu.make_async_copy(v_ref, v_out, sems.at[1]),
    ]
    for copy in copies:
        copy.start()

    owners, portion = dealt.shape[0] - 1, dealt.shape[1]
    wide_in = lax.broadcasted_iota(jnp.int32, (LANES, 4 * LANES), 0)
    wide_out = lax.broadcasted_iota(jnp.int32, (LANES, 4 * LANES), 1)
    column_of = wide_in // 16 * 4 + wide_in % 4
    plane = wide_in // 4 % 4 == wide_out // LANES
    spreading = jnp.concatenate(
        [
            jnp.where(plane & (column_of == wide_out % LANES // 2), 0.5, 0.0),
            jnp.where(plane & (column_of // 2 == wide_out % LANES // 4), 0.125, 0.0),
        ],
        axis=0,
    ).astype(jnp.bfloat16)
    lane = lax.broadcasted_iota(jnp.int32, (portion, LANES), 1)
    even = lax.broadcasted_iota(jnp.int32, (portion, LANES), 0) % 2 == 0
    blocks = [dealt[owner] for owner in range(owners)]
    blocks[-1] = jnp.where(lane % 4 == 3, dealt[owners], blocks[-1])
    width, rows = rebuilt.shape[1], 2 * portion
    chunks = 4
    share = 8 // chunks
    for chunk in range(chunks):
        for h in range(chunk * share, (chunk + 1) * share):
            part = jnp.zeros((portion, LANES), jnp.float32)
            for owner in range(8):
                shift = (16 * (owner - h)) % LANES
                moved = pltpu.roll(blocks[owner], shift, 1) if shift else blocks[owner]
                part = jnp.where(lane // 16 == owner, moved, part)
            other = jnp.where(even, pltpu.roll(part, portion - 1, 0), pltpu.roll(part, 1, 0))
            total = part + other
            for twin in range(2):
                doubled[pl.ds(h * rows + twin, portion, stride=2), :] = part
                paired[pl.ds(h * rows + twin, portion, stride=2), :] = total
        span = slice(chunk * share * rows, (chunk + 1) * share * rows)
        high, low = split(jnp.concatenate([doubled[span, :], paired[span, :]], axis=1))
        whole = jnp.dot(high, spreading, preferred_element_type=jnp.float32)
        whole += jnp.dot(low, spreading, preferred_element_type=jnp.float32)
        for h in range(share):
            for z in range(4):
                base = ((chunk * share + h) * 4 + z) * rows
                rebuilt[base : base + rows, :] = whole[
                    h * rows : (h + 1) * rows, z * LANES : z * LANES + width
                ]
        size = share * 4 * rows
        copies.append(
            pltpu.make_async_copy(
                rebuilt.at[chunk * size : (chunk + 1) * size],
                rebuilt_out.at[chunk * size : (chunk + 1) * size],
                sems.at[2 + chunk],
            )
        )
        copies[-1].start()
    for copy in copies:
        copy.wait()


def tiled(field):
    planes, columns, extent = field.shape
    field = field.reshape(planes, columns, extent // LANES, LANES)
    return jnp.transpose(field, (0, 2, 1, 3)).reshape(-1, LANES)


def untiled(field, shape):
    planes, columns, extent = shape
    field = field.reshape(planes, extent // LANES, columns, LANES)
    return jnp.transpose(field, (0, 2, 1, 3)).reshape(shape)


def body(substrate, catalyst):
    planes, columns, extent = substrate.shape
    slabs_x, owners = lax.axis_size("gx"), lax.axis_size("gy")
    half, pairs, tiles = extent // 2, columns // 2, extent // LANES
    portion = half // owners
    values = 2 * planes * pairs
    fused = (
        planes == 16 and pairs == 4 and owners == 8 and values == LANES and portion % 8 == 0
    )
    dims = (planes, columns, extent, owners, slabs_x)
    f32 = jnp.float32
    flat = (planes * tiles * columns, LANES)
    vmem = pl.BlockSpec(memory_space=pltpu.VMEM)
    anywhere = pl.BlockSpec(memory_space=pl.ANY)
    u, v, dealt = pl.pallas_call(
        functools.partial(kernel, dims),
        out_shape=(
            pltpu.VMEM(flat, f32),
            pltpu.VMEM(flat, f32),
            pltpu.VMEM((owners + 1, portion, values), f32),
        ),
        in_specs=[anywhere] * 2,
        out_specs=(vmem,) * 3,
        scratch_shapes=[
            pltpu.VMEM((2,) + flat, f32),
            pltpu.VMEM((2, columns + 6, planes, extent), f32),
            pltpu.VMEM((2, columns + 6, planes, LANES), f32),
            pltpu.VMEM((planes, LANES), f32),
            pltpu.VMEM((2, planes, LANES), f32),
            pltpu.VMEM((2, 2, planes, LANES), f32),
            pltpu.VMEM((2, columns + 6, planes, extent + LANES), f32),
            pltpu.VMEM((tiles, values, LANES), f32),
            pltpu.VMEM((2, owners, portion, values), f32),
            pltpu.SemaphoreType.DMA((2,)),
            pltpu.SemaphoreType.DMA((12,)),
            pltpu.SemaphoreType.DMA((12,)),
            pltpu.SemaphoreType.DMA((owners,)),
            pltpu.SemaphoreType.DMA((owners,)),
            pltpu.SemaphoreType.DMA((owners,)),
            pltpu.SemaphoreType.DMA,
            pltpu.SemaphoreType.REGULAR,
        ],
        compiler_params=pltpu.CompilerParams(collective_id=0, has_side_effects=True),
    )(tiled(substrate), tiled(catalyst))
    rows, width = 2 * portion, columns * owners
    if fused:
        u, v, dealt = (
            pltpu.with_memory_space_constraint(x, pltpu.VMEM) for x in (u, v, dealt)
        )
        u, v, rebuilt = pl.pallas_call(
            finish,
            out_shape=(
                jax.ShapeDtypeStruct(flat, f32),
                jax.ShapeDtypeStruct(flat, f32),
                jax.ShapeDtypeStruct((2 * planes * rows, width), f32),
            ),
            in_specs=[vmem] * 3,
            out_specs=(anywhere,) * 3,
            scratch_shapes=[
                pltpu.VMEM((8 * rows, LANES), f32),
                pltpu.VMEM((8 * rows, LANES), f32),
                pltpu.VMEM((2 * planes * rows, width), f32),
                pltpu.SemaphoreType.DMA((6,)),
            ],
        )(u, v, dealt)
        rebuilt = rebuilt.reshape(2, planes, rows, width)
    else:
        level = dealt.reshape(owners + 1, portion, 2, planes, pairs)
        latest = jnp.concatenate([level[owners - 1, ..., :-1], level[owners, ..., -1:]], axis=-1)
        level = jnp.concatenate([level[: owners - 1], latest[None]], axis=0)
        level = jnp.transpose(level, (2, 3, 1, 0, 4)).reshape(2, planes, portion // 2, 2, columns * owners // 4, 2)
        coarse = 0.25 * jnp.sum(level, axis=(3, 5), keepdims=True)
        blend = (coarse + 0.5 * (level - coarse)).reshape(2, planes, portion, columns * owners // 2)
        rebuilt = jnp.repeat(jnp.repeat(blend, 2, axis=2), 2, axis=3)
    return untiled(u, substrate.shape), untiled(v, substrate.shape), rebuilt


def solution(mesh):
    in_specs = (P(None, "gy", "gx"), P(None, "gy", "gx"))
    out_specs = (P(None, "gy", "gx"), P(None, "gy", "gx"), P(None, None, ("gx", "gy"), None))
    return jax.shard_map(body, mesh=mesh, in_specs=in_specs, out_specs=out_specs, check_vma=False)
```

```python
import functools

import jax
import jax.numpy as jnp
from jax import lax
from jax.experimental import pallas as pl
from jax.experimental.pallas import tpu as pltpu
from jax.sharding import PartitionSpec as P

feed_rate = 0.037
kill_rate = 0.06
substrate_diffusion = 0.15
catalyst_diffusion = 0.08

MESH = pl.DeviceIdType.MESH
LANES = 128


def react(substrate, catalyst, spread_substrate, spread_catalyst):
    reaction = substrate * catalyst * catalyst
    new_substrate = (
        substrate
        + substrate_diffusion * spread_substrate
        - reaction
        + feed_rate * (1.0 - substrate)
    )
    new_catalyst = (
        catalyst
        + catalyst_diffusion * spread_catalyst
        + reaction
        - (feed_rate + kill_rate) * catalyst
    )
    return new_substrate, new_catalyst


def split(value):
    high = value.astype(jnp.bfloat16)
    low = (value - high.astype(jnp.float32)).astype(jnp.bfloat16)
    return high, low


def spread_of(before, here, after):
    planes, extent = here.shape
    total = pltpu.roll(here, 1, 0) + pltpu.roll(here, planes - 1, 0)
    total = total + before + after
    total = total + pltpu.roll(here, 1, 1) + pltpu.roll(here, extent - 1, 1)
    return total - 6.0 * here


def kernel(dims, *refs):
    planes, columns, extent, owners, slabs_x = dims
    (u_ref, v_ref, u_out, v_out, gathered, loaded, state, edge, packed, got, corner, middle, sums, outgoing,
     load_sem, send_sem, recv_sem, far) = refs
    tiles, pairs, last = extent // LANES, columns // 2, owners - 1
    half = extent // 2
    portion = half // owners
    widths = (LANES, extent) if tiles > 1 else (extent,)
    dealt_to = [(width - 2) // (2 * portion) for width in widths[:-1]] + [owners]
    spans = list(zip((0,) + widths[:-1], widths))
    shares = list(zip([0] + dealt_to[:-1], dealt_to))
    parts = range(len(widths))
    gx, gy = lax.axis_index("gx"), lax.axis_index("gy")
    at_top, at_bottom = gy // last, (last - gy) // last

    barrier = pltpu.get_barrier_semaphore()
    across_of = [lax.rem(gx + shift, slabs_x) for shift in (1, slabs_x - 1)]
    along_of = [lax.rem(gy + shift, owners) for shift in (1, owners - 1)]

    def greet(semaphore, x, y):
        pl.semaphore_signal(semaphore, inc=1, device_id=(x, y), device_id_type=MESH)

    for x in across_of:
        greet(barrier, x, gy)
        greet(barrier, x, along_of[1])

    @pl.when(gy < last)
    def _():
        for x in across_of:
            greet(barrier, x, gy + 1)

    for peer in range(owners):

        @pl.when((peer > gy) | (peer == gy - 1))
        def _():
            greet(barrier, gx, peer)

    near_count = 4 + gy + (1 - at_top) + 2 * (1 - at_bottom)
    far_count = last - gy - 1 + 2 * at_bottom

    loads = [
        pltpu.make_async_copy(source, loaded.at[field], load_sem)
        for field, source in enumerate((u_ref, v_ref))
    ]
    for load in loads:
        load.start()
    pltpu.make_async_copy(loaded, loaded, load_sem).wait()

    low = 4
    high = low + columns
    lane = lax.broadcasted_iota(jnp.int32, (planes, LANES), 1)
    group = lax.rem(lane + 2, LANES) // 4
    pack = jnp.zeros((planes, LANES), jnp.float32)
    for field in range(2):
        for column in range(columns):
            slab = jnp.concatenate(
                [
                    loaded[field, pl.ds(tile * columns + column, planes, stride=tiles * columns), :]
                    for tile in range(tiles)
                ],
                axis=1,
            )
            state[field, low + column] = slab
            at = field * columns + column
            tips = jnp.where(lane < LANES // 2, slab[:, :LANES], slab[:, extent - LANES :])
            tips = pltpu.roll(tips, 4 * at, 1) if at else tips
            pack = jnp.where(group == at, tips, pack)
    packed[...] = pack

    pl.semaphore_wait(barrier, near_count)

    def send(sender, receiver, source, target, x, y):
        return pltpu.make_async_remote_copy(
            src_ref=source,
            dst_ref=target,
            send_sem=send_sem.at[sender],
            recv_sem=recv_sem.at[receiver],
            device_id=(x, y),
            device_id_type=MESH,
        )

    def wait_sent(sender, ref):
        send(sender, 0, ref, ref, gx, gy).wait_send()

    def wait_got(receiver, ref):
        send(0, receiver, ref, ref, gx, gy).wait_recv()

    def columns_of(first_column, count, part):
        return state.at[:, first_column : first_column + count, :, slice(*spans[part])]

    across = [send(0, 0, packed, got.at[side], across_of[side], gy) for side in range(2)]
    corners_up = [send(0, 1, packed, corner.at[0, side], across_of[side], along_of[0]) for side in range(2)]
    corners_down = [send(0, 2, packed, corner.at[1, side], across_of[side], along_of[1]) for side in range(2)]
    up, down, wrap = [
        [
            send(sender, receiver + 3 * part, columns_of(source, 2, part), columns_of(target, 2, part), gx, along_of[way])
            for part in parts
        ]
        for sender, receiver, source, target, way in (
            (1, 1, high - 2, low - 2, 0),
            (1, 2, low, high, 1),
            (2, 3, high - 4, low - 4, 0),
        )
    ]
    dealt_recv = 1 + 3 * len(widths)

    @pl.when(gy == last)
    def _():
        for x in across_of:
            greet(far, x, 0)

    for peer in range(owners - 2):

        @pl.when(peer < gy - 1)
        def _():
            greet(far, gx, peer)

    for copy in across + corners_up:
        copy.start()

    @pl.when(gy > 0)
    def _():
        for copy in corners_down:
            copy.start()

    for part in parts:

        @pl.when(gy < last)
        def _():
            up[part].start()

        @pl.when((gy > 0) & (gy < last))
        def _():
            down[part].start()

        @pl.when(gy == last)
        def _():
            copies = [up[part], wrap[part]]
            copies.insert(0 if part == 0 else 2, down[part])
            for copy in copies:
                copy.start()

    row = lax.broadcasted_iota(jnp.int32, (half, extent), 0)
    fine = lax.broadcasted_iota(jnp.int32, (half, extent), 1)
    to_level = jnp.where(fine // 2 == row, 0.25, 0.0).astype(jnp.bfloat16)

    wait_got(0, got)

    def merged(below, above):
        return jnp.where(lax.rem(lane, 4) < 2, above, below)

    def place(c, tips, column):
        for field in range(2):
            at = field * columns + column
            edge[field, c] = pltpu.roll(tips, LANES - 4 * at, 1) if at else tips

    both = merged(got[0], got[1])
    for column in range(columns):
        place(low + column, both, column)

    def wide(field, c, width, outer=()):
        tail = jnp.zeros((planes, LANES), jnp.float32) if c in outer else edge[field, c]
        return jnp.concatenate([state[field, c, :, :width], tail], axis=1)

    def first(c, width, outer=()):
        u, v = wide(0, c, width), wide(1, c, width)
        su = spread_of(wide(0, c - 1, width, outer), u, wide(0, c + 1, width, outer))
        sv = spread_of(wide(1, c - 1, width, outer), v, wide(1, c + 1, width, outer))
        for field, new in enumerate(react(u, v, su, sv)):
            middle[field, c, :, :width] = new[:, :width]
            middle[field, c, :, extent:] = new[:, width:]

    def half_way(field, c, width):
        return jnp.concatenate([middle[field, c, :, :width], middle[field, c, :, extent:]], axis=1)

    def second(c, width):
        u, v = half_way(0, c, width), half_way(1, c, width)
        su = spread_of(half_way(0, c - 1, width), u, half_way(0, c + 1, width))
        sv = spread_of(half_way(1, c - 1, width), v, half_way(1, c + 1, width))
        return react(u[:, :width], v[:, :width], su[:, :width], sv[:, :width])

    def pair(k, c, width=extent, own=True, slot=0):
        new = [second(c, width), second(c + 1, width)]
        for field, out in enumerate((u_out, v_out)):
            for tile in range(width // LANES):
                lanes = slice(tile * LANES, (tile + 1) * LANES)
                both_of = [new[i][field][:, lanes] for i in range(2)]
                if own:
                    for i in range(2):
                        rows = pl.ds(tile * columns + c - low + i, planes, stride=tiles * columns)
                        out[rows, :] = both_of[i]
                rows = pl.ds(field * planes * pairs + k, planes, stride=pairs)
                sums[slot, tile, rows, :] = both_of[0] + both_of[1]

    final = len(widths) - 1

    def wait_side(way, part):
        if part == 0:
            wait_got(1 + way, state.at[:, 0:3, :, :LANES])
        else:
            up[part].wait_recv() if way == 0 else down[part].wait_recv()

    def low_side(part, wrapped):
        width = widths[part]
        wait_side(0, part)
        if part == 0:
            beyond = merged(corner[0, 0], corner[0, 1])
            for step in range(1, 4 if wrapped else 2):
                place(low - step, beyond, columns - step)
        first(low, width)
        first(low - 1, width, () if wrapped else (low - 2,))
        pair(0, low, width, own=part == final)

    def high_side(part):
        width = widths[part]
        wait_side(1, part)
        if part == 0:
            place(high, merged(corner[1, 0], corner[1, 1]), 0)
        first(high - 1, width)
        first(high, width, (high + 1,))
        pair(pairs - 1, high - 2, width, own=part == final)

    def level_of(part, slots):
        width = widths[part]
        contract = (((1,), (1,)), ((), ()))
        taking = to_level[: width // 2, :width]
        values = jnp.concatenate(
            [jnp.concatenate([sums[slot, tile] for tile in range(width // LANES)], axis=1) for slot in range(slots)],
            axis=0,
        )
        upper, lower = split(values)
        level = lax.dot_general(taking, upper, contract, preferred_element_type=jnp.float32)
        level += lax.dot_general(taking, lower, contract, preferred_element_type=jnp.float32)
        size = sums.shape[2]
        for owner in range(*shares[part]):
            for slot in range(slots):
                outgoing[slot, owner] = level[
                    owner * portion : (owner + 1) * portion, slot * size : (slot + 1) * size
                ]

    def deal(slot, owner):
        target = owners if slot else gy
        return send(3 + slot, dealt_recv, outgoing.at[slot, owner], gathered.at[target], gx, owner)

    for c in range(low + 1, high - 1):
        first(c, extent)
    for k in range(1, pairs - 1):
        pair(k, low + 2 * k)

    for part in parts:

        @pl.when(gy > 0)
        def _():
            low_side(part, False)

        @pl.when(gy < last)
        def _():
            high_side(part)

        if part == 0:

            @pl.when(gy < last - 1)
            def _():
                pl.semaphore_wait(far, far_count)

        @pl.when(gy == 0)
        def _():
            if part == 0:
                for copy in corners_down + down:
                    copy.start()
            low_side(part, True)

            wrap[part].wait_recv()
            width = widths[part]
            first(low - 2, width)
            first(low - 3, width, (low - 4,))
            pair(pairs - 1, low - 2, width, own=False, slot=1)
            level_of(part, 2)
            for owner in range(*shares[part]):
                if owner:
                    deal(0, owner).start()
                    deal(1, owner).start()

        @pl.when(gy > 0)
        def _():
            level_of(part, 1)
            for owner in range(*shares[part]):

                @pl.when(owner != gy)
                def _():
                    deal(0, owner).start()

    gathered[gy] = outgoing[0, gy]

    @pl.when(gy == last)
    def _():
        for part in parts[:-1]:
            wait_side(1, part)
            if part == 0:
                place(high, merged(corner[1, 0], corner[1, 1]), 0)
        wait_side(1, final)
        if final == 0:
            place(high, merged(corner[1, 0], corner[1, 1]), 0)
        first(high - 1, extent)
        first(high, extent, (high + 1,))
        pair(pairs - 1, high - 2)

    @pl.when(gy == 0)
    def _():
        gathered[owners] = outgoing[1, 0]
        wait_got(dealt_recv, gathered.at[1:owners])
        wait_sent(4, outgoing.at[1, 1:])

    @pl.when(gy > 0)
    def _():
        wait_got(dealt_recv, gathered.at[:owners])

    wait_sent(0, state.at[:, 0:3, :, :LANES])
    wait_sent(1, state.at[:, 0:4])
    wait_sent(3, outgoing.at[0, 1:])

    @pl.when(gy == last)
    def _():
        wait_sent(2, state.at[:, 0:2])


def finish(u_ref, v_ref, dealt, u_out, v_out, rebuilt_out, doubled, paired, rebuilt, sems):
    copies = [
        pltpu.make_async_copy(u_ref, u_out, sems.at[0]),
        pltpu.make_async_copy(v_ref, v_out, sems.at[1]),
    ]
    for copy in copies:
        copy.start()

    owners, portion = dealt.shape[0] - 1, dealt.shape[1]
    wide_in = lax.broadcasted_iota(jnp.int32, (LANES, 4 * LANES), 0)
    wide_out = lax.broadcasted_iota(jnp.int32, (LANES, 4 * LANES), 1)
    column_of = wide_in // 16 * 4 + wide_in % 4
    plane = wide_in // 4 % 4 == wide_out // LANES
    spreading = jnp.concatenate(
        [
            jnp.where(plane & (column_of == wide_out % LANES // 2), 0.5, 0.0),
            jnp.where(plane & (column_of // 2 == wide_out % LANES // 4), 0.125, 0.0),
        ],
        axis=0,
    ).astype(jnp.bfloat16)
    lane = lax.broadcasted_iota(jnp.int32, (portion, LANES), 1)
    even = lax.broadcasted_iota(jnp.int32, (portion, LANES), 0) % 2 == 0
    blocks = [dealt[owner] for owner in range(owners)]
    blocks[-1] = jnp.where(lane % 4 == 3, dealt[owners], blocks[-1])
    width, rows = rebuilt.shape[1], 2 * portion
    chunks = 4
    share = 8 // chunks
    for chunk in range(chunks):
        for h in range(chunk * share, (chunk + 1) * share):
            part = jnp.zeros((portion, LANES), jnp.float32)
            for owner in range(8):
                shift = (16 * (owner - h)) % LANES
                moved = pltpu.roll(blocks[owner], shift, 1) if shift else blocks[owner]
                part = jnp.where(lane // 16 == owner, moved, part)
            other = jnp.where(even, pltpu.roll(part, portion - 1, 0), pltpu.roll(part, 1, 0))
            total = part + other
            for twin in range(2):
                doubled[pl.ds(h * rows + twin, portion, stride=2), :] = part
                paired[pl.ds(h * rows + twin, portion, stride=2), :] = total
        span = slice(chunk * share * rows, (chunk + 1) * share * rows)
        high, low = split(jnp.concatenate([doubled[span, :], paired[span, :]], axis=1))
        whole = jnp.dot(high, spreading, preferred_element_type=jnp.float32)
        whole += jnp.dot(low, spreading, preferred_element_type=jnp.float32)
        for h in range(share):
            for z in range(4):
                base = ((chunk * share + h) * 4 + z) * rows
                rebuilt[base : base + rows, :] = whole[
                    h * rows : (h + 1) * rows, z * LANES : z * LANES + width
                ]
        size = share * 4 * rows
        copies.append(
            pltpu.make_async_copy(
                rebuilt.at[chunk * size : (chunk + 1) * size],
                rebuilt_out.at[chunk * size : (chunk + 1) * size],
                sems.at[2],
            )
        )
        copies[-1].start()
    for copy in copies[:2] + [pltpu.make_async_copy(rebuilt, rebuilt_out, sems.at[2])]:
        copy.wait()


def tiled(field):
    planes, columns, extent = field.shape
    field = field.reshape(planes, columns, extent // LANES, LANES)
    return jnp.transpose(field, (0, 2, 1, 3)).reshape(-1, LANES)


def untiled(field, shape):
    planes, columns, extent = shape
    field = field.reshape(planes, extent // LANES, columns, LANES)
    return jnp.transpose(field, (0, 2, 1, 3)).reshape(shape)


def body(substrate, catalyst):
    planes, columns, extent = substrate.shape
    slabs_x, owners = lax.axis_size("gx"), lax.axis_size("gy")
    half, pairs, tiles = extent // 2, columns // 2, extent // LANES
    portion = half // owners
    values = 2 * planes * pairs
    fused = (
        planes == 16 and pairs == 4 and owners == 8 and values == LANES and portion % 8 == 0
    )
    dims = (planes, columns, extent, owners, slabs_x)
    f32 = jnp.float32
    flat = (planes * tiles * columns, LANES)
    vmem = pl.BlockSpec(memory_space=pltpu.VMEM)
    anywhere = pl.BlockSpec(memory_space=pl.ANY)
    u, v, dealt = pl.pallas_call(
        functools.partial(kernel, dims),
        out_shape=(
            pltpu.VMEM(flat, f32),
            pltpu.VMEM(flat, f32),
            pltpu.VMEM((owners + 1, portion, values), f32),
        ),
        in_specs=[anywhere] * 2,
        out_specs=(vmem,) * 3,
        scratch_shapes=[
            pltpu.VMEM((2,) + flat, f32),
            pltpu.VMEM((2, columns + 6, planes, extent), f32),
            pltpu.VMEM((2, columns + 6, planes, LANES), f32),
            pltpu.VMEM((planes, LANES), f32),
            pltpu.VMEM((2, planes, LANES), f32),
            pltpu.VMEM((2, 2, planes, LANES), f32),
            pltpu.VMEM((2, columns + 6, planes, extent + LANES), f32),
            pltpu.VMEM((2, tiles, values, LANES), f32),
            pltpu.VMEM((2, owners, portion, values), f32),
            pltpu.SemaphoreType.DMA,
            pltpu.SemaphoreType.DMA((5,)),
            pltpu.SemaphoreType.DMA((8 if tiles > 1 else 5,)),
            pltpu.SemaphoreType.REGULAR,
        ],
        compiler_params=pltpu.CompilerParams(collective_id=0, has_side_effects=True),
    )(tiled(substrate), tiled(catalyst))
    rows, width = 2 * portion, columns * owners
    if fused:
        u, v, dealt = (
            pltpu.with_memory_space_constraint(x, pltpu.VMEM) for x in (u, v, dealt)
        )
        u, v, rebuilt = pl.pallas_call(
            finish,
            out_shape=(
                jax.ShapeDtypeStruct(flat, f32),
                jax.ShapeDtypeStruct(flat, f32),
                jax.ShapeDtypeStruct((2 * planes * rows, width), f32),
            ),
            in_specs=[vmem] * 3,
            out_specs=(anywhere,) * 3,
            scratch_shapes=[
                pltpu.VMEM((8 * rows, LANES), f32),
                pltpu.VMEM((8 * rows, LANES), f32),
                pltpu.VMEM((2 * planes * rows, width), f32),
                pltpu.SemaphoreType.DMA((3,)),
            ],
        )(u, v, dealt)
        rebuilt = rebuilt.reshape(2, planes, rows, width)
    else:
        level = dealt.reshape(owners + 1, portion, 2, planes, pairs)
        latest = jnp.concatenate([level[owners - 1, ..., :-1], level[owners, ..., -1:]], axis=-1)
        level = jnp.concatenate([level[: owners - 1], latest[None]], axis=0)
        level = jnp.transpose(level, (2, 3, 1, 0, 4)).reshape(2, planes, portion // 2, 2, columns * owners // 4, 2)
        coarse = 0.25 * jnp.sum(level, axis=(3, 5), keepdims=True)
        blend = (coarse + 0.5 * (level - coarse)).reshape(2, planes, portion, columns * owners // 2)
        rebuilt = jnp.repeat(jnp.repeat(blend, 2, axis=2), 2, axis=3)
    return untiled(u, substrate.shape), untiled(v, substrate.shape), rebuilt


def solution(mesh):
    in_specs = (P(None, "gy", "gx"), P(None, "gy", "gx"))
    out_specs = (P(None, "gy", "gx"), P(None, "gy", "gx"), P(None, None, ("gx", "gy"), None))
    return jax.shard_map(body, mesh=mesh, in_specs=in_specs, out_specs=out_specs, check_vma=False)
```

```python
import functools

import jax
import jax.numpy as jnp
from jax import lax
from jax.experimental import pallas as pl
from jax.experimental.pallas import tpu as pltpu
from jax.sharding import PartitionSpec as P

feed_rate = 0.037
kill_rate = 0.06
substrate_diffusion = 0.15
catalyst_diffusion = 0.08

MESH = pl.DeviceIdType.MESH
LANES = 128


def react(substrate, catalyst, spread_substrate, spread_catalyst):
    reaction = substrate * catalyst * catalyst
    new_substrate = (
        substrate
        + substrate_diffusion * spread_substrate
        - reaction
        + feed_rate * (1.0 - substrate)
    )
    new_catalyst = (
        catalyst
        + catalyst_diffusion * spread_catalyst
        + reaction
        - (feed_rate + kill_rate) * catalyst
    )
    return new_substrate, new_catalyst


def split(value):
    high = value.astype(jnp.bfloat16)
    low = (value - high.astype(jnp.float32)).astype(jnp.bfloat16)
    return high, low


def spread_of(before, here, after):
    planes, extent = here.shape
    total = pltpu.roll(here, 1, 0) + pltpu.roll(here, planes - 1, 0)
    total = total + before + after
    total = total + pltpu.roll(here, 1, 1) + pltpu.roll(here, extent - 1, 1)
    return total - 6.0 * here


def kernel(dims, *refs):
    planes, columns, extent, owners, slabs_x = dims
    (u_ref, v_ref, u_out, v_out, gathered, loaded, state, edge, packed, folded, got, corner, middle, sums, outgoing,
     load_sem, send_sem, recv_sem, far) = refs
    tiles, pairs, last = extent // LANES, columns // 2, owners - 1
    half = extent // 2
    portion = half // owners
    widths = (LANES, extent) if tiles > 1 else (extent,)
    dealt_to = [(width - 2) // (2 * portion) for width in widths[:-1]] + [owners]
    spans = list(zip((0,) + widths[:-1], widths))
    shares = list(zip([0] + dealt_to[:-1], dealt_to))
    parts = range(len(widths))
    gx, gy = lax.axis_index("gx"), lax.axis_index("gy")
    at_top, at_bottom = gy // last, (last - gy) // last

    barrier = pltpu.get_barrier_semaphore()
    across_of = [lax.rem(gx + shift, slabs_x) for shift in (1, slabs_x - 1)]
    along_of = [lax.rem(gy + shift, owners) for shift in (1, owners - 1)]

    def greet(semaphore, x, y):
        pl.semaphore_signal(semaphore, inc=1, device_id=(x, y), device_id_type=MESH)

    for x in across_of:
        greet(barrier, x, gy)
        greet(barrier, x, along_of[1])

    @pl.when(gy < last)
    def _():
        for x in across_of:
            greet(barrier, x, gy + 1)

    for peer in range(owners):

        @pl.when((peer > gy) | (peer == gy - 1))
        def _():
            greet(barrier, gx, peer)

    near_count = 4 + gy + (1 - at_top) + 2 * (1 - at_bottom)
    far_count = last - gy - 1 + 2 * at_bottom

    loads = [
        pltpu.make_async_copy(source, loaded.at[field], load_sem)
        for field, source in enumerate((u_ref, v_ref))
    ]
    for load in loads:
        load.start()
    pltpu.make_async_copy(loaded, loaded, load_sem).wait()

    low = 4
    high = low + columns
    lane = lax.broadcasted_iota(jnp.int32, (planes, LANES), 1)
    group = lax.rem(lane + 2, LANES) // 4
    pack = jnp.zeros((planes, LANES), jnp.float32)
    for field in range(2):
        for column in range(columns):
            slab = jnp.concatenate(
                [
                    loaded[field, pl.ds(tile * columns + column, planes, stride=tiles * columns), :]
                    for tile in range(tiles)
                ],
                axis=1,
            )
            state[field, low + column] = slab
            at = field * columns + column
            tips = jnp.where(lane < LANES // 2, slab[:, :LANES], slab[:, extent - LANES :])
            tips = pltpu.roll(tips, 4 * at, 1) if at else tips
            pack = jnp.where(group == at, tips, pack)
    packed[...] = pack
    fold = planes // 2
    narrow = lax.broadcasted_iota(jnp.int32, (fold, LANES), 1)
    near_half = lax.rem(narrow + 2, LANES) < LANES // 2
    folded[...] = jnp.where(near_half, pack[:fold], pltpu.roll(pack[fold:], LANES // 2, 1))

    pl.semaphore_wait(barrier, near_count)

    def send(sender, receiver, source, target, x, y):
        return pltpu.make_async_remote_copy(
            src_ref=source,
            dst_ref=target,
            send_sem=send_sem.at[sender],
            recv_sem=recv_sem.at[receiver],
            device_id=(x, y),
            device_id_type=MESH,
        )

    def wait_sent(sender, ref):
        send(sender, 0, ref, ref, gx, gy).wait_send()

    def wait_got(receiver, ref):
        send(0, receiver, ref, ref, gx, gy).wait_recv()

    def columns_of(first_column, count, part):
        return state.at[:, first_column : first_column + count, :, slice(*spans[part])]

    across = [send(0, 0, packed, got.at[side], across_of[side], gy) for side in range(2)]
    corners_up = [send(0, 1, folded, corner.at[0, side], across_of[side], along_of[0]) for side in range(2)]
    corners_down = [send(0, 2, folded, corner.at[1, side], across_of[side], along_of[1]) for side in range(2)]
    up, down, wrap = [
        [
            send(sender, receiver + 3 * part, columns_of(source, 2, part), columns_of(target, 2, part), gx, along_of[way])
            for part in parts
        ]
        for sender, receiver, source, target, way in (
            (1, 1, high - 2, low - 2, 0),
            (1, 2, low, high, 1),
            (2, 3, high - 4, low - 4, 0),
        )
    ]
    dealt_recv = 1 + 3 * len(widths)

    @pl.when(gy == last)
    def _():
        for x in across_of:
            greet(far, x, 0)

    for peer in range(owners - 2):

        @pl.when(peer < gy - 1)
        def _():
            greet(far, gx, peer)

    for copy in across + corners_up:
        copy.start()

    @pl.when(gy > 0)
    def _():
        for copy in corners_down:
            copy.start()

    def start_columns(part):
        @pl.when(gy < last)
        def _():
            up[part].start()

        @pl.when(gy > 0)
        def _():
            down[part].start()

    start_columns(0)

    @pl.when(gy == last)
    def _():
        for part in parts:
            up[part].start()
            wrap[part].start()

    row = lax.broadcasted_iota(jnp.int32, (half, extent), 0)
    fine = lax.broadcasted_iota(jnp.int32, (half, extent), 1)
    to_level = jnp.where(fine // 2 == row, 0.25, 0.0).astype(jnp.bfloat16)

    wait_got(0, got)
    for part in parts[1:]:
        start_columns(part)

    def merged(below, above):
        return jnp.where(lax.rem(lane[: below.shape[0]], 4) < 2, above, below)

    def unfolded(way):
        tips = merged(corner[way, 0], corner[way, 1])
        return jnp.concatenate([tips, pltpu.roll(tips, LANES // 2, 1)], axis=0)

    def place(c, tips, column):
        for field in range(2):
            at = field * columns + column
            edge[field, c] = pltpu.roll(tips, LANES - 4 * at, 1) if at else tips

    both = merged(got[0], got[1])
    for column in range(columns):
        place(low + column, both, column)

    def wide(field, c, width, outer=()):
        tail = jnp.zeros((planes, LANES), jnp.float32) if c in outer else edge[field, c]
        return jnp.concatenate([state[field, c, :, :width], tail], axis=1)

    def first(c, width, outer=()):
        u, v = wide(0, c, width), wide(1, c, width)
        su = spread_of(wide(0, c - 1, width, outer), u, wide(0, c + 1, width, outer))
        sv = spread_of(wide(1, c - 1, width, outer), v, wide(1, c + 1, width, outer))
        for field, new in enumerate(react(u, v, su, sv)):
            middle[field, c, :, :width] = new[:, :width]
            middle[field, c, :, extent:] = new[:, width:]

    def half_way(field, c, width):
        return jnp.concatenate([middle[field, c, :, :width], middle[field, c, :, extent:]], axis=1)

    def second(c, width):
        u, v = half_way(0, c, width), half_way(1, c, width)
        su = spread_of(half_way(0, c - 1, width), u, half_way(0, c + 1, width))
        sv = spread_of(half_way(1, c - 1, width), v, half_way(1, c + 1, width))
        return react(u[:, :width], v[:, :width], su[:, :width], sv[:, :width])

    def pair(k, c, width=extent, own=True, slot=0):
        new = [second(c, width), second(c + 1, width)]
        for field, out in enumerate((u_out, v_out)):
            for tile in range(width // LANES):
                lanes = slice(tile * LANES, (tile + 1) * LANES)
                both_of = [new[i][field][:, lanes] for i in range(2)]
                if own:
                    for i in range(2):
                        rows = pl.ds(tile * columns + c - low + i, planes, stride=tiles * columns)
                        out[rows, :] = both_of[i]
                rows = pl.ds(field * planes * pairs + k, planes, stride=pairs)
                sums[slot, tile, rows, :] = both_of[0] + both_of[1]

    final = len(widths) - 1

    def wait_side(way, part):
        if part == 0:
            wait_got(1 + way, state.at[:, 0:5, :fold, :LANES])
        else:
            up[part].wait_recv() if way == 0 else down[part].wait_recv()

    def low_side(part, wrapped):
        width = widths[part]
        wait_side(0, part)
        if part == 0:
            beyond = unfolded(0)
            for step in range(1, 4 if wrapped else 2):
                place(low - step, beyond, columns - step)
        first(low, width)
        first(low - 1, width, () if wrapped else (low - 2,))
        pair(0, low, width, own=part == final, slot=1 if wrapped else 0)

    def high_side(part):
        width = widths[part]
        wait_side(1, part)
        if part == 0:
            place(high, unfolded(1), 0)
        first(high - 1, width)
        first(high, width, (high + 1,))
        pair(pairs - 1, high - 2, width, own=part == final)

    def level_of(part, slot):
        width = widths[part]
        contract = (((1,), (1,)), ((), ()))
        taking = to_level[: width // 2, :width]
        upper, lower = split(jnp.concatenate([sums[slot, tile] for tile in range(width // LANES)], axis=1))
        level = lax.dot_general(taking, upper, contract, preferred_element_type=jnp.float32)
        level += lax.dot_general(taking, lower, contract, preferred_element_type=jnp.float32)
        for owner in range(*shares[part]):
            outgoing[slot, owner] = level[owner * portion : (owner + 1) * portion]

    def deal(slot, owner):
        target = owners if slot else gy
        return send(3 + slot, dealt_recv, outgoing.at[slot, owner], gathered.at[target], gx, owner)

    for c in range(low + 1, high - 1):
        first(c, extent)
    for k in range(1, pairs - 1):
        pair(k, low + 2 * k)

    for part in parts:

        @pl.when(gy > 0)
        def _():
            low_side(part, False)

        @pl.when(gy < last)
        def _():
            high_side(part)

        if part == 0:

            @pl.when(gy < last - 1)
            def _():
                pl.semaphore_wait(far, far_count)

        if part == 0:

            @pl.when(gy == 0)
            def _():
                for copy in corners_down + down:
                    copy.start()

        level_of(part, 0)
        for owner in range(*shares[part]):

            @pl.when(owner != gy)
            def _():
                deal(0, owner).start()

    @pl.when(gy == 0)
    def _():
        for part in parts:
            low_side(part, True)
            wrap[part].wait_recv()
            width = widths[part]
            first(low - 2, width)
            first(low - 3, width, (low - 4,))
            pair(pairs - 1, low - 2, width, own=False, slot=1)
            level_of(part, 1)
            for owner in range(*shares[part]):
                if owner:
                    deal(1, owner).start()

    gathered[gy] = outgoing[0, gy]

    @pl.when(gy == last)
    def _():
        for part in parts[:-1]:
            wait_side(1, part)
            if part == 0:
                place(high, unfolded(1), 0)
        wait_side(1, final)
        if final == 0:
            place(high, unfolded(1), 0)
        first(high - 1, extent)
        first(high, extent, (high + 1,))
        pair(pairs - 1, high - 2)

    @pl.when(gy == 0)
    def _():
        gathered[owners] = outgoing[1, 0]
        wait_got(dealt_recv, gathered.at[1:owners])
        wait_sent(4, outgoing.at[1, 1:])

    @pl.when(gy > 0)
    def _():
        wait_got(dealt_recv, gathered.at[:owners])

    wait_sent(0, state.at[:, 0:2, :, :LANES])
    wait_sent(1, state.at[:, 0:4])
    wait_sent(3, outgoing.at[0, 1:])

    @pl.when(gy == last)
    def _():
        wait_sent(2, state.at[:, 0:2])


def finish(u_ref, v_ref, dealt, u_out, v_out, rebuilt_out, doubled, paired, rebuilt, sems):
    copies = [
        pltpu.make_async_copy(u_ref, u_out, sems.at[0]),
        pltpu.make_async_copy(v_ref, v_out, sems.at[1]),
    ]
    for copy in copies:
        copy.start()

    owners, portion = dealt.shape[0] - 1, dealt.shape[1]
    wide_in = lax.broadcasted_iota(jnp.int32, (LANES, 4 * LANES), 0)
    wide_out = lax.broadcasted_iota(jnp.int32, (LANES, 4 * LANES), 1)
    column_of = wide_in // 16 * 4 + wide_in % 4
    plane = wide_in // 4 % 4 == wide_out // LANES
    spreading = jnp.concatenate(
        [
            jnp.where(plane & (column_of == wide_out % LANES // 2), 0.5, 0.0),
            jnp.where(plane & (column_of // 2 == wide_out % LANES // 4), 0.125, 0.0),
        ],
        axis=0,
    ).astype(jnp.bfloat16)
    lane = lax.broadcasted_iota(jnp.int32, (portion, LANES), 1)
    even = lax.broadcasted_iota(jnp.int32, (portion, LANES), 0) % 2 == 0
    blocks = [dealt[owner] for owner in range(owners)]
    blocks[0] = jnp.where(lane % 4 == 0, dealt[owners], blocks[0])
    blocks[-1] = jnp.where(lane % 4 == 3, dealt[owners], blocks[-1])
    width, rows = rebuilt.shape[1], 2 * portion
    chunks = 4
    share = 8 // chunks
    for chunk in range(chunks):
        for h in range(chunk * share, (chunk + 1) * share):
            part = jnp.zeros((portion, LANES), jnp.float32)
            for owner in range(8):
                shift = (16 * (owner - h)) % LANES
                moved = pltpu.roll(blocks[owner], shift, 1) if shift else blocks[owner]
                part = jnp.where(lane // 16 == owner, moved, part)
            other = jnp.where(even, pltpu.roll(part, portion - 1, 0), pltpu.roll(part, 1, 0))
            total = part + other
            for twin in range(2):
                doubled[pl.ds(h * rows + twin, portion, stride=2), :] = part
                paired[pl.ds(h * rows + twin, portion, stride=2), :] = total
        span = slice(chunk * share * rows, (chunk + 1) * share * rows)
        high, low = split(jnp.concatenate([doubled[span, :], paired[span, :]], axis=1))
        whole = jnp.dot(high, spreading, preferred_element_type=jnp.float32)
        whole += jnp.dot(low, spreading, preferred_element_type=jnp.float32)
        for h in range(share):
            for z in range(4):
                base = ((chunk * share + h) * 4 + z) * rows
                rebuilt[base : base + rows, :] = whole[
                    h * rows : (h + 1) * rows, z * LANES : z * LANES + width
                ]
        size = share * 4 * rows
        copies.append(
            pltpu.make_async_copy(
                rebuilt.at[chunk * size : (chunk + 1) * size],
                rebuilt_out.at[chunk * size : (chunk + 1) * size],
                sems.at[2],
            )
        )
        copies[-1].start()
    for copy in copies[:2] + [pltpu.make_async_copy(rebuilt, rebuilt_out, sems.at[2])]:
        copy.wait()


def tiled(field):
    planes, columns, extent = field.shape
    field = field.reshape(planes, columns, extent // LANES, LANES)
    return jnp.transpose(field, (0, 2, 1, 3)).reshape(-1, LANES)


def untiled(field, shape):
    planes, columns, extent = shape
    field = field.reshape(planes, extent // LANES, columns, LANES)
    return jnp.transpose(field, (0, 2, 1, 3)).reshape(shape)


def body(substrate, catalyst):
    planes, columns, extent = substrate.shape
    slabs_x, owners = lax.axis_size("gx"), lax.axis_size("gy")
    half, pairs, tiles = extent // 2, columns // 2, extent // LANES
    portion = half // owners
    values = 2 * planes * pairs
    fused = (
        planes == 16 and pairs == 4 and owners == 8 and values == LANES and portion % 8 == 0
    )
    dims = (planes, columns, extent, owners, slabs_x)
    f32 = jnp.float32
    flat = (planes * tiles * columns, LANES)
    vmem = pl.BlockSpec(memory_space=pltpu.VMEM)
    anywhere = pl.BlockSpec(memory_space=pl.ANY)
    u, v, dealt = pl.pallas_call(
        functools.partial(kernel, dims),
        out_shape=(
            pltpu.VMEM(flat, f32),
            pltpu.VMEM(flat, f32),
            pltpu.VMEM((owners + 1, portion, values), f32),
        ),
        in_specs=[anywhere] * 2,
        out_specs=(vmem,) * 3,
        scratch_shapes=[
            pltpu.VMEM((2,) + flat, f32),
            pltpu.VMEM((2, columns + 6, planes, extent), f32),
            pltpu.VMEM((2, columns + 6, planes, LANES), f32),
            pltpu.VMEM((planes, LANES), f32),
            pltpu.VMEM((planes // 2, LANES), f32),
            pltpu.VMEM((2, planes, LANES), f32),
            pltpu.VMEM((2, 2, planes // 2, LANES), f32),
            pltpu.VMEM((2, columns + 6, planes, extent + LANES), f32),
            pltpu.VMEM((2, tiles, values, LANES), f32),
            pltpu.VMEM((2, owners, portion, values), f32),
            pltpu.SemaphoreType.DMA,
            pltpu.SemaphoreType.DMA((5,)),
            pltpu.SemaphoreType.DMA((8 if tiles > 1 else 5,)),
            pltpu.SemaphoreType.REGULAR,
        ],
        compiler_params=pltpu.CompilerParams(collective_id=0, has_side_effects=True),
    )(tiled(substrate), tiled(catalyst))
    rows, width = 2 * portion, columns * owners
    if fused:
        u, v, dealt = (
            pltpu.with_memory_space_constraint(x, pltpu.VMEM) for x in (u, v, dealt)
        )
        u, v, rebuilt = pl.pallas_call(
            finish,
            out_shape=(
                jax.ShapeDtypeStruct(flat, f32),
                jax.ShapeDtypeStruct(flat, f32),
                jax.ShapeDtypeStruct((2 * planes * rows, width), f32),
            ),
            in_specs=[vmem] * 3,
            out_specs=(anywhere,) * 3,
            scratch_shapes=[
                pltpu.VMEM((8 * rows, LANES), f32),
                pltpu.VMEM((8 * rows, LANES), f32),
                pltpu.VMEM((2 * planes * rows, width), f32),
                pltpu.SemaphoreType.DMA((3,)),
            ],
        )(u, v, dealt)
        rebuilt = rebuilt.reshape(2, planes, rows, width)
    else:
        level = dealt.reshape(owners + 1, portion, 2, planes, pairs)
        outer = level[owners]
        lowest = jnp.concatenate([outer[..., :1], level[0, ..., 1:]], axis=-1)
        highest = jnp.concatenate([level[owners - 1, ..., :-1], outer[..., -1:]], axis=-1)
        level = jnp.concatenate([lowest[None], level[1 : owners - 1], highest[None]], axis=0)
        level = jnp.transpose(level, (2, 3, 1, 0, 4)).reshape(2, planes, portion // 2, 2, columns * owners // 4, 2)
        coarse = 0.25 * jnp.sum(level, axis=(3, 5), keepdims=True)
        blend = (coarse + 0.5 * (level - coarse)).reshape(2, planes, portion, columns * owners // 2)
        rebuilt = jnp.repeat(jnp.repeat(blend, 2, axis=2), 2, axis=3)
    return untiled(u, substrate.shape), untiled(v, substrate.shape), rebuilt


def solution(mesh):
    in_specs = (P(None, "gy", "gx"), P(None, "gy", "gx"))
    out_specs = (P(None, "gy", "gx"), P(None, "gy", "gx"), P(None, None, ("gx", "gy"), None))
    return jax.shard_map(body, mesh=mesh, in_specs=in_specs, out_specs=out_specs, check_vma=False)
```

```python
import functools

import jax
import jax.numpy as jnp
from jax import lax
from jax.experimental import pallas as pl
from jax.experimental.pallas import tpu as pltpu
from jax.sharding import PartitionSpec as P

feed_rate = 0.037
kill_rate = 0.06
substrate_diffusion = 0.15
catalyst_diffusion = 0.08

MESH = pl.DeviceIdType.MESH
LANES = 128


def react(substrate, catalyst, spread_substrate, spread_catalyst):
    reaction = substrate * catalyst * catalyst
    new_substrate = (
        substrate
        + substrate_diffusion * spread_substrate
        - reaction
        + feed_rate * (1.0 - substrate)
    )
    new_catalyst = (
        catalyst
        + catalyst_diffusion * spread_catalyst
        + reaction
        - (feed_rate + kill_rate) * catalyst
    )
    return new_substrate, new_catalyst


def split(value):
    high = value.astype(jnp.bfloat16)
    low = (value - high.astype(jnp.float32)).astype(jnp.bfloat16)
    return high, low


def spread_of(before, here, after):
    planes, extent = here.shape
    total = pltpu.roll(here, 1, 0) + pltpu.roll(here, planes - 1, 0)
    total = total + before + after
    total = total + pltpu.roll(here, 1, 1) + pltpu.roll(here, extent - 1, 1)
    return total - 6.0 * here


def kernel(dims, *refs):
    planes, columns, extent, owners, slabs_x = dims
    (u_ref, v_ref, u_out, v_out, gathered, loaded, state, edge, packed, folded, got, corner, middle, sums, outgoing,
     load_sem, send_sem, recv_sem, far) = refs
    tiles, pairs, last = extent // LANES, columns // 2, owners - 1
    half = extent // 2
    portion = half // owners
    widths = (LANES, extent) if tiles > 1 else (extent,)
    dealt_to = [(width - 2) // (2 * portion) for width in widths[:-1]] + [owners]
    spans = list(zip((0,) + widths[:-1], widths))
    shares = list(zip([0] + dealt_to[:-1], dealt_to))
    parts = range(len(widths))
    gx, gy = lax.axis_index("gx"), lax.axis_index("gy")
    at_top, at_bottom = gy // last, (last - gy) // last

    barrier = pltpu.get_barrier_semaphore()
    across_of = [lax.rem(gx + shift, slabs_x) for shift in (1, slabs_x - 1)]
    along_of = [lax.rem(gy + shift, owners) for shift in (1, owners - 1)]

    def greet(semaphore, x, y):
        pl.semaphore_signal(semaphore, inc=1, device_id=(x, y), device_id_type=MESH)

    for x in across_of:
        greet(barrier, x, gy)
        greet(barrier, x, along_of[1])

    @pl.when(gy < last)
    def _():
        for x in across_of:
            greet(barrier, x, gy + 1)

    for peer in range(owners):

        @pl.when((peer > gy) | (peer == gy - 1))
        def _():
            greet(barrier, gx, peer)

    near_count = 4 + gy + (1 - at_top) + 2 * (1 - at_bottom)
    far_count = last - gy - 1 + 2 * at_bottom

    loads = [
        pltpu.make_async_copy(source, loaded.at[field], load_sem)
        for field, source in enumerate((u_ref, v_ref))
    ]
    for load in loads:
        load.start()
    pltpu.make_async_copy(loaded, loaded, load_sem).wait()

    low = 4
    high = low + columns
    lane = lax.broadcasted_iota(jnp.int32, (planes, LANES), 1)
    group = lax.rem(lane + 2, LANES) // 4
    pack = jnp.zeros((planes, LANES), jnp.float32)
    for field in range(2):
        for column in range(columns):
            slab = jnp.concatenate(
                [
                    loaded[field, pl.ds(tile * columns + column, planes, stride=tiles * columns), :]
                    for tile in range(tiles)
                ],
                axis=1,
            )
            state[field, low + column] = slab
            at = field * columns + column
            tips = jnp.where(lane < LANES // 2, slab[:, :LANES], slab[:, extent - LANES :])
            tips = pltpu.roll(tips, 4 * at, 1) if at else tips
            pack = jnp.where(group == at, tips, pack)
    packed[...] = pack
    fold = planes // 2
    narrow = lax.broadcasted_iota(jnp.int32, (fold, LANES), 1)
    near_half = lax.rem(narrow + 2, LANES) < LANES // 2
    folded[...] = jnp.where(near_half, pack[:fold], pltpu.roll(pack[fold:], LANES // 2, 1))

    pl.semaphore_wait(barrier, near_count)

    def send(sender, receiver, source, target, x, y):
        return pltpu.make_async_remote_copy(
            src_ref=source,
            dst_ref=target,
            send_sem=send_sem.at[sender],
            recv_sem=recv_sem.at[receiver],
            device_id=(x, y),
            device_id_type=MESH,
        )

    def wait_sent(sender, ref):
        send(sender, 0, ref, ref, gx, gy).wait_send()

    def wait_got(receiver, ref):
        send(0, receiver, ref, ref, gx, gy).wait_recv()

    def columns_of(first_column, count, part):
        return state.at[:, first_column : first_column + count, :, slice(*spans[part])]

    across = [send(0, 0, packed, got.at[side], across_of[side], gy) for side in range(2)]
    corners_up = [send(0, 1, folded, corner.at[0, side], across_of[side], along_of[0]) for side in range(2)]
    corners_down = [send(0, 2, folded, corner.at[1, side], across_of[side], along_of[1]) for side in range(2)]
    up, down, wrap = [
        [
            send(sender, receiver + 3 * part, columns_of(source, 2, part), columns_of(target, 2, part), gx, along_of[way])
            for part in parts
        ]
        for sender, receiver, source, target, way in (
            (1, 1, high - 2, low - 2, 0),
            (1, 2, low, high, 1),
            (2, 3, high - 4, low - 4, 0),
        )
    ]
    dealt_recv = 1 + 3 * len(widths)

    @pl.when(gy == last)
    def _():
        for x in across_of:
            greet(far, x, 0)

    for peer in range(owners - 2):

        @pl.when(peer < gy - 1)
        def _():
            greet(far, gx, peer)

    for copy in across + corners_up:
        copy.start()

    @pl.when(gy > 0)
    def _():
        for copy in corners_down:
            copy.start()

    @pl.when(gy < last)
    def _():
        up[0].start()

    @pl.when(gy > 0)
    def _():
        down[0].start()

    @pl.when((gy > 0) & (gy < last))
    def _():
        for part in parts[1:]:
            down[part].start()

    @pl.when(gy == last)
    def _():
        for part in parts:
            up[part].start()
            wrap[part].start()

    row = lax.broadcasted_iota(jnp.int32, (half, extent), 0)
    fine = lax.broadcasted_iota(jnp.int32, (half, extent), 1)
    to_level = jnp.where(fine // 2 == row, 0.25, 0.0).astype(jnp.bfloat16)

    wait_got(0, got)
    for part in parts[1:]:

        @pl.when(gy < last)
        def _():
            up[part].start()

        @pl.when(gy == last)
        def _():
            down[part].start()


    def merged(below, above):
        return jnp.where(lax.rem(lane[: below.shape[0]], 4) < 2, above, below)

    def unfolded(way):
        tips = merged(corner[way, 0], corner[way, 1])
        return jnp.concatenate([tips, pltpu.roll(tips, LANES // 2, 1)], axis=0)

    def place(c, tips, column):
        for field in range(2):
            at = field * columns + column
            edge[field, c] = pltpu.roll(tips, LANES - 4 * at, 1) if at else tips

    both = merged(got[0], got[1])
    for column in range(columns):
        place(low + column, both, column)

    def wide(field, c, width, outer=()):
        tail = jnp.zeros((planes, LANES), jnp.float32) if c in outer else edge[field, c]
        return jnp.concatenate([state[field, c, :, :width], tail], axis=1)

    def first(c, width, outer=()):
        u, v = wide(0, c, width), wide(1, c, width)
        su = spread_of(wide(0, c - 1, width, outer), u, wide(0, c + 1, width, outer))
        sv = spread_of(wide(1, c - 1, width, outer), v, wide(1, c + 1, width, outer))
        for field, new in enumerate(react(u, v, su, sv)):
            middle[field, c, :, :width] = new[:, :width]
            middle[field, c, :, extent:] = new[:, width:]

    def half_way(field, c, width):
        return jnp.concatenate([middle[field, c, :, :width], middle[field, c, :, extent:]], axis=1)

    def second(c, width):
        u, v = half_way(0, c, width), half_way(1, c, width)
        su = spread_of(half_way(0, c - 1, width), u, half_way(0, c + 1, width))
        sv = spread_of(half_way(1, c - 1, width), v, half_way(1, c + 1, width))
        return react(u[:, :width], v[:, :width], su[:, :width], sv[:, :width])

    def pair(k, c, width=extent, own=True, slot=0):
        new = [second(c, width), second(c + 1, width)]
        for field, out in enumerate((u_out, v_out)):
            for tile in range(width // LANES):
                lanes = slice(tile * LANES, (tile + 1) * LANES)
                both_of = [new[i][field][:, lanes] for i in range(2)]
                if own:
                    for i in range(2):
                        rows = pl.ds(tile * columns + c - low + i, planes, stride=tiles * columns)
                        out[rows, :] = both_of[i]
                rows = pl.ds(field * planes * pairs + k, planes, stride=pairs)
                sums[slot, tile, rows, :] = both_of[0] + both_of[1]

    final = len(widths) - 1

    def wait_side(way, part):
        if part == 0:
            wait_got(1 + way, state.at[:, 0:5, :fold, :LANES])
        else:
            up[part].wait_recv() if way == 0 else down[part].wait_recv()

    def low_side(part, wrapped):
        width = widths[part]
        wait_side(0, part)
        if part == 0:
            beyond = unfolded(0)
            for step in range(1, 4 if wrapped else 2):
                place(low - step, beyond, columns - step)
        first(low, width)
        first(low - 1, width, () if wrapped else (low - 2,))
        pair(0, low, width, own=part == final, slot=1 if wrapped else 0)

    def high_side(part):
        width = widths[part]
        wait_side(1, part)
        if part == 0:
            place(high, unfolded(1), 0)
        first(high - 1, width)
        first(high, width, (high + 1,))
        pair(pairs - 1, high - 2, width, own=part == final)

    def level_of(part, slot):
        width = widths[part]
        contract = (((1,), (1,)), ((), ()))
        taking = to_level[: width // 2, :width]
        upper, lower = split(jnp.concatenate([sums[slot, tile] for tile in range(width // LANES)], axis=1))
        level = lax.dot_general(taking, upper, contract, preferred_element_type=jnp.float32)
        level += lax.dot_general(taking, lower, contract, preferred_element_type=jnp.float32)
        for owner in range(*shares[part]):
            outgoing[slot, owner] = level[owner * portion : (owner + 1) * portion]

    def deal(slot, owner):
        target = owners if slot else gy
        return send(3 + slot, dealt_recv, outgoing.at[slot, owner], gathered.at[target], gx, owner)

    for c in range(low + 1, high - 1):
        first(c, extent)
    for k in range(1, pairs - 1):
        pair(k, low + 2 * k)

    for part in parts:

        @pl.when(gy > 0)
        def _():
            low_side(part, False)

        @pl.when(gy < last)
        def _():
            high_side(part)

        if part == 0:

            @pl.when(gy < last - 1)
            def _():
                pl.semaphore_wait(far, far_count)

        if part == 0:

            @pl.when(gy == 0)
            def _():
                for copy in corners_down + down:
                    copy.start()

        level_of(part, 0)
        for owner in range(*shares[part]):

            @pl.when(owner != gy)
            def _():
                deal(0, owner).start()

    @pl.when(gy == 0)
    def _():
        for part in parts:
            low_side(part, True)
            wrap[part].wait_recv()
            width = widths[part]
            first(low - 2, width)
            first(low - 3, width, (low - 4,))
            pair(pairs - 1, low - 2, width, own=False, slot=1)
            level_of(part, 1)
            for owner in range(*shares[part]):
                if owner:
                    deal(1, owner).start()

    gathered[gy] = outgoing[0, gy]

    @pl.when(gy == last)
    def _():
        for part in parts[:-1]:
            wait_side(1, part)
            if part == 0:
                place(high, unfolded(1), 0)
        wait_side(1, final)
        if final == 0:
            place(high, unfolded(1), 0)
        first(high - 1, extent)
        first(high, extent, (high + 1,))
        pair(pairs - 1, high - 2)

    @pl.when(gy == 0)
    def _():
        gathered[owners] = outgoing[1, 0]
        wait_got(dealt_recv, gathered.at[1:owners])
        wait_sent(4, outgoing.at[1, 1:])

    @pl.when(gy > 0)
    def _():
        wait_got(dealt_recv, gathered.at[:owners])

    wait_sent(0, state.at[:, 0:2, :, :LANES])
    wait_sent(1, state.at[:, 0:4])
    wait_sent(3, outgoing.at[0, 1:])

    @pl.when(gy == last)
    def _():
        wait_sent(2, state.at[:, 0:2])


def finish(u_ref, v_ref, dealt, u_out, v_out, rebuilt_out, doubled, paired, rebuilt, sems):
    copies = [
        pltpu.make_async_copy(u_ref, u_out, sems.at[0]),
        pltpu.make_async_copy(v_ref, v_out, sems.at[1]),
    ]
    for copy in copies:
        copy.start()

    owners, portion = dealt.shape[0] - 1, dealt.shape[1]
    wide_in = lax.broadcasted_iota(jnp.int32, (LANES, 4 * LANES), 0)
    wide_out = lax.broadcasted_iota(jnp.int32, (LANES, 4 * LANES), 1)
    column_of = wide_in // 16 * 4 + wide_in % 4
    plane = wide_in // 4 % 4 == wide_out // LANES
    spreading = jnp.concatenate(
        [
            jnp.where(plane & (column_of == wide_out % LANES // 2), 0.5, 0.0),
            jnp.where(plane & (column_of // 2 == wide_out % LANES // 4), 0.125, 0.0),
        ],
        axis=0,
    ).astype(jnp.bfloat16)
    lane = lax.broadcasted_iota(jnp.int32, (portion, LANES), 1)
    even = lax.broadcasted_iota(jnp.int32, (portion, LANES), 0) % 2 == 0
    blocks = [dealt[owner] for owner in range(owners)]
    blocks[0] = jnp.where(lane % 4 == 0, dealt[owners], blocks[0])
    blocks[-1] = jnp.where(lane % 4 == 3, dealt[owners], blocks[-1])
    width, rows = rebuilt.shape[1], 2 * portion
    chunks = 4
    share = 8 // chunks
    for chunk in range(chunks):
        for h in range(chunk * share, (chunk + 1) * share):
            part = jnp.zeros((portion, LANES), jnp.float32)
            for owner in range(8):
                shift = (16 * (owner - h)) % LANES
                moved = pltpu.roll(blocks[owner], shift, 1) if shift else blocks[owner]
                part = jnp.where(lane // 16 == owner, moved, part)
            other = jnp.where(even, pltpu.roll(part, portion - 1, 0), pltpu.roll(part, 1, 0))
            total = part + other
            for twin in range(2):
                doubled[pl.ds(h * rows + twin, portion, stride=2), :] = part
                paired[pl.ds(h * rows + twin, portion, stride=2), :] = total
        span = slice(chunk * share * rows, (chunk + 1) * share * rows)
        high, low = split(jnp.concatenate([doubled[span, :], paired[span, :]], axis=1))
        whole = jnp.dot(high, spreading, preferred_element_type=jnp.float32)
        whole += jnp.dot(low, spreading, preferred_element_type=jnp.float32)
        for h in range(share):
            for z in range(4):
                base = ((chunk * share + h) * 4 + z) * rows
                rebuilt[base : base + rows, :] = whole[
                    h * rows : (h + 1) * rows, z * LANES : z * LANES + width
                ]
        size = share * 4 * rows
        copies.append(
            pltpu.make_async_copy(
                rebuilt.at[chunk * size : (chunk + 1) * size],
                rebuilt_out.at[chunk * size : (chunk + 1) * size],
                sems.at[2],
            )
        )
        copies[-1].start()
    for copy in copies[:2] + [pltpu.make_async_copy(rebuilt, rebuilt_out, sems.at[2])]:
        copy.wait()


def tiled(field):
    planes, columns, extent = field.shape
    field = field.reshape(planes, columns, extent // LANES, LANES)
    return jnp.transpose(field, (0, 2, 1, 3)).reshape(-1, LANES)


def untiled(field, shape):
    planes, columns, extent = shape
    field = field.reshape(planes, extent // LANES, columns, LANES)
    return jnp.transpose(field, (0, 2, 1, 3)).reshape(shape)


def body(substrate, catalyst):
    planes, columns, extent = substrate.shape
    slabs_x, owners = lax.axis_size("gx"), lax.axis_size("gy")
    half, pairs, tiles = extent // 2, columns // 2, extent // LANES
    portion = half // owners
    values = 2 * planes * pairs
    fused = (
        planes == 16 and pairs == 4 and owners == 8 and values == LANES and portion % 8 == 0
    )
    dims = (planes, columns, extent, owners, slabs_x)
    f32 = jnp.float32
    flat = (planes * tiles * columns, LANES)
    vmem = pl.BlockSpec(memory_space=pltpu.VMEM)
    anywhere = pl.BlockSpec(memory_space=pl.ANY)
    u, v, dealt = pl.pallas_call(
        functools.partial(kernel, dims),
        out_shape=(
            pltpu.VMEM(flat, f32),
            pltpu.VMEM(flat, f32),
            pltpu.VMEM((owners + 1, portion, values), f32),
        ),
        in_specs=[anywhere] * 2,
        out_specs=(vmem,) * 3,
        scratch_shapes=[
            pltpu.VMEM((2,) + flat, f32),
            pltpu.VMEM((2, columns + 6, planes, extent), f32),
            pltpu.VMEM((2, columns + 6, planes, LANES), f32),
            pltpu.VMEM((planes, LANES), f32),
            pltpu.VMEM((planes // 2, LANES), f32),
            pltpu.VMEM((2, planes, LANES), f32),
            pltpu.VMEM((2, 2, planes // 2, LANES), f32),
            pltpu.VMEM((2, columns + 6, planes, extent + LANES), f32),
            pltpu.VMEM((2, tiles, values, LANES), f32),
            pltpu.VMEM((2, owners, portion, values), f32),
            pltpu.SemaphoreType.DMA,
            pltpu.SemaphoreType.DMA((5,)),
            pltpu.SemaphoreType.DMA((8 if tiles > 1 else 5,)),
            pltpu.SemaphoreType.REGULAR,
        ],
        compiler_params=pltpu.CompilerParams(collective_id=0, has_side_effects=True),
    )(tiled(substrate), tiled(catalyst))
    rows, width = 2 * portion, columns * owners
    if fused:
        u, v, dealt = (
            pltpu.with_memory_space_constraint(x, pltpu.VMEM) for x in (u, v, dealt)
        )
        u, v, rebuilt = pl.pallas_call(
            finish,
            out_shape=(
                jax.ShapeDtypeStruct(flat, f32),
                jax.ShapeDtypeStruct(flat, f32),
                jax.ShapeDtypeStruct((2 * planes * rows, width), f32),
            ),
            in_specs=[vmem] * 3,
            out_specs=(anywhere,) * 3,
            scratch_shapes=[
                pltpu.VMEM((8 * rows, LANES), f32),
                pltpu.VMEM((8 * rows, LANES), f32),
                pltpu.VMEM((2 * planes * rows, width), f32),
                pltpu.SemaphoreType.DMA((3,)),
            ],
        )(u, v, dealt)
        rebuilt = rebuilt.reshape(2, planes, rows, width)
    else:
        level = dealt.reshape(owners + 1, portion, 2, planes, pairs)
        outer = level[owners]
        lowest = jnp.concatenate([outer[..., :1], level[0, ..., 1:]], axis=-1)
        highest = jnp.concatenate([level[owners - 1, ..., :-1], outer[..., -1:]], axis=-1)
        level = jnp.concatenate([lowest[None], level[1 : owners - 1], highest[None]], axis=0)
        level = jnp.transpose(level, (2, 3, 1, 0, 4)).reshape(2, planes, portion // 2, 2, columns * owners // 4, 2)
        coarse = 0.25 * jnp.sum(level, axis=(3, 5), keepdims=True)
        blend = (coarse + 0.5 * (level - coarse)).reshape(2, planes, portion, columns * owners // 2)
        rebuilt = jnp.repeat(jnp.repeat(blend, 2, axis=2), 2, axis=3)
    return untiled(u, substrate.shape), untiled(v, substrate.shape), rebuilt


def solution(mesh):
    in_specs = (P(None, "gy", "gx"), P(None, "gy", "gx"))
    out_specs = (P(None, "gy", "gx"), P(None, "gy", "gx"), P(None, None, ("gx", "gy"), None))
    return jax.shard_map(body, mesh=mesh, in_specs=in_specs, out_specs=out_specs, check_vma=False)
```

```python
import functools

import jax
import jax.numpy as jnp
from jax import lax
from jax.experimental import pallas as pl
from jax.experimental.pallas import tpu as pltpu
from jax.sharding import PartitionSpec as P

feed_rate = 0.037
kill_rate = 0.06
substrate_diffusion = 0.15
catalyst_diffusion = 0.08

MESH = pl.DeviceIdType.MESH
LANES = 128


def react(substrate, catalyst, spread_substrate, spread_catalyst):
    reaction = substrate * catalyst * catalyst
    new_substrate = (
        substrate
        + substrate_diffusion * spread_substrate
        - reaction
        + feed_rate * (1.0 - substrate)
    )
    new_catalyst = (
        catalyst
        + catalyst_diffusion * spread_catalyst
        + reaction
        - (feed_rate + kill_rate) * catalyst
    )
    return new_substrate, new_catalyst


def split(value):
    high = value.astype(jnp.bfloat16)
    low = (value - high.astype(jnp.float32)).astype(jnp.bfloat16)
    return high, low


def spread_of(before, here, after):
    planes, extent = here.shape
    total = pltpu.roll(here, 1, 0) + pltpu.roll(here, planes - 1, 0)
    for beside in (before, after):
        total = total if beside is None else total + beside
    total = total + pltpu.roll(here, 1, 1) + pltpu.roll(here, extent - 1, 1)
    return total - 6.0 * here


def kernel(dims, *refs):
    planes, columns, extent, owners, slabs_x = dims
    (u_ref, v_ref, u_out, v_out, gathered, loaded, state, edge, packed, folded, got, corner, middle, sums, outgoing,
     load_sem, send_sem, recv_sem, far) = refs
    tiles, pairs, last = extent // LANES, columns // 2, owners - 1
    half = extent // 2
    portion = half // owners
    widths = (LANES, extent) if tiles > 1 else (extent,)
    dealt_to = [(width - 2) // (2 * portion) for width in widths[:-1]] + [owners]
    spans = list(zip((0,) + widths[:-1], widths))
    shares = list(zip([0] + dealt_to[:-1], dealt_to))
    parts = range(len(widths))
    gx, gy = lax.axis_index("gx"), lax.axis_index("gy")
    at_top, at_bottom = gy // last, (last - gy) // last

    barrier = pltpu.get_barrier_semaphore()
    across_of = [lax.rem(gx + shift, slabs_x) for shift in (1, slabs_x - 1)]
    along_of = [lax.rem(gy + shift, owners) for shift in (1, owners - 1)]

    def greet(semaphore, x, y):
        pl.semaphore_signal(semaphore, inc=1, device_id=(x, y), device_id_type=MESH)

    for x in across_of:
        greet(barrier, x, gy)
        greet(barrier, x, along_of[1])

    @pl.when(gy < last)
    def _():
        for x in across_of:
            greet(barrier, x, gy + 1)

    for peer in range(owners):

        @pl.when((peer > gy) | (peer == gy - 1))
        def _():
            greet(barrier, gx, peer)

    near_count = 4 + gy + (1 - at_top) + 2 * (1 - at_bottom)
    far_count = last - gy - 1 + 2 * at_bottom

    loads = [
        pltpu.make_async_copy(source, loaded.at[field], load_sem)
        for field, source in enumerate((u_ref, v_ref))
    ]
    for load in loads:
        load.start()
    pltpu.make_async_copy(loaded, loaded, load_sem).wait()

    low = 2
    high = low + columns
    lane = lax.broadcasted_iota(jnp.int32, (planes, LANES), 1)
    group = lax.rem(lane + 2, LANES) // 4
    pack = jnp.zeros((planes, LANES), jnp.float32)
    for field in range(2):
        for column in range(columns):
            slab = jnp.concatenate(
                [
                    loaded[field, pl.ds(tile * columns + column, planes, stride=tiles * columns), :]
                    for tile in range(tiles)
                ],
                axis=1,
            )
            state[field, low + column] = slab
            at = field * columns + column
            tips = jnp.where(lane < LANES // 2, slab[:, :LANES], slab[:, extent - LANES :])
            tips = pltpu.roll(tips, 4 * at, 1) if at else tips
            pack = jnp.where(group == at, tips, pack)
    packed[...] = pack
    fold = planes // 2
    narrow = lax.broadcasted_iota(jnp.int32, (fold, LANES), 1)
    near_half = lax.rem(narrow + 2, LANES) < LANES // 2
    folded[...] = jnp.where(near_half, pack[:fold], pltpu.roll(pack[fold:], LANES // 2, 1))

    pl.semaphore_wait(barrier, near_count)

    def send(sender, receiver, source, target, x, y):
        return pltpu.make_async_remote_copy(
            src_ref=source,
            dst_ref=target,
            send_sem=send_sem.at[sender],
            recv_sem=recv_sem.at[receiver],
            device_id=(x, y),
            device_id_type=MESH,
        )

    def wait_sent(sender, ref):
        send(sender, 0, ref, ref, gx, gy).wait_send()

    def wait_got(receiver, ref):
        send(0, receiver, ref, ref, gx, gy).wait_recv()

    def columns_of(first_column, count, part):
        return state.at[:, first_column : first_column + count, :, slice(*spans[part])]

    across = [send(0, 0, packed, got.at[side], across_of[side], gy) for side in range(2)]
    corners_up = [send(0, 1, folded, corner.at[0, side], across_of[side], along_of[0]) for side in range(2)]
    corners_down = [send(0, 2, folded, corner.at[1, side], across_of[side], along_of[1]) for side in range(2)]
    up, down = [
        [
            send(1, receiver + 2 * part, columns_of(source, 2, part), columns_of(target, 2, part), gx, along_of[way])
            for part in parts
        ]
        for receiver, source, target, way in ((1, high - 2, low - 2, 0), (2, low, high, 1))
    ]
    dealt_recv = 1 + 2 * len(widths)

    @pl.when(gy == last)
    def _():
        for x in across_of:
            greet(far, x, 0)

    for peer in range(owners - 2):

        @pl.when(peer < gy - 1)
        def _():
            greet(far, gx, peer)

    for copy in across + corners_up:
        copy.start()

    @pl.when(gy > 0)
    def _():
        for copy in corners_down:
            copy.start()

    @pl.when(gy < last)
    def _():
        up[0].start()

    @pl.when(gy > 0)
    def _():
        down[0].start()

    @pl.when((gy > 0) & (gy < last))
    def _():
        for part in parts[1:]:
            down[part].start()

    @pl.when(gy == last)
    def _():
        for part in parts:
            up[part].start()

    row = lax.broadcasted_iota(jnp.int32, (half, extent), 0)
    fine = lax.broadcasted_iota(jnp.int32, (half, extent), 1)
    to_level = jnp.where(fine // 2 == row, 0.25, 0.0).astype(jnp.bfloat16)

    wait_got(0, got)
    for part in parts[1:]:

        @pl.when(gy < last)
        def _():
            up[part].start()

        @pl.when(gy == last)
        def _():
            down[part].start()


    def merged(below, above):
        return jnp.where(lax.rem(lane[: below.shape[0]], 4) < 2, above, below)

    def unfolded(way):
        tips = merged(corner[way, 0], corner[way, 1])
        return jnp.concatenate([tips, pltpu.roll(tips, LANES // 2, 1)], axis=0)

    def place(c, tips, column):
        for field in range(2):
            at = field * columns + column
            edge[field, c] = pltpu.roll(tips, LANES - 4 * at, 1) if at else tips

    both = merged(got[0], got[1])
    for column in range(columns):
        place(low + column, both, column)

    def wide(field, c, width, outer=()):
        tail = jnp.zeros((planes, LANES), jnp.float32) if c in outer else edge[field, c]
        return jnp.concatenate([state[field, c, :, :width], tail], axis=1)

    def first(c, width, outer=()):
        u, v = wide(0, c, width), wide(1, c, width)
        su = spread_of(wide(0, c - 1, width, outer), u, wide(0, c + 1, width, outer))
        sv = spread_of(wide(1, c - 1, width, outer), v, wide(1, c + 1, width, outer))
        for field, new in enumerate(react(u, v, su, sv)):
            middle[field, c, :, :width] = new[:, :width]
            middle[field, c, :, extent:] = new[:, width:]

    def half_way(field, c, width):
        return jnp.concatenate([middle[field, c, :, :width], middle[field, c, :, extent:]], axis=1)

    def second(c, width):
        u, v = half_way(0, c, width), half_way(1, c, width)
        su = spread_of(half_way(0, c - 1, width), u, half_way(0, c + 1, width))
        sv = spread_of(half_way(1, c - 1, width), v, half_way(1, c + 1, width))
        return react(u[:, :width], v[:, :width], su[:, :width], sv[:, :width])

    def pair(k, c, width=extent, own=True, slot=0):
        new = [second(c, width), second(c + 1, width)]
        for field, out in enumerate((u_out, v_out)):
            for tile in range(width // LANES):
                lanes = slice(tile * LANES, (tile + 1) * LANES)
                both_of = [new[i][field][:, lanes] for i in range(2)]
                if own:
                    for i in range(2):
                        rows = pl.ds(tile * columns + c - low + i, planes, stride=tiles * columns)
                        out[rows, :] = both_of[i]
                rows = pl.ds(field * planes * pairs + k, planes, stride=pairs)
                sums[slot, tile, rows, :] = both_of[0] + both_of[1]

    def side_of_pair(c, before, after, width, slot):
        here, near = [], []
        for field in range(2):
            here.append(half_way(field, c, width))
            near.append([None if at is None else half_way(field, at, width) for at in (before, after)])
        spread = [spread_of(near[field][0], here[field], near[field][1])[:, :width] for field in range(2)]
        inner = [here[field][:, :width] for field in range(2)]
        new = react(inner[0], inner[1], spread[0], spread[1])
        for field, diffusion in enumerate((substrate_diffusion, catalyst_diffusion)):
            total = new[field] + diffusion * inner[field]
            for tile in range(width // LANES):
                rows = pl.ds(field * planes * pairs + pairs - 1, planes, stride=pairs)
                sums[slot, tile, rows, :] = total[:, tile * LANES : (tile + 1) * LANES]

    final = len(widths) - 1

    def wait_side(way, part):
        if part == 0:
            wait_got(1 + way, state.at[:, 0:5, :fold, :LANES])
        else:
            up[part].wait_recv() if way == 0 else down[part].wait_recv()

    def low_side(part, wrapped):
        width = widths[part]
        wait_side(0, part)
        if part == 0:
            beyond = unfolded(0)
            for step in range(1, 3 if wrapped else 2):
                place(low - step, beyond, columns - step)
        first(low, width)
        first(low - 1, width, () if wrapped else (low - 2,))
        pair(0, low, width, own=part == final, slot=1 if wrapped else 0)

    def high_side(part):
        width = widths[part]
        wait_side(1, part)
        if part == 0:
            place(high, unfolded(1), 0)
        first(high - 1, width)
        first(high, width, (high + 1,))
        pair(pairs - 1, high - 2, width, own=part == final)

    def level_of(part, slot):
        width = widths[part]
        contract = (((1,), (1,)), ((), ()))
        taking = to_level[: width // 2, :width]
        upper, lower = split(jnp.concatenate([sums[slot, tile] for tile in range(width // LANES)], axis=1))
        level = lax.dot_general(taking, upper, contract, preferred_element_type=jnp.float32)
        level += lax.dot_general(taking, lower, contract, preferred_element_type=jnp.float32)
        for owner in range(*shares[part]):
            outgoing[slot, owner] = level[owner * portion : (owner + 1) * portion]

    def deal(slot, owner):
        target = owners if slot else gy
        return send(2 + slot, dealt_recv, outgoing.at[slot, owner], gathered.at[target], gx, owner)

    for c in range(low + 1, high - 1):
        first(c, extent)
    for k in range(1, pairs - 1):
        pair(k, low + 2 * k)

    @pl.when(gy == last)
    def _():
        side_of_pair(high - 2, high - 3, None, extent, 0)

    for part in parts:

        @pl.when(gy > 0)
        def _():
            low_side(part, False)

        @pl.when(gy < last)
        def _():
            high_side(part)

        if part == 0:

            @pl.when(gy < last - 1)
            def _():
                pl.semaphore_wait(far, far_count)

        if part == 0:

            @pl.when(gy == 0)
            def _():
                for copy in corners_down + down:
                    copy.start()

        level_of(part, 0)
        for owner in range(*shares[part]):

            @pl.when(owner != gy)
            def _():
                deal(0, owner).start()

    @pl.when(gy == 0)
    def _():
        for part in parts:
            low_side(part, True)
            side_of_pair(low - 1, None, low, widths[part], 1)
            level_of(part, 1)
            for owner in range(*shares[part]):
                if owner:
                    deal(1, owner).start()

    gathered[gy] = outgoing[0, gy]

    @pl.when(gy == last)
    def _():
        for part in parts[:-1]:
            wait_side(1, part)
            if part == 0:
                place(high, unfolded(1), 0)
        wait_side(1, final)
        if final == 0:
            place(high, unfolded(1), 0)
        first(high - 1, extent)
        first(high, extent, (high + 1,))
        pair(pairs - 1, high - 2)

    @pl.when(gy == 0)
    def _():
        gathered[owners] = outgoing[1, 0]
        wait_got(dealt_recv, gathered.at[1:owners])
        wait_sent(3, outgoing.at[1, 1:])

    @pl.when(gy > 0)
    def _():
        wait_got(dealt_recv, gathered.at[:owners])

    wait_sent(0, state.at[:, 0:2, :, :LANES])
    wait_sent(1, state.at[:, 0:4])
    wait_sent(2, outgoing.at[0, 1:])


def finish(u_ref, v_ref, dealt, u_out, v_out, rebuilt_out, doubled, paired, rebuilt, sems):
    copies = [
        pltpu.make_async_copy(u_ref, u_out, sems.at[0]),
        pltpu.make_async_copy(v_ref, v_out, sems.at[1]),
    ]
    for copy in copies:
        copy.start()

    owners, portion = dealt.shape[0] - 1, dealt.shape[1]
    wide_in = lax.broadcasted_iota(jnp.int32, (LANES, 4 * LANES), 0)
    wide_out = lax.broadcasted_iota(jnp.int32, (LANES, 4 * LANES), 1)
    column_of = wide_in // 16 * 4 + wide_in % 4
    plane = wide_in // 4 % 4 == wide_out // LANES
    spreading = jnp.concatenate(
        [
            jnp.where(plane & (column_of == wide_out % LANES // 2), 0.5, 0.0),
            jnp.where(plane & (column_of // 2 == wide_out % LANES // 4), 0.125, 0.0),
        ],
        axis=0,
    ).astype(jnp.bfloat16)
    lane = lax.broadcasted_iota(jnp.int32, (portion, LANES), 1)
    even = lax.broadcasted_iota(jnp.int32, (portion, LANES), 0) % 2 == 0
    blocks = [dealt[owner] for owner in range(owners)]
    blocks[0] = jnp.where(lane % 4 == 0, dealt[owners], blocks[0])
    blocks[-1] = jnp.where(lane % 4 == 3, blocks[-1] + dealt[owners], blocks[-1])
    width, rows = rebuilt.shape[1], 2 * portion
    chunks = 4
    share = 8 // chunks
    for chunk in range(chunks):
        for h in range(chunk * share, (chunk + 1) * share):
            part = jnp.zeros((portion, LANES), jnp.float32)
            for owner in range(8):
                shift = (16 * (owner - h)) % LANES
                moved = pltpu.roll(blocks[owner], shift, 1) if shift else blocks[owner]
                part = jnp.where(lane // 16 == owner, moved, part)
            other = jnp.where(even, pltpu.roll(part, portion - 1, 0), pltpu.roll(part, 1, 0))
            total = part + other
            for twin in range(2):
                doubled[pl.ds(h * rows + twin, portion, stride=2), :] = part
                paired[pl.ds(h * rows + twin, portion, stride=2), :] = total
        span = slice(chunk * share * rows, (chunk + 1) * share * rows)
        high, low = split(jnp.concatenate([doubled[span, :], paired[span, :]], axis=1))
        whole = jnp.dot(high, spreading, preferred_element_type=jnp.float32)
        whole += jnp.dot(low, spreading, preferred_element_type=jnp.float32)
        for h in range(share):
            for z in range(4):
                base = ((chunk * share + h) * 4 + z) * rows
                rebuilt[base : base + rows, :] = whole[
                    h * rows : (h + 1) * rows, z * LANES : z * LANES + width
                ]
        size = share * 4 * rows
        copies.append(
            pltpu.make_async_copy(
                rebuilt.at[chunk * size : (chunk + 1) * size],
                rebuilt_out.at[chunk * size : (chunk + 1) * size],
                sems.at[2],
            )
        )
        copies[-1].start()
    for copy in copies[:2] + [pltpu.make_async_copy(rebuilt, rebuilt_out, sems.at[2])]:
        copy.wait()


def tiled(field):
    planes, columns, extent = field.shape
    field = field.reshape(planes, columns, extent // LANES, LANES)
    return jnp.transpose(field, (0, 2, 1, 3)).reshape(-1, LANES)


def untiled(field, shape):
    planes, columns, extent = shape
    field = field.reshape(planes, extent // LANES, columns, LANES)
    return jnp.transpose(field, (0, 2, 1, 3)).reshape(shape)


def body(substrate, catalyst):
    planes, columns, extent = substrate.shape
    slabs_x, owners = lax.axis_size("gx"), lax.axis_size("gy")
    half, pairs, tiles = extent // 2, columns // 2, extent // LANES
    portion = half // owners
    values = 2 * planes * pairs
    fused = (
        planes == 16 and pairs == 4 and owners == 8 and values == LANES and portion % 8 == 0
    )
    dims = (planes, columns, extent, owners, slabs_x)
    f32 = jnp.float32
    flat = (planes * tiles * columns, LANES)
    vmem = pl.BlockSpec(memory_space=pltpu.VMEM)
    anywhere = pl.BlockSpec(memory_space=pl.ANY)
    u, v, dealt = pl.pallas_call(
        functools.partial(kernel, dims),
        out_shape=(
            pltpu.VMEM(flat, f32),
            pltpu.VMEM(flat, f32),
            pltpu.VMEM((owners + 1, portion, values), f32),
        ),
        in_specs=[anywhere] * 2,
        out_specs=(vmem,) * 3,
        scratch_shapes=[
            pltpu.VMEM((2,) + flat, f32),
            pltpu.VMEM((2, columns + 4, planes, extent), f32),
            pltpu.VMEM((2, columns + 4, planes, LANES), f32),
            pltpu.VMEM((planes, LANES), f32),
            pltpu.VMEM((planes // 2, LANES), f32),
            pltpu.VMEM((2, planes, LANES), f32),
            pltpu.VMEM((2, 2, planes // 2, LANES), f32),
            pltpu.VMEM((2, columns + 4, planes, extent + LANES), f32),
            pltpu.VMEM((2, tiles, values, LANES), f32),
            pltpu.VMEM((2, owners, portion, values), f32),
            pltpu.SemaphoreType.DMA,
            pltpu.SemaphoreType.DMA((4,)),
            pltpu.SemaphoreType.DMA((6 if tiles > 1 else 4,)),
            pltpu.SemaphoreType.REGULAR,
        ],
        compiler_params=pltpu.CompilerParams(collective_id=0, has_side_effects=True),
    )(tiled(substrate), tiled(catalyst))
    rows, width = 2 * portion, columns * owners
    if fused:
        u, v, dealt = (
            pltpu.with_memory_space_constraint(x, pltpu.VMEM) for x in (u, v, dealt)
        )
        u, v, rebuilt = pl.pallas_call(
            finish,
            out_shape=(
                jax.ShapeDtypeStruct(flat, f32),
                jax.ShapeDtypeStruct(flat, f32),
                jax.ShapeDtypeStruct((2 * planes * rows, width), f32),
            ),
            in_specs=[vmem] * 3,
            out_specs=(anywhere,) * 3,
            scratch_shapes=[
                pltpu.VMEM((8 * rows, LANES), f32),
                pltpu.VMEM((8 * rows, LANES), f32),
                pltpu.VMEM((2 * planes * rows, width), f32),
                pltpu.SemaphoreType.DMA((3,)),
            ],
        )(u, v, dealt)
        rebuilt = rebuilt.reshape(2, planes, rows, width)
    else:
        level = dealt.reshape(owners + 1, portion, 2, planes, pairs)
        outer = level[owners]
        lowest = jnp.concatenate([outer[..., :1], level[0, ..., 1:]], axis=-1)
        highest = level[owners - 1]
        highest = jnp.concatenate([highest[..., :-1], highest[..., -1:] + outer[..., -1:]], axis=-1)
        level = jnp.concatenate([lowest[None], level[1 : owners - 1], highest[None]], axis=0)
        level = jnp.transpose(level, (2, 3, 1, 0, 4)).reshape(2, planes, portion // 2, 2, columns * owners // 4, 2)
        coarse = 0.25 * jnp.sum(level, axis=(3, 5), keepdims=True)
        blend = (coarse + 0.5 * (level - coarse)).reshape(2, planes, portion, columns * owners // 2)
        rebuilt = jnp.repeat(jnp.repeat(blend, 2, axis=2), 2, axis=3)
    return untiled(u, substrate.shape), untiled(v, substrate.shape), rebuilt


def solution(mesh):
    in_specs = (P(None, "gy", "gx"), P(None, "gy", "gx"))
    out_specs = (P(None, "gy", "gx"), P(None, "gy", "gx"), P(None, None, ("gx", "gy"), None))
    return jax.shard_map(body, mesh=mesh, in_specs=in_specs, out_specs=out_specs, check_vma=False)
```

```python
import functools

import jax
import jax.numpy as jnp
from jax import lax
from jax.experimental import pallas as pl
from jax.experimental.pallas import tpu as pltpu
from jax.sharding import PartitionSpec as P

feed_rate = 0.037
kill_rate = 0.06
substrate_diffusion = 0.15
catalyst_diffusion = 0.08

MESH = pl.DeviceIdType.MESH
LANES = 128


def react(substrate, catalyst, spread_substrate, spread_catalyst):
    reaction = substrate * catalyst * catalyst
    new_substrate = (
        substrate
        + substrate_diffusion * spread_substrate
        - reaction
        + feed_rate * (1.0 - substrate)
    )
    new_catalyst = (
        catalyst
        + catalyst_diffusion * spread_catalyst
        + reaction
        - (feed_rate + kill_rate) * catalyst
    )
    return new_substrate, new_catalyst


def split(value):
    high = value.astype(jnp.bfloat16)
    low = (value - high.astype(jnp.float32)).astype(jnp.bfloat16)
    return high, low


def spread_of(before, here, after):
    planes, extent = here.shape
    total = pltpu.roll(here, 1, 0) + pltpu.roll(here, planes - 1, 0)
    for beside in (before, after):
        total = total if beside is None else total + beside
    total = total + pltpu.roll(here, 1, 1) + pltpu.roll(here, extent - 1, 1)
    return total - 6.0 * here


def spreading_of():
    wide_in = lax.broadcasted_iota(jnp.int32, (LANES, 4 * LANES), 0)
    wide_out = lax.broadcasted_iota(jnp.int32, (LANES, 4 * LANES), 1)
    column_of = wide_in // 16 * 4 + wide_in % 4
    plane = wide_in // 4 % 4 == wide_out // LANES
    return jnp.concatenate(
        [
            jnp.where(plane & (column_of == wide_out % LANES // 2), 0.5, 0.0),
            jnp.where(plane & (column_of // 2 == wide_out % LANES // 4), 0.125, 0.0),
        ],
        axis=0,
    ).astype(jnp.bfloat16)


def kernel(dims, *refs):
    planes, columns, extent, owners, slabs_x = dims
    (u_ref, v_ref, u_out, v_out, gathered, spreading, loaded, state, edge, packed, folded, got, corner, middle, sums, outgoing,
     load_sem, send_sem, recv_sem, far) = refs
    tiles, pairs, last = extent // LANES, columns // 2, owners - 1
    half = extent // 2
    portion = half // owners
    widths = (LANES, extent) if tiles > 1 else (extent,)
    dealt_to = [(width - 2) // (2 * portion) for width in widths[:-1]] + [owners]
    spans = list(zip((0,) + widths[:-1], widths))
    shares = list(zip([0] + dealt_to[:-1], dealt_to))
    parts = range(len(widths))
    gx, gy = lax.axis_index("gx"), lax.axis_index("gy")
    at_top, at_bottom = gy // last, (last - gy) // last

    barrier = pltpu.get_barrier_semaphore()
    across_of = [lax.rem(gx + shift, slabs_x) for shift in (1, slabs_x - 1)]
    along_of = [lax.rem(gy + shift, owners) for shift in (1, owners - 1)]

    def greet(semaphore, x, y):
        pl.semaphore_signal(semaphore, inc=1, device_id=(x, y), device_id_type=MESH)

    for x in across_of:
        greet(barrier, x, gy)
        greet(barrier, x, along_of[1])

    @pl.when(gy < last)
    def _():
        for x in across_of:
            greet(barrier, x, gy + 1)

    for peer in range(owners):

        @pl.when((peer > gy) | (peer == gy - 1))
        def _():
            greet(barrier, gx, peer)

    near_count = 4 + gy + (1 - at_top) + 2 * (1 - at_bottom)
    far_count = last - gy - 1 + 2 * at_bottom

    loads = [
        pltpu.make_async_copy(source, loaded.at[field], load_sem)
        for field, source in enumerate((u_ref, v_ref))
    ]
    for load in loads:
        load.start()
    pltpu.make_async_copy(loaded, loaded, load_sem).wait()

    low = 2
    high = low + columns
    lane = lax.broadcasted_iota(jnp.int32, (planes, LANES), 1)
    group = lax.rem(lane + 2, LANES) // 4
    pack = jnp.zeros((planes, LANES), jnp.float32)
    for field in range(2):
        for column in range(columns):
            slab = jnp.concatenate(
                [
                    loaded[field, pl.ds(tile * columns + column, planes, stride=tiles * columns), :]
                    for tile in range(tiles)
                ],
                axis=1,
            )
            state[field, low + column] = slab
            at = field * columns + column
            tips = jnp.where(lane < LANES // 2, slab[:, :LANES], slab[:, extent - LANES :])
            tips = pltpu.roll(tips, 4 * at, 1) if at else tips
            pack = jnp.where(group == at, tips, pack)
    packed[...] = pack
    fold = planes // 2
    narrow = lax.broadcasted_iota(jnp.int32, (fold, LANES), 1)
    near_half = lax.rem(narrow + 2, LANES) < LANES // 2
    folded[...] = jnp.where(near_half, pack[:fold], pltpu.roll(pack[fold:], LANES // 2, 1))

    pl.semaphore_wait(barrier, near_count)

    def send(sender, receiver, source, target, x, y):
        return pltpu.make_async_remote_copy(
            src_ref=source,
            dst_ref=target,
            send_sem=send_sem.at[sender],
            recv_sem=recv_sem.at[receiver],
            device_id=(x, y),
            device_id_type=MESH,
        )

    def wait_sent(sender, ref):
        send(sender, 0, ref, ref, gx, gy).wait_send()

    def wait_got(receiver, ref):
        send(0, receiver, ref, ref, gx, gy).wait_recv()

    def columns_of(first_column, count, part):
        return state.at[:, first_column : first_column + count, :, slice(*spans[part])]

    across = [send(0, 0, packed, got.at[side], across_of[side], gy) for side in range(2)]
    corners_up = [send(0, 1, folded, corner.at[0, side], across_of[side], along_of[0]) for side in range(2)]
    corners_down = [send(0, 2, folded, corner.at[1, side], across_of[side], along_of[1]) for side in range(2)]
    up, down = [
        [
            send(1, receiver + 2 * part, columns_of(source, 2, part), columns_of(target, 2, part), gx, along_of[way])
            for part in parts
        ]
        for receiver, source, target, way in ((1, high - 2, low - 2, 0), (2, low, high, 1))
    ]
    dealt_recv = 1 + 2 * len(widths)

    @pl.when(gy == last)
    def _():
        for x in across_of:
            greet(far, x, 0)

    for peer in range(owners - 2):

        @pl.when(peer < gy - 1)
        def _():
            greet(far, gx, peer)

    for copy in across + corners_up:
        copy.start()

    @pl.when(gy > 0)
    def _():
        for copy in corners_down:
            copy.start()

    @pl.when(gy < last)
    def _():
        up[0].start()

    @pl.when(gy > 0)
    def _():
        down[0].start()

    @pl.when((gy > 0) & (gy < last))
    def _():
        for part in parts[1:]:
            down[part].start()

    @pl.when(gy == last)
    def _():
        for part in parts:
            up[part].start()

    row = lax.broadcasted_iota(jnp.int32, (half, extent), 0)
    fine = lax.broadcasted_iota(jnp.int32, (half, extent), 1)
    to_level = jnp.where(fine // 2 == row, 0.25, 0.0).astype(jnp.bfloat16)

    spreading[...] = spreading_of()

    wait_got(0, got)
    for part in parts[1:]:

        @pl.when(gy < last)
        def _():
            up[part].start()

        @pl.when(gy == last)
        def _():
            down[part].start()


    def merged(below, above):
        return jnp.where(lax.rem(lane[: below.shape[0]], 4) < 2, above, below)

    def unfolded(way):
        tips = merged(corner[way, 0], corner[way, 1])
        return jnp.concatenate([tips, pltpu.roll(tips, LANES // 2, 1)], axis=0)

    def place(c, tips, column):
        for field in range(2):
            at = field * columns + column
            edge[field, c] = pltpu.roll(tips, LANES - 4 * at, 1) if at else tips

    both = merged(got[0], got[1])
    for column in range(columns):
        place(low + column, both, column)

    def wide(field, c, width, outer=()):
        tail = jnp.zeros((planes, LANES), jnp.float32) if c in outer else edge[field, c]
        return jnp.concatenate([state[field, c, :, :width], tail], axis=1)

    def first(c, width, outer=()):
        u, v = wide(0, c, width), wide(1, c, width)
        su = spread_of(wide(0, c - 1, width, outer), u, wide(0, c + 1, width, outer))
        sv = spread_of(wide(1, c - 1, width, outer), v, wide(1, c + 1, width, outer))
        for field, new in enumerate(react(u, v, su, sv)):
            middle[field, c, :, :width] = new[:, :width]
            middle[field, c, :, extent:] = new[:, width:]

    def half_way(field, c, width):
        return jnp.concatenate([middle[field, c, :, :width], middle[field, c, :, extent:]], axis=1)

    def second(c, width):
        u, v = half_way(0, c, width), half_way(1, c, width)
        su = spread_of(half_way(0, c - 1, width), u, half_way(0, c + 1, width))
        sv = spread_of(half_way(1, c - 1, width), v, half_way(1, c + 1, width))
        return react(u[:, :width], v[:, :width], su[:, :width], sv[:, :width])

    def pair(k, c, width=extent, own=True, slot=0):
        new = [second(c, width), second(c + 1, width)]
        for field, out in enumerate((u_out, v_out)):
            for tile in range(width // LANES):
                lanes = slice(tile * LANES, (tile + 1) * LANES)
                both_of = [new[i][field][:, lanes] for i in range(2)]
                if own:
                    for i in range(2):
                        rows = pl.ds(tile * columns + c - low + i, planes, stride=tiles * columns)
                        out[rows, :] = both_of[i]
                rows = pl.ds(field * planes * pairs + k, planes, stride=pairs)
                sums[slot, tile, rows, :] = both_of[0] + both_of[1]

    def side_of_pair(c, before, after, width, slot):
        here, near = [], []
        for field in range(2):
            here.append(half_way(field, c, width))
            near.append([None if at is None else half_way(field, at, width) for at in (before, after)])
        spread = [spread_of(near[field][0], here[field], near[field][1])[:, :width] for field in range(2)]
        inner = [here[field][:, :width] for field in range(2)]
        new = react(inner[0], inner[1], spread[0], spread[1])
        for field, diffusion in enumerate((substrate_diffusion, catalyst_diffusion)):
            total = new[field] + diffusion * inner[field]
            for tile in range(width // LANES):
                rows = pl.ds(field * planes * pairs + pairs - 1, planes, stride=pairs)
                sums[slot, tile, rows, :] = total[:, tile * LANES : (tile + 1) * LANES]

    final = len(widths) - 1

    def wait_side(way, part):
        if part == 0:
            wait_got(1 + way, state.at[:, 0:5, :fold, :LANES])
        else:
            up[part].wait_recv() if way == 0 else down[part].wait_recv()

    def low_side(part, wrapped):
        width = widths[part]
        wait_side(0, part)
        if part == 0:
            beyond = unfolded(0)
            for step in range(1, 3 if wrapped else 2):
                place(low - step, beyond, columns - step)
        first(low, width)
        first(low - 1, width, () if wrapped else (low - 2,))
        pair(0, low, width, own=part == final, slot=1 if wrapped else 0)

    def high_side(part):
        width = widths[part]
        wait_side(1, part)
        if part == 0:
            place(high, unfolded(1), 0)
        first(high - 1, width)
        first(high, width, (high + 1,))
        pair(pairs - 1, high - 2, width, own=part == final)

    def level_of(part, slot):
        width = widths[part]
        contract = (((1,), (1,)), ((), ()))
        taking = to_level[: width // 2, :width]
        upper, lower = split(jnp.concatenate([sums[slot, tile] for tile in range(width // LANES)], axis=1))
        level = lax.dot_general(
            jnp.concatenate([taking, taking], axis=1),
            jnp.concatenate([upper, lower], axis=1),
            contract,
            preferred_element_type=jnp.float32,
        )
        for owner in range(*shares[part]):
            outgoing[slot, owner] = level[owner * portion : (owner + 1) * portion]

    def deal(slot, owner):
        target = owners if slot else gy
        return send(2 + slot, dealt_recv, outgoing.at[slot, owner], gathered.at[target], gx, owner)

    for c in range(low + 1, high - 1):
        first(c, extent)
    for k in range(1, pairs - 1):
        pair(k, low + 2 * k)

    @pl.when(gy == last)
    def _():
        side_of_pair(high - 2, high - 3, None, extent, 0)

    for part in parts:

        @pl.when(gy > 0)
        def _():
            low_side(part, False)

        @pl.when(gy < last)
        def _():
            high_side(part)

        if part == 0:

            @pl.when(gy < last - 1)
            def _():
                pl.semaphore_wait(far, far_count)

        if part == 0:

            @pl.when(gy == 0)
            def _():
                for copy in corners_down + down:
                    copy.start()

        level_of(part, 0)
        for owner in range(*shares[part]):

            @pl.when(owner != gy)
            def _():
                deal(0, owner).start()

    @pl.when(gy == 0)
    def _():
        for part in parts:
            low_side(part, True)
            side_of_pair(low - 1, None, low, widths[part], 1)
            level_of(part, 1)
            for owner in range(*shares[part]):
                if owner:
                    deal(1, owner).start()

    gathered[gy] = outgoing[0, gy]

    @pl.when(gy == last)
    def _():
        for part in parts[:-1]:
            wait_side(1, part)
            if part == 0:
                place(high, unfolded(1), 0)
        wait_side(1, final)
        if final == 0:
            place(high, unfolded(1), 0)
        first(high - 1, extent)
        first(high, extent, (high + 1,))
        pair(pairs - 1, high - 2)

    @pl.when(gy == 0)
    def _():
        gathered[owners] = outgoing[1, 0]
        wait_got(dealt_recv, gathered.at[1:owners])
        wait_sent(3, outgoing.at[1, 1:])

    @pl.when(gy > 0)
    def _():
        wait_got(dealt_recv, gathered.at[:owners])

    wait_sent(0, state.at[:, 0:2, :, :LANES])
    wait_sent(1, state.at[:, 0:4])
    wait_sent(2, outgoing.at[0, 1:])


def finish(u_ref, v_ref, dealt, spreading, u_out, v_out, rebuilt_out, doubled, paired, rebuilt, sems):
    copies = [
        pltpu.make_async_copy(u_ref, u_out, sems.at[0]),
        pltpu.make_async_copy(v_ref, v_out, sems.at[1]),
    ]
    for copy in copies:
        copy.start()

    owners, portion = dealt.shape[0] - 1, dealt.shape[1]
    lane = lax.broadcasted_iota(jnp.int32, (portion, LANES), 1)
    even = lax.broadcasted_iota(jnp.int32, (portion, LANES), 0) % 2 == 0
    blocks = [dealt[owner] for owner in range(owners)]
    blocks[0] = jnp.where(lane % 4 == 0, dealt[owners], blocks[0])
    blocks[-1] = jnp.where(lane % 4 == 3, blocks[-1] + dealt[owners], blocks[-1])
    width, rows = rebuilt.shape[1], 2 * portion
    chunks = 4
    share = 8 // chunks
    for chunk in range(chunks):
        for h in range(chunk * share, (chunk + 1) * share):
            part = jnp.zeros((portion, LANES), jnp.float32)
            for owner in range(8):
                shift = (16 * (owner - h)) % LANES
                moved = pltpu.roll(blocks[owner], shift, 1) if shift else blocks[owner]
                part = jnp.where(lane // 16 == owner, moved, part)
            other = jnp.where(even, pltpu.roll(part, portion - 1, 0), pltpu.roll(part, 1, 0))
            total = part + other
            for twin in range(2):
                doubled[pl.ds(h * rows + twin, portion, stride=2), :] = part
                paired[pl.ds(h * rows + twin, portion, stride=2), :] = total
        span = slice(chunk * share * rows, (chunk + 1) * share * rows)
        high, low = split(jnp.concatenate([doubled[span, :], paired[span, :]], axis=1))
        whole = jnp.dot(
            jnp.concatenate([high, low], axis=1),
            jnp.concatenate([spreading[...], spreading[...]], axis=0),
            preferred_element_type=jnp.float32,
        )
        for h in range(share):
            for z in range(4):
                base = ((chunk * share + h) * 4 + z) * rows
                rebuilt[base : base + rows, :] = whole[
                    h * rows : (h + 1) * rows, z * LANES : z * LANES + width
                ]
        size = share * 4 * rows
        copies.append(
            pltpu.make_async_copy(
                rebuilt.at[chunk * size : (chunk + 1) * size],
                rebuilt_out.at[chunk * size : (chunk + 1) * size],
                sems.at[2],
            )
        )
        copies[-1].start()
    for copy in copies[:2] + [pltpu.make_async_copy(rebuilt, rebuilt_out, sems.at[2])]:
        copy.wait()


def tiled(field):
    planes, columns, extent = field.shape
    field = field.reshape(planes, columns, extent // LANES, LANES)
    return jnp.transpose(field, (0, 2, 1, 3)).reshape(-1, LANES)


def untiled(field, shape):
    planes, columns, extent = shape
    field = field.reshape(planes, extent // LANES, columns, LANES)
    return jnp.transpose(field, (0, 2, 1, 3)).reshape(shape)


def body(substrate, catalyst):
    planes, columns, extent = substrate.shape
    slabs_x, owners = lax.axis_size("gx"), lax.axis_size("gy")
    half, pairs, tiles = extent // 2, columns // 2, extent // LANES
    portion = half // owners
    values = 2 * planes * pairs
    fused = (
        planes == 16 and pairs == 4 and owners == 8 and values == LANES and portion % 8 == 0
    )
    dims = (planes, columns, extent, owners, slabs_x)
    f32 = jnp.float32
    flat = (planes * tiles * columns, LANES)
    vmem = pl.BlockSpec(memory_space=pltpu.VMEM)
    anywhere = pl.BlockSpec(memory_space=pl.ANY)
    u, v, dealt, spreading = pl.pallas_call(
        functools.partial(kernel, dims),
        out_shape=(
            pltpu.VMEM(flat, f32),
            pltpu.VMEM(flat, f32),
            pltpu.VMEM((owners + 1, portion, values), f32),
            pltpu.VMEM((2 * LANES, 4 * LANES), jnp.bfloat16),
        ),
        in_specs=[anywhere] * 2,
        out_specs=(vmem,) * 4,
        scratch_shapes=[
            pltpu.VMEM((2,) + flat, f32),
            pltpu.VMEM((2, columns + 4, planes, extent), f32),
            pltpu.VMEM((2, columns + 4, planes, LANES), f32),
            pltpu.VMEM((planes, LANES), f32),
            pltpu.VMEM((planes // 2, LANES), f32),
            pltpu.VMEM((2, planes, LANES), f32),
            pltpu.VMEM((2, 2, planes // 2, LANES), f32),
            pltpu.VMEM((2, columns + 4, planes, extent + LANES), f32),
            pltpu.VMEM((2, tiles, values, LANES), f32),
            pltpu.VMEM((2, owners, portion, values), f32),
            pltpu.SemaphoreType.DMA,
            pltpu.SemaphoreType.DMA((4,)),
            pltpu.SemaphoreType.DMA((6 if tiles > 1 else 4,)),
            pltpu.SemaphoreType.REGULAR,
        ],
        compiler_params=pltpu.CompilerParams(collective_id=0, has_side_effects=True),
    )(tiled(substrate), tiled(catalyst))
    rows, width = 2 * portion, columns * owners
    if fused:
        u, v, dealt, spreading = (
            pltpu.with_memory_space_constraint(x, pltpu.VMEM) for x in (u, v, dealt, spreading)
        )
        u, v, rebuilt = pl.pallas_call(
            finish,
            out_shape=(
                jax.ShapeDtypeStruct(flat, f32),
                jax.ShapeDtypeStruct(flat, f32),
                jax.ShapeDtypeStruct((2 * planes * rows, width), f32),
            ),
            in_specs=[vmem] * 4,
            out_specs=(anywhere,) * 3,
            scratch_shapes=[
                pltpu.VMEM((8 * rows, LANES), f32),
                pltpu.VMEM((8 * rows, LANES), f32),
                pltpu.VMEM((2 * planes * rows, width), f32),
                pltpu.SemaphoreType.DMA((3,)),
            ],
        )(u, v, dealt, spreading)
        rebuilt = rebuilt.reshape(2, planes, rows, width)
    else:
        level = dealt.reshape(owners + 1, portion, 2, planes, pairs)
        outer = level[owners]
        lowest = jnp.concatenate([outer[..., :1], level[0, ..., 1:]], axis=-1)
        highest = level[owners - 1]
        highest = jnp.concatenate([highest[..., :-1], highest[..., -1:] + outer[..., -1:]], axis=-1)
        level = jnp.concatenate([lowest[None], level[1 : owners - 1], highest[None]], axis=0)
        level = jnp.transpose(level, (2, 3, 1, 0, 4)).reshape(2, planes, portion // 2, 2, columns * owners // 4, 2)
        coarse = 0.25 * jnp.sum(level, axis=(3, 5), keepdims=True)
        blend = (coarse + 0.5 * (level - coarse)).reshape(2, planes, portion, columns * owners // 2)
        rebuilt = jnp.repeat(jnp.repeat(blend, 2, axis=2), 2, axis=3)
    return untiled(u, substrate.shape), untiled(v, substrate.shape), rebuilt


def solution(mesh):
    in_specs = (P(None, "gy", "gx"), P(None, "gy", "gx"))
    out_specs = (P(None, "gy", "gx"), P(None, "gy", "gx"), P(None, None, ("gx", "gy"), None))
    return jax.shard_map(body, mesh=mesh, in_specs=in_specs, out_specs=out_specs, check_vma=False)
```

```python
import functools

import jax
import jax.numpy as jnp
from jax import lax
from jax.experimental import pallas as pl
from jax.experimental.pallas import tpu as pltpu
from jax.sharding import PartitionSpec as P

feed_rate = 0.037
kill_rate = 0.06
substrate_diffusion = 0.15
catalyst_diffusion = 0.08

MESH = pl.DeviceIdType.MESH
LANES = 128


def react(substrate, catalyst, spread_substrate, spread_catalyst):
    reaction = substrate * catalyst * catalyst
    new_substrate = (
        substrate
        + substrate_diffusion * spread_substrate
        - reaction
        + feed_rate * (1.0 - substrate)
    )
    new_catalyst = (
        catalyst
        + catalyst_diffusion * spread_catalyst
        + reaction
        - (feed_rate + kill_rate) * catalyst
    )
    return new_substrate, new_catalyst


def split(value):
    high = value.astype(jnp.bfloat16)
    low = (value - high.astype(jnp.float32)).astype(jnp.bfloat16)
    return high, low


def spread_of(before, here, after):
    planes, extent = here.shape
    total = pltpu.roll(here, 1, 0) + pltpu.roll(here, planes - 1, 0)
    for beside in (before, after):
        total = total if beside is None else total + beside
    total = total + pltpu.roll(here, 1, 1) + pltpu.roll(here, extent - 1, 1)
    return total - 6.0 * here


def spreading_of():
    wide_in = lax.broadcasted_iota(jnp.int32, (LANES, 4 * LANES), 0)
    wide_out = lax.broadcasted_iota(jnp.int32, (LANES, 4 * LANES), 1)
    column_of = wide_in // 16 * 4 + wide_in % 4
    plane = wide_in // 4 % 4 == wide_out // LANES
    return jnp.concatenate(
        [
            jnp.where(plane & (column_of == wide_out % LANES // 2), 0.5, 0.0),
            jnp.where(plane & (column_of // 2 == wide_out % LANES // 4), 0.125, 0.0),
        ],
        axis=0,
    ).astype(jnp.bfloat16)


def kernel(dims, *refs):
    planes, columns, extent, owners, slabs_x = dims
    (u_ref, v_ref, u_out, v_out, gathered, spreading, loaded, state, edge, packed, folded, got, corner, middle, sums, outgoing,
     load_sem, send_sem, recv_sem, far) = refs
    tiles, pairs, last = extent // LANES, columns // 2, owners - 1
    half = extent // 2
    portion = half // owners
    widths = (LANES, extent) if tiles > 1 else (extent,)
    dealt_to = [(width - 2) // (2 * portion) for width in widths[:-1]] + [owners]
    spans = list(zip((0,) + widths[:-1], widths))
    shares = list(zip([0] + dealt_to[:-1], dealt_to))
    parts = range(len(widths))
    gx, gy = lax.axis_index("gx"), lax.axis_index("gy")
    at_top, at_bottom = gy // last, (last - gy) // last

    barrier = pltpu.get_barrier_semaphore()
    across_of = [lax.rem(gx + shift, slabs_x) for shift in (1, slabs_x - 1)]
    along_of = [lax.rem(gy + shift, owners) for shift in (1, owners - 1)]

    def greet(semaphore, x, y):
        pl.semaphore_signal(semaphore, inc=1, device_id=(x, y), device_id_type=MESH)

    for x in across_of:
        greet(barrier, x, gy)
        greet(barrier, x, along_of[1])

    @pl.when(gy < last)
    def _():
        for x in across_of:
            greet(barrier, x, gy + 1)

    for peer in range(owners):

        @pl.when((peer > gy) | (peer == gy - 1))
        def _():
            greet(barrier, gx, peer)

    near_count = 4 + gy + (1 - at_top) + 2 * (1 - at_bottom)
    far_count = last - gy - 1 + 2 * at_bottom

    loads = [
        pltpu.make_async_copy(source, loaded.at[field], load_sem)
        for field, source in enumerate((u_ref, v_ref))
    ]
    for load in loads:
        load.start()
    pltpu.make_async_copy(loaded, loaded, load_sem).wait()

    low = 2
    high = low + columns
    def lay_out(column):
        for field in range(2):
            state[field, low + column] = jnp.concatenate(
                [
                    loaded[field, pl.ds(tile * columns + column, planes, stride=tiles * columns), :]
                    for tile in range(tiles)
                ],
                axis=1,
            )

    outer_columns = (0, 1, columns - 2, columns - 1)
    for column in outer_columns:
        lay_out(column)

    pl.semaphore_wait(barrier, near_count)

    def send(sender, receiver, source, target, x, y):
        return pltpu.make_async_remote_copy(
            src_ref=source,
            dst_ref=target,
            send_sem=send_sem.at[sender],
            recv_sem=recv_sem.at[receiver],
            device_id=(x, y),
            device_id_type=MESH,
        )

    def wait_sent(sender, ref):
        send(sender, 0, ref, ref, gx, gy).wait_send()

    def wait_got(receiver, ref):
        send(0, receiver, ref, ref, gx, gy).wait_recv()

    def columns_of(first_column, count, part):
        return state.at[:, first_column : first_column + count, :, slice(*spans[part])]

    across = [send(0, 0, packed, got.at[side], across_of[side], gy) for side in range(2)]
    corners_up = [send(0, 1, folded, corner.at[0, side], across_of[side], along_of[0]) for side in range(2)]
    corners_down = [send(0, 2, folded, corner.at[1, side], across_of[side], along_of[1]) for side in range(2)]
    up, down = [
        [
            send(1, receiver + 2 * part, columns_of(source, 2, part), columns_of(target, 2, part), gx, along_of[way])
            for part in parts
        ]
        for receiver, source, target, way in ((1, high - 2, low - 2, 0), (2, low, high, 1))
    ]
    dealt_recv = 1 + 2 * len(widths)

    @pl.when(gy == last)
    def _():
        for x in across_of:
            greet(far, x, 0)

    for peer in range(owners - 2):

        @pl.when(peer < gy - 1)
        def _():
            greet(far, gx, peer)

    up[0].start()

    @pl.when(gy > 0)
    def _():
        down[0].start()

    for column in range(columns):
        if column not in outer_columns:
            lay_out(column)
    lane = lax.broadcasted_iota(jnp.int32, (planes, LANES), 1)
    group = lax.rem(lane + 2, LANES) // 4
    pack = jnp.zeros((planes, LANES), jnp.float32)
    for field in range(2):
        for column in range(columns):
            at = field * columns + column
            tips = jnp.where(
                lane < LANES // 2,
                state[field, low + column, :, :LANES],
                state[field, low + column, :, extent - LANES :],
            )
            tips = pltpu.roll(tips, 4 * at, 1) if at else tips
            pack = jnp.where(group == at, tips, pack)
    packed[...] = pack
    fold = planes // 2
    narrow = lax.broadcasted_iota(jnp.int32, (fold, LANES), 1)
    near_half = lax.rem(narrow + 2, LANES) < LANES // 2
    folded[...] = jnp.where(near_half, pack[:fold], pltpu.roll(pack[fold:], LANES // 2, 1))

    for copy in across + corners_up:
        copy.start()

    @pl.when(gy > 0)
    def _():
        for copy in corners_down:
            copy.start()

    @pl.when((gy > 0) & (gy < last))
    def _():
        for part in parts[1:]:
            down[part].start()

    @pl.when(gy == last)
    def _():
        for part in parts[1:]:
            up[part].start()

    row = lax.broadcasted_iota(jnp.int32, (half, extent), 0)
    fine = lax.broadcasted_iota(jnp.int32, (half, extent), 1)
    to_level = jnp.where(fine // 2 == row, 0.25, 0.0).astype(jnp.bfloat16)

    spreading[...] = spreading_of()

    wait_got(0, got)
    for part in parts[1:]:

        @pl.when(gy < last)
        def _():
            up[part].start()

        @pl.when(gy == last)
        def _():
            down[part].start()


    def merged(below, above):
        return jnp.where(lax.rem(lane[: below.shape[0]], 4) < 2, above, below)

    def unfolded(way):
        tips = merged(corner[way, 0], corner[way, 1])
        return jnp.concatenate([tips, pltpu.roll(tips, LANES // 2, 1)], axis=0)

    def place(c, tips, column):
        for field in range(2):
            at = field * columns + column
            edge[field, c] = pltpu.roll(tips, LANES - 4 * at, 1) if at else tips

    both = merged(got[0], got[1])
    for column in range(columns):
        place(low + column, both, column)

    def wide(field, c, width, outer=()):
        tail = jnp.zeros((planes, LANES), jnp.float32) if c in outer else edge[field, c]
        return jnp.concatenate([state[field, c, :, :width], tail], axis=1)

    def first(c, width, outer=()):
        u, v = wide(0, c, width), wide(1, c, width)
        su = spread_of(wide(0, c - 1, width, outer), u, wide(0, c + 1, width, outer))
        sv = spread_of(wide(1, c - 1, width, outer), v, wide(1, c + 1, width, outer))
        for field, new in enumerate(react(u, v, su, sv)):
            middle[field, c, :, :width] = new[:, :width]
            middle[field, c, :, extent:] = new[:, width:]

    def half_way(field, c, width):
        return jnp.concatenate([middle[field, c, :, :width], middle[field, c, :, extent:]], axis=1)

    def second(c, width):
        u, v = half_way(0, c, width), half_way(1, c, width)
        su = spread_of(half_way(0, c - 1, width), u, half_way(0, c + 1, width))
        sv = spread_of(half_way(1, c - 1, width), v, half_way(1, c + 1, width))
        return react(u[:, :width], v[:, :width], su[:, :width], sv[:, :width])

    def pair(k, c, width=extent, own=True, slot=0):
        new = [second(c, width), second(c + 1, width)]
        for field, out in enumerate((u_out, v_out)):
            for tile in range(width // LANES):
                lanes = slice(tile * LANES, (tile + 1) * LANES)
                both_of = [new[i][field][:, lanes] for i in range(2)]
                if own:
                    for i in range(2):
                        rows = pl.ds(tile * columns + c - low + i, planes, stride=tiles * columns)
                        out[rows, :] = both_of[i]
                rows = pl.ds(field * planes * pairs + k, planes, stride=pairs)
                sums[slot, tile, rows, :] = both_of[0] + both_of[1]

    def side_of_pair(c, before, after, width, slot):
        here, near = [], []
        for field in range(2):
            here.append(half_way(field, c, width))
            near.append([None if at is None else half_way(field, at, width) for at in (before, after)])
        spread = [spread_of(near[field][0], here[field], near[field][1])[:, :width] for field in range(2)]
        inner = [here[field][:, :width] for field in range(2)]
        new = react(inner[0], inner[1], spread[0], spread[1])
        for field, diffusion in enumerate((substrate_diffusion, catalyst_diffusion)):
            total = new[field] + diffusion * inner[field]
            for tile in range(width // LANES):
                rows = pl.ds(field * planes * pairs + pairs - 1, planes, stride=pairs)
                sums[slot, tile, rows, :] = total[:, tile * LANES : (tile + 1) * LANES]

    final = len(widths) - 1

    def wait_side(way, part):
        if part == 0:
            wait_got(1 + way, state.at[:, 0:5, :fold, :LANES])
        else:
            up[part].wait_recv() if way == 0 else down[part].wait_recv()

    def sides(part, below=True, above=True, wrapped=False):
        width = widths[part]
        if below:
            wait_side(0, part)
            if part == 0:
                beyond = unfolded(0)
                for step in range(1, 3 if wrapped else 2):
                    place(low - step, beyond, columns - step)
        if above:
            wait_side(1, part)
            if part == 0:
                place(high, unfolded(1), 0)
        if below:
            first(low, width)
            first(low - 1, width, () if wrapped else (low - 2,))
        if above:
            first(high - 1, width)
            first(high, width, (high + 1,))
        if below:
            pair(0, low, width, own=part == final, slot=1 if wrapped else 0)
        if above:
            pair(pairs - 1, high - 2, width, own=part == final)

    def level_of(part, slot):
        width = widths[part]
        contract = (((1,), (1,)), ((), ()))
        taking = to_level[: width // 2, :width]
        upper, lower = split(jnp.concatenate([sums[slot, tile] for tile in range(width // LANES)], axis=1))
        level = lax.dot_general(
            jnp.concatenate([taking, taking], axis=1),
            jnp.concatenate([upper, lower], axis=1),
            contract,
            preferred_element_type=jnp.float32,
        )
        for owner in range(*shares[part]):
            outgoing[slot, owner] = level[owner * portion : (owner + 1) * portion]

    def deal(slot, owner):
        target = owners if slot else gy
        return send(2 + slot, dealt_recv, outgoing.at[slot, owner], gathered.at[target], gx, owner)

    for c in range(low + 1, high - 1):
        first(c, extent)
    for k in range(1, pairs - 1):
        pair(k, low + 2 * k)

    @pl.when(gy == last)
    def _():
        side_of_pair(high - 2, high - 3, None, extent, 0)

    for part in parts:

        @pl.when((gy > 0) & (gy < last))
        def _():
            sides(part)

        @pl.when(gy == last)
        def _():
            sides(part, above=False)

        @pl.when(gy == 0)
        def _():
            sides(part, below=False)

        if part == 0:

            @pl.when(gy < last - 1)
            def _():
                pl.semaphore_wait(far, far_count)

        if part == 0:

            @pl.when(gy == 0)
            def _():
                for copy in corners_down + down:
                    copy.start()

        level_of(part, 0)
        for owner in range(*shares[part]):

            @pl.when(owner != gy)
            def _():
                deal(0, owner).start()

    @pl.when(gy == 0)
    def _():
        for part in parts:
            sides(part, above=False, wrapped=True)
            side_of_pair(low - 1, None, low, widths[part], 1)
            level_of(part, 1)
            for owner in range(*shares[part]):
                if owner:
                    deal(1, owner).start()

    gathered[gy] = outgoing[0, gy]

    @pl.when(gy == last)
    def _():
        for part in parts[:-1]:
            wait_side(1, part)
            if part == 0:
                place(high, unfolded(1), 0)
        wait_side(1, final)
        if final == 0:
            place(high, unfolded(1), 0)
        first(high - 1, extent)
        first(high, extent, (high + 1,))
        pair(pairs - 1, high - 2)

    @pl.when(gy == 0)
    def _():
        gathered[owners] = outgoing[1, 0]
        wait_got(dealt_recv, gathered.at[1:owners])
        wait_sent(3, outgoing.at[1, 1:])

    @pl.when(gy > 0)
    def _():
        wait_got(dealt_recv, gathered.at[:owners])

    wait_sent(0, state.at[:, 0:2, :, :LANES])
    wait_sent(1, state.at[:, 0:4])
    wait_sent(2, outgoing.at[0, 1:])


def finish(u_ref, v_ref, dealt, spreading, u_out, v_out, rebuilt_out, doubled, paired, rebuilt, sems):
    copies = [
        pltpu.make_async_copy(u_ref, u_out, sems.at[0]),
        pltpu.make_async_copy(v_ref, v_out, sems.at[1]),
    ]
    for copy in copies:
        copy.start()

    owners, portion = dealt.shape[0] - 1, dealt.shape[1]
    lane = lax.broadcasted_iota(jnp.int32, (portion, LANES), 1)
    even = lax.broadcasted_iota(jnp.int32, (portion, LANES), 0) % 2 == 0
    blocks = [dealt[owner] for owner in range(owners)]
    blocks[0] = jnp.where(lane % 4 == 0, dealt[owners], blocks[0])
    blocks[-1] = jnp.where(lane % 4 == 3, blocks[-1] + dealt[owners], blocks[-1])
    width, rows = rebuilt.shape[1], 2 * portion
    chunks = 4
    share = 8 // chunks
    for chunk in range(chunks):
        for h in range(chunk * share, (chunk + 1) * share):
            part = jnp.zeros((portion, LANES), jnp.float32)
            for owner in range(8):
                shift = (16 * (owner - h)) % LANES
                moved = pltpu.roll(blocks[owner], shift, 1) if shift else blocks[owner]
                part = jnp.where(lane // 16 == owner, moved, part)
            other = jnp.where(even, pltpu.roll(part, portion - 1, 0), pltpu.roll(part, 1, 0))
            total = part + other
            for twin in range(2):
                doubled[pl.ds(h * rows + twin, portion, stride=2), :] = part
                paired[pl.ds(h * rows + twin, portion, stride=2), :] = total
        span = slice(chunk * share * rows, (chunk + 1) * share * rows)
        high, low = split(jnp.concatenate([doubled[span, :], paired[span, :]], axis=1))
        whole = jnp.dot(
            jnp.concatenate([high, low], axis=1),
            jnp.concatenate([spreading[...], spreading[...]], axis=0),
            preferred_element_type=jnp.float32,
        )
        for h in range(share):
            for z in range(4):
                base = ((chunk * share + h) * 4 + z) * rows
                rebuilt[base : base + rows, :] = whole[
                    h * rows : (h + 1) * rows, z * LANES : z * LANES + width
                ]
        size = share * 4 * rows
        copies.append(
            pltpu.make_async_copy(
                rebuilt.at[chunk * size : (chunk + 1) * size],
                rebuilt_out.at[chunk * size : (chunk + 1) * size],
                sems.at[2],
            )
        )
        copies[-1].start()
    for copy in copies[:2] + [pltpu.make_async_copy(rebuilt, rebuilt_out, sems.at[2])]:
        copy.wait()


def tiled(field):
    planes, columns, extent = field.shape
    field = field.reshape(planes, columns, extent // LANES, LANES)
    return jnp.transpose(field, (0, 2, 1, 3)).reshape(-1, LANES)


def untiled(field, shape):
    planes, columns, extent = shape
    field = field.reshape(planes, extent // LANES, columns, LANES)
    return jnp.transpose(field, (0, 2, 1, 3)).reshape(shape)


def body(substrate, catalyst):
    planes, columns, extent = substrate.shape
    slabs_x, owners = lax.axis_size("gx"), lax.axis_size("gy")
    half, pairs, tiles = extent // 2, columns // 2, extent // LANES
    portion = half // owners
    values = 2 * planes * pairs
    fused = (
        planes == 16 and pairs == 4 and owners == 8 and values == LANES and portion % 8 == 0
    )
    dims = (planes, columns, extent, owners, slabs_x)
    f32 = jnp.float32
    flat = (planes * tiles * columns, LANES)
    vmem = pl.BlockSpec(memory_space=pltpu.VMEM)
    anywhere = pl.BlockSpec(memory_space=pl.ANY)
    u, v, dealt, spreading = pl.pallas_call(
        functools.partial(kernel, dims),
        out_shape=(
            pltpu.VMEM(flat, f32),
            pltpu.VMEM(flat, f32),
            pltpu.VMEM((owners + 1, portion, values), f32),
            pltpu.VMEM((2 * LANES, 4 * LANES), jnp.bfloat16),
        ),
        in_specs=[anywhere] * 2,
        out_specs=(vmem,) * 4,
        scratch_shapes=[
            pltpu.VMEM((2,) + flat, f32),
            pltpu.VMEM((2, columns + 4, planes, extent), f32),
            pltpu.VMEM((2, columns + 4, planes, LANES), f32),
            pltpu.VMEM((planes, LANES), f32),
            pltpu.VMEM((planes // 2, LANES), f32),
            pltpu.VMEM((2, planes, LANES), f32),
            pltpu.VMEM((2, 2, planes // 2, LANES), f32),
            pltpu.VMEM((2, columns + 4, planes, extent + LANES), f32),
            pltpu.VMEM((2, tiles, values, LANES), f32),
            pltpu.VMEM((2, owners, portion, values), f32),
            pltpu.SemaphoreType.DMA,
            pltpu.SemaphoreType.DMA((4,)),
            pltpu.SemaphoreType.DMA((6 if tiles > 1 else 4,)),
            pltpu.SemaphoreType.REGULAR,
        ],
        compiler_params=pltpu.CompilerParams(collective_id=0, has_side_effects=True),
    )(tiled(substrate), tiled(catalyst))
    rows, width = 2 * portion, columns * owners
    if fused:
        u, v, dealt, spreading = (
            pltpu.with_memory_space_constraint(x, pltpu.VMEM) for x in (u, v, dealt, spreading)
        )
        u, v, rebuilt = pl.pallas_call(
            finish,
            out_shape=(
                jax.ShapeDtypeStruct(flat, f32),
                jax.ShapeDtypeStruct(flat, f32),
                jax.ShapeDtypeStruct((2 * planes * rows, width), f32),
            ),
            in_specs=[vmem] * 4,
            out_specs=(anywhere,) * 3,
            scratch_shapes=[
                pltpu.VMEM((8 * rows, LANES), f32),
                pltpu.VMEM((8 * rows, LANES), f32),
                pltpu.VMEM((2 * planes * rows, width), f32),
                pltpu.SemaphoreType.DMA((3,)),
            ],
        )(u, v, dealt, spreading)
        rebuilt = rebuilt.reshape(2, planes, rows, width)
    else:
        level = dealt.reshape(owners + 1, portion, 2, planes, pairs)
        outer = level[owners]
        lowest = jnp.concatenate([outer[..., :1], level[0, ..., 1:]], axis=-1)
        highest = level[owners - 1]
        highest = jnp.concatenate([highest[..., :-1], highest[..., -1:] + outer[..., -1:]], axis=-1)
        level = jnp.concatenate([lowest[None], level[1 : owners - 1], highest[None]], axis=0)
        level = jnp.transpose(level, (2, 3, 1, 0, 4)).reshape(2, planes, portion // 2, 2, columns * owners // 4, 2)
        coarse = 0.25 * jnp.sum(level, axis=(3, 5), keepdims=True)
        blend = (coarse + 0.5 * (level - coarse)).reshape(2, planes, portion, columns * owners // 2)
        rebuilt = jnp.repeat(jnp.repeat(blend, 2, axis=2), 2, axis=3)
    return untiled(u, substrate.shape), untiled(v, substrate.shape), rebuilt


def solution(mesh):
    in_specs = (P(None, "gy", "gx"), P(None, "gy", "gx"))
    out_specs = (P(None, "gy", "gx"), P(None, "gy", "gx"), P(None, None, ("gx", "gy"), None))
    return jax.shard_map(body, mesh=mesh, in_specs=in_specs, out_specs=out_specs, check_vma=False)
```

```python
import functools

import jax
import jax.numpy as jnp
from jax import lax
from jax.experimental import pallas as pl
from jax.experimental.pallas import tpu as pltpu
from jax.sharding import PartitionSpec as P

feed_rate = 0.037
kill_rate = 0.06
substrate_diffusion = 0.15
catalyst_diffusion = 0.08

MESH = pl.DeviceIdType.MESH
LANES = 128


def react(substrate, catalyst, spread_substrate, spread_catalyst):
    reaction = substrate * catalyst * catalyst
    new_substrate = (
        substrate
        + substrate_diffusion * spread_substrate
        - reaction
        + feed_rate * (1.0 - substrate)
    )
    new_catalyst = (
        catalyst
        + catalyst_diffusion * spread_catalyst
        + reaction
        - (feed_rate + kill_rate) * catalyst
    )
    return new_substrate, new_catalyst


def split(value):
    high = value.astype(jnp.bfloat16)
    low = (value - high.astype(jnp.float32)).astype(jnp.bfloat16)
    return high, low


def spread_of(before, here, after):
    planes, extent = here.shape
    total = pltpu.roll(here, 1, 0) + pltpu.roll(here, planes - 1, 0)
    for beside in (before, after):
        total = total if beside is None else total + beside
    total = total + pltpu.roll(here, 1, 1) + pltpu.roll(here, extent - 1, 1)
    return total - 6.0 * here


def spreading_of():
    wide_in = lax.broadcasted_iota(jnp.int32, (LANES, 4 * LANES), 0)
    wide_out = lax.broadcasted_iota(jnp.int32, (LANES, 4 * LANES), 1)
    column_of = wide_in // 16 * 4 + wide_in % 4
    plane = wide_in // 4 % 4 == wide_out // LANES
    return jnp.concatenate(
        [
            jnp.where(plane & (column_of == wide_out % LANES // 2), 0.5, 0.0),
            jnp.where(plane & (column_of // 2 == wide_out % LANES // 4), 0.125, 0.0),
        ],
        axis=0,
    ).astype(jnp.bfloat16)


def kernel(dims, *refs):
    planes, columns, extent, owners, slabs_x = dims
    (u_ref, v_ref, u_out, v_out, gathered, spreading, loaded, state, edge, packed, folded, got, corner, middle, sums, outgoing,
     load_sem, send_sem, recv_sem, far) = refs
    tiles, pairs, last = extent // LANES, columns // 2, owners - 1
    half = extent // 2
    portion = half // owners
    widths = (LANES, extent) if tiles > 1 else (extent,)
    dealt_to = [(width - 2) // (2 * portion) for width in widths[:-1]] + [owners]
    spans = list(zip((0,) + widths[:-1], widths))
    shares = list(zip([0] + dealt_to[:-1], dealt_to))
    parts = range(len(widths))
    gx, gy = lax.axis_index("gx"), lax.axis_index("gy")
    at_top, at_bottom = gy // last, (last - gy) // last

    barrier = pltpu.get_barrier_semaphore()
    across_of = [lax.rem(gx + shift, slabs_x) for shift in (1, slabs_x - 1)]
    along_of = [lax.rem(gy + shift, owners) for shift in (1, owners - 1)]

    def greet(semaphore, x, y):
        pl.semaphore_signal(semaphore, inc=1, device_id=(x, y), device_id_type=MESH)

    for x in across_of:
        greet(barrier, x, gy)
        greet(barrier, x, along_of[1])

    @pl.when(gy < last)
    def _():
        for x in across_of:
            greet(barrier, x, gy + 1)

    for peer in range(owners):

        @pl.when((peer > gy) | (peer == gy - 1))
        def _():
            greet(barrier, gx, peer)

    near_count = 4 + gy + (1 - at_top) + 2 * (1 - at_bottom)
    far_count = last - gy - 1 + 2 * at_bottom

    loads = [
        pltpu.make_async_copy(source, loaded.at[field], load_sem)
        for field, source in enumerate((u_ref, v_ref))
    ]
    for load in loads:
        load.start()
    pltpu.make_async_copy(loaded, loaded, load_sem).wait()

    low = 2
    high = low + columns
    def lay_out(column):
        for field in range(2):
            state[field, low + column] = jnp.concatenate(
                [
                    loaded[field, pl.ds(tile * columns + column, planes, stride=tiles * columns), :]
                    for tile in range(tiles)
                ],
                axis=1,
            )

    outer_columns = (0, 1, columns - 2, columns - 1)
    for column in outer_columns:
        lay_out(column)

    pl.semaphore_wait(barrier, near_count)

    def send(sender, receiver, source, target, x, y):
        return pltpu.make_async_remote_copy(
            src_ref=source,
            dst_ref=target,
            send_sem=send_sem.at[sender],
            recv_sem=recv_sem.at[receiver],
            device_id=(x, y),
            device_id_type=MESH,
        )

    def wait_sent(sender, ref):
        send(sender, 0, ref, ref, gx, gy).wait_send()

    def wait_got(receiver, ref):
        send(0, receiver, ref, ref, gx, gy).wait_recv()

    def columns_of(first_column, count, part):
        return state.at[:, first_column : first_column + count, :, slice(*spans[part])]

    across = [send(0, 0, packed, got.at[side], across_of[side], gy) for side in range(2)]
    corners_up = [send(0, 1, folded, corner.at[0, side], across_of[side], along_of[0]) for side in range(2)]
    corners_down = [send(0, 2, folded, corner.at[1, side], across_of[side], along_of[1]) for side in range(2)]
    up, down = [
        [
            send(1, receiver + 2 * part, columns_of(source, 2, part), columns_of(target, 2, part), gx, along_of[way])
            for part in parts
        ]
        for receiver, source, target, way in ((1, high - 2, low - 2, 0), (2, low, high, 1))
    ]
    dealt_recv = 1 + 2 * len(widths)

    @pl.when(gy == last)
    def _():
        for x in across_of:
            greet(far, x, 0)

    for peer in range(owners - 2):

        @pl.when(peer < gy - 1)
        def _():
            greet(far, gx, peer)

    up[0].start()

    @pl.when(gy > 0)
    def _():
        down[0].start()

    for column in range(columns):
        if column not in outer_columns:
            lay_out(column)
    lane = lax.broadcasted_iota(jnp.int32, (planes, LANES), 1)
    group = lax.rem(lane + 2, LANES) // 4
    pack = jnp.zeros((planes, LANES), jnp.float32)
    for field in range(2):
        for column in range(columns):
            at = field * columns + column
            tips = jnp.where(
                lane < LANES // 2,
                state[field, low + column, :, :LANES],
                state[field, low + column, :, extent - LANES :],
            )
            tips = pltpu.roll(tips, 4 * at, 1) if at else tips
            pack = jnp.where(group == at, tips, pack)
    packed[...] = pack
    fold = planes // 2
    narrow = lax.broadcasted_iota(jnp.int32, (fold, LANES), 1)
    near_half = lax.rem(narrow + 2, LANES) < LANES // 2
    folded[...] = jnp.where(near_half, pack[:fold], pltpu.roll(pack[fold:], LANES // 2, 1))

    for copy in across + corners_up:
        copy.start()

    @pl.when(gy > 0)
    def _():
        for copy in corners_down:
            copy.start()

    @pl.when((gy > 0) & (gy < last))
    def _():
        for part in parts[1:]:
            down[part].start()

    @pl.when(gy == last)
    def _():
        for part in parts[1:]:
            up[part].start()

    row = lax.broadcasted_iota(jnp.int32, (half, extent), 0)
    fine = lax.broadcasted_iota(jnp.int32, (half, extent), 1)
    to_level = jnp.where(fine // 2 == row, 0.25, 0.0).astype(jnp.bfloat16)

    spreading[...] = spreading_of()

    wait_got(0, got)
    for part in parts[1:]:

        @pl.when(gy < last)
        def _():
            up[part].start()

        @pl.when(gy == last)
        def _():
            down[part].start()


    def merged(below, above):
        return jnp.where(lax.rem(lane[: below.shape[0]], 4) < 2, above, below)

    def unfolded(way):
        tips = merged(corner[way, 0], corner[way, 1])
        return jnp.concatenate([tips, pltpu.roll(tips, LANES // 2, 1)], axis=0)

    def place(c, tips, column):
        for field in range(2):
            at = field * columns + column
            edge[field, c] = pltpu.roll(tips, LANES - 4 * at, 1) if at else tips

    both = merged(got[0], got[1])
    for column in range(columns):
        place(low + column, both, column)

    def wide(field, c, width, outer=()):
        tail = jnp.zeros((planes, LANES), jnp.float32) if c in outer else edge[field, c]
        return jnp.concatenate([state[field, c, :, :width], tail], axis=1)

    def first(c, width, outer=()):
        u, v = wide(0, c, width), wide(1, c, width)
        su = spread_of(wide(0, c - 1, width, outer), u, wide(0, c + 1, width, outer))
        sv = spread_of(wide(1, c - 1, width, outer), v, wide(1, c + 1, width, outer))
        for field, new in enumerate(react(u, v, su, sv)):
            middle[field, c, :, :width] = new[:, :width]
            middle[field, c, :, extent:] = new[:, width:]

    def half_way(field, c, width):
        return jnp.concatenate([middle[field, c, :, :width], middle[field, c, :, extent:]], axis=1)

    def second(c, width):
        u, v = half_way(0, c, width), half_way(1, c, width)
        su = spread_of(half_way(0, c - 1, width), u, half_way(0, c + 1, width))
        sv = spread_of(half_way(1, c - 1, width), v, half_way(1, c + 1, width))
        return react(u[:, :width], v[:, :width], su[:, :width], sv[:, :width])

    def pair(k, c, width=extent, own=True, slot=0):
        new = [second(c, width), second(c + 1, width)]
        for field, out in enumerate((u_out, v_out)):
            for tile in range(width // LANES):
                lanes = slice(tile * LANES, (tile + 1) * LANES)
                both_of = [new[i][field][:, lanes] for i in range(2)]
                if own:
                    for i in range(2):
                        rows = pl.ds(tile * columns + c - low + i, planes, stride=tiles * columns)
                        out[rows, :] = both_of[i]
                rows = pl.ds(field * planes * pairs + k, planes, stride=pairs)
                sums[slot, tile, rows, :] = both_of[0] + both_of[1]

    def side_of_pair(c, before, after, width, slot):
        here, near = [], []
        for field in range(2):
            here.append(half_way(field, c, width))
            near.append([None if at is None else half_way(field, at, width) for at in (before, after)])
        spread = [spread_of(near[field][0], here[field], near[field][1])[:, :width] for field in range(2)]
        inner = [here[field][:, :width] for field in range(2)]
        new = react(inner[0], inner[1], spread[0], spread[1])
        for field, diffusion in enumerate((substrate_diffusion, catalyst_diffusion)):
            total = new[field] + diffusion * inner[field]
            for tile in range(width // LANES):
                rows = pl.ds(field * planes * pairs + pairs - 1, planes, stride=pairs)
                sums[slot, tile, rows, :] = total[:, tile * LANES : (tile + 1) * LANES]

    final = len(widths) - 1

    def wait_side(way, part):
        if part == 0:
            wait_got(1 + way, state.at[:, 0:5, :fold, :LANES])
        else:
            up[part].wait_recv() if way == 0 else down[part].wait_recv()

    def sides(part, below=True, above=True, wrapped=False):
        width = widths[part]
        if below:
            wait_side(0, part)
            if part == 0:
                beyond = unfolded(0)
                for step in range(1, 3 if wrapped else 2):
                    place(low - step, beyond, columns - step)
        if above:
            wait_side(1, part)
            if part == 0:
                place(high, unfolded(1), 0)
        if below:
            first(low, width)
            first(low - 1, width, () if wrapped else (low - 2,))
        if above:
            first(high - 1, width)
            first(high, width, (high + 1,))
        if below:
            pair(0, low, width, own=part == final, slot=1 if wrapped else 0)
        if above:
            pair(pairs - 1, high - 2, width, own=part == final)

    def level_of(part, slot):
        width = widths[part]
        contract = (((1,), (1,)), ((), ()))
        taking = to_level[: width // 2, :width]
        upper, lower = split(jnp.concatenate([sums[slot, tile] for tile in range(width // LANES)], axis=1))
        level = lax.dot_general(
            jnp.concatenate([taking, taking], axis=1),
            jnp.concatenate([upper, lower], axis=1),
            contract,
            preferred_element_type=jnp.float32,
        )
        for owner in range(*shares[part]):
            outgoing[slot, owner] = level[owner * portion : (owner + 1) * portion]

    def deal(slot, owner):
        target = owners if slot else gy
        return send(2 + slot, dealt_recv, outgoing.at[slot, owner], gathered.at[target], gx, owner)

    for c in range(low + 1, high - 1):
        first(c, extent)
    for k in range(1, pairs - 1):
        pair(k, low + 2 * k)

    @pl.when(gy == last)
    def _():
        side_of_pair(high - 2, high - 3, None, extent, 0)

    for part in parts:

        @pl.when((gy > 0) & (gy < last))
        def _():
            sides(part)

        @pl.when(gy == last)
        def _():
            sides(part, above=False)

        @pl.when(gy == 0)
        def _():
            sides(part, below=False)

        if part == 0:

            @pl.when(gy < last - 1)
            def _():
                pl.semaphore_wait(far, far_count)

        if part == 0:

            @pl.when(gy == 0)
            def _():
                for copy in corners_down + down:
                    copy.start()

        level_of(part, 0)
        for owner in range(*shares[part]):

            @pl.when(owner != gy)
            def _():
                deal(0, owner).start()

    @pl.when(gy == 0)
    def _():
        for part in parts:
            sides(part, above=False, wrapped=True)
            side_of_pair(low - 1, None, low, widths[part], 1)
            level_of(part, 1)
            for owner in range(*shares[part]):
                if owner:
                    deal(1, owner).start()

    gathered[gy] = outgoing[0, gy]

    @pl.when(gy == last)
    def _():
        for part in parts[:-1]:
            wait_side(1, part)
            if part == 0:
                place(high, unfolded(1), 0)
        wait_side(1, final)
        if final == 0:
            place(high, unfolded(1), 0)
        first(high - 1, extent)
        first(high, extent, (high + 1,))
        pair(pairs - 1, high - 2)

    @pl.when(gy == 0)
    def _():
        gathered[owners] = outgoing[1, 0]
        wait_got(dealt_recv, gathered.at[1:owners])
        wait_sent(3, outgoing.at[1, 1:])

    @pl.when(gy > 0)
    def _():
        wait_got(dealt_recv, gathered.at[:owners])

    wait_sent(0, state.at[:, 0:2, :, :LANES])
    wait_sent(1, state.at[:, 0:4])
    wait_sent(2, outgoing.at[0, 1:])


def finish(u_ref, v_ref, dealt, spreading, u_out, v_out, rebuilt_out, doubled, paired, rebuilt, sems):
    copies = [
        pltpu.make_async_copy(u_ref, u_out, sems.at[0]),
        pltpu.make_async_copy(v_ref, v_out, sems.at[1]),
    ]
    for copy in copies:
        copy.start()

    owners, portion = dealt.shape[0] - 1, dealt.shape[1]
    lane = lax.broadcasted_iota(jnp.int32, (portion, LANES), 1)
    even = lax.broadcasted_iota(jnp.int32, (portion, LANES), 0) % 2 == 0
    blocks = [dealt[owner] for owner in range(owners)]
    blocks[0] = jnp.where(lane % 4 == 0, dealt[owners], blocks[0])
    blocks[-1] = jnp.where(lane % 4 == 3, blocks[-1] + dealt[owners], blocks[-1])
    width, rows = rebuilt.shape[1], 2 * portion
    groups, quarters = 8, 4
    for h in range(groups):
        part = jnp.zeros((portion, LANES), jnp.float32)
        for owner in range(8):
            shift = (16 * (owner - h)) % LANES
            moved = pltpu.roll(blocks[owner], shift, 1) if shift else blocks[owner]
            part = jnp.where(lane // 16 == owner, moved, part)
        other = jnp.where(even, pltpu.roll(part, portion - 1, 0), pltpu.roll(part, 1, 0))
        total = part + other
        for twin in range(2):
            doubled[pl.ds(h * rows + twin, portion, stride=2), :] = part
            paired[pl.ds(h * rows + twin, portion, stride=2), :] = total
    high, low = split(jnp.concatenate([doubled[...], paired[...]], axis=1))
    whole = jnp.dot(
        jnp.concatenate([high, low], axis=1),
        jnp.concatenate([spreading[...], spreading[...]], axis=0),
        preferred_element_type=jnp.float32,
    )
    size = groups // quarters * 4 * rows
    for quarter in range(quarters):
        for h in range(quarter * groups // quarters, (quarter + 1) * groups // quarters):
            for z in range(4):
                base = (h * 4 + z) * rows
                rebuilt[base : base + rows, :] = whole[
                    h * rows : (h + 1) * rows, z * LANES : z * LANES + width
                ]
        copies.append(
            pltpu.make_async_copy(
                rebuilt.at[quarter * size : (quarter + 1) * size],
                rebuilt_out.at[quarter * size : (quarter + 1) * size],
                sems.at[2],
            )
        )
        copies[-1].start()
    for copy in copies[:2] + [pltpu.make_async_copy(rebuilt, rebuilt_out, sems.at[2])]:
        copy.wait()


def tiled(field):
    planes, columns, extent = field.shape
    field = field.reshape(planes, columns, extent // LANES, LANES)
    return jnp.transpose(field, (0, 2, 1, 3)).reshape(-1, LANES)


def untiled(field, shape):
    planes, columns, extent = shape
    field = field.reshape(planes, extent // LANES, columns, LANES)
    return jnp.transpose(field, (0, 2, 1, 3)).reshape(shape)


def body(substrate, catalyst):
    planes, columns, extent = substrate.shape
    slabs_x, owners = lax.axis_size("gx"), lax.axis_size("gy")
    half, pairs, tiles = extent // 2, columns // 2, extent // LANES
    portion = half // owners
    values = 2 * planes * pairs
    fused = (
        planes == 16 and pairs == 4 and owners == 8 and values == LANES and portion % 8 == 0
    )
    dims = (planes, columns, extent, owners, slabs_x)
    f32 = jnp.float32
    flat = (planes * tiles * columns, LANES)
    vmem = pl.BlockSpec(memory_space=pltpu.VMEM)
    anywhere = pl.BlockSpec(memory_space=pl.ANY)
    u, v, dealt, spreading = pl.pallas_call(
        functools.partial(kernel, dims),
        out_shape=(
            pltpu.VMEM(flat, f32),
            pltpu.VMEM(flat, f32),
            pltpu.VMEM((owners + 1, portion, values), f32),
            pltpu.VMEM((2 * LANES, 4 * LANES), jnp.bfloat16),
        ),
        in_specs=[anywhere] * 2,
        out_specs=(vmem,) * 4,
        scratch_shapes=[
            pltpu.VMEM((2,) + flat, f32),
            pltpu.VMEM((2, columns + 4, planes, extent), f32),
            pltpu.VMEM((2, columns + 4, planes, LANES), f32),
            pltpu.VMEM((planes, LANES), f32),
            pltpu.VMEM((planes // 2, LANES), f32),
            pltpu.VMEM((2, planes, LANES), f32),
            pltpu.VMEM((2, 2, planes // 2, LANES), f32),
            pltpu.VMEM((2, columns + 4, planes, extent + LANES), f32),
            pltpu.VMEM((2, tiles, values, LANES), f32),
            pltpu.VMEM((2, owners, portion, values), f32),
            pltpu.SemaphoreType.DMA,
            pltpu.SemaphoreType.DMA((4,)),
            pltpu.SemaphoreType.DMA((6 if tiles > 1 else 4,)),
            pltpu.SemaphoreType.REGULAR,
        ],
        compiler_params=pltpu.CompilerParams(collective_id=0, has_side_effects=True),
    )(tiled(substrate), tiled(catalyst))
    rows, width = 2 * portion, columns * owners
    if fused:
        u, v, dealt, spreading = (
            pltpu.with_memory_space_constraint(x, pltpu.VMEM) for x in (u, v, dealt, spreading)
        )
        u, v, rebuilt = pl.pallas_call(
            finish,
            out_shape=(
                jax.ShapeDtypeStruct(flat, f32),
                jax.ShapeDtypeStruct(flat, f32),
                jax.ShapeDtypeStruct((2 * planes * rows, width), f32),
            ),
            in_specs=[vmem] * 4,
            out_specs=(anywhere,) * 3,
            scratch_shapes=[
                pltpu.VMEM((8 * rows, LANES), f32),
                pltpu.VMEM((8 * rows, LANES), f32),
                pltpu.VMEM((2 * planes * rows, width), f32),
                pltpu.SemaphoreType.DMA((3,)),
            ],
        )(u, v, dealt, spreading)
        rebuilt = rebuilt.reshape(2, planes, rows, width)
    else:
        level = dealt.reshape(owners + 1, portion, 2, planes, pairs)
        outer = level[owners]
        lowest = jnp.concatenate([outer[..., :1], level[0, ..., 1:]], axis=-1)
        highest = level[owners - 1]
        highest = jnp.concatenate([highest[..., :-1], highest[..., -1:] + outer[..., -1:]], axis=-1)
        level = jnp.concatenate([lowest[None], level[1 : owners - 1], highest[None]], axis=0)
        level = jnp.transpose(level, (2, 3, 1, 0, 4)).reshape(2, planes, portion // 2, 2, columns * owners // 4, 2)
        coarse = 0.25 * jnp.sum(level, axis=(3, 5), keepdims=True)
        blend = (coarse + 0.5 * (level - coarse)).reshape(2, planes, portion, columns * owners // 2)
        rebuilt = jnp.repeat(jnp.repeat(blend, 2, axis=2), 2, axis=3)
    return untiled(u, substrate.shape), untiled(v, substrate.shape), rebuilt


def solution(mesh):
    in_specs = (P(None, "gy", "gx"), P(None, "gy", "gx"))
    out_specs = (P(None, "gy", "gx"), P(None, "gy", "gx"), P(None, None, ("gx", "gy"), None))
    return jax.shard_map(body, mesh=mesh, in_specs=in_specs, out_specs=out_specs, check_vma=False)
```

```python
import functools

import jax
import jax.numpy as jnp
from jax import lax
from jax.experimental import pallas as pl
from jax.experimental.pallas import tpu as pltpu
from jax.sharding import PartitionSpec as P

feed_rate = 0.037
kill_rate = 0.06
substrate_diffusion = 0.15
catalyst_diffusion = 0.08

MESH = pl.DeviceIdType.MESH
LANES = 128


def react(substrate, catalyst, spread_substrate, spread_catalyst):
    reaction = substrate * catalyst * catalyst
    new_substrate = (
        substrate
        + substrate_diffusion * spread_substrate
        - reaction
        + feed_rate * (1.0 - substrate)
    )
    new_catalyst = (
        catalyst
        + catalyst_diffusion * spread_catalyst
        + reaction
        - (feed_rate + kill_rate) * catalyst
    )
    return new_substrate, new_catalyst


def split(value):
    high = value.astype(jnp.bfloat16)
    low = (value - high.astype(jnp.float32)).astype(jnp.bfloat16)
    return high, low


def spread_of(before, here, after):
    planes, extent = here.shape
    total = pltpu.roll(here, 1, 0) + pltpu.roll(here, planes - 1, 0)
    for beside in (before, after):
        total = total if beside is None else total + beside
    total = total + pltpu.roll(here, 1, 1) + pltpu.roll(here, extent - 1, 1)
    return total - 6.0 * here


def spreading_of():
    wide_in = lax.broadcasted_iota(jnp.int32, (LANES, 4 * LANES), 0)
    wide_out = lax.broadcasted_iota(jnp.int32, (LANES, 4 * LANES), 1)
    column_of = wide_in // 16 * 4 + wide_in % 4
    plane = wide_in // 4 % 4 == wide_out // LANES
    return jnp.concatenate(
        [
            jnp.where(plane & (column_of == wide_out % LANES // 2), 0.5, 0.0),
            jnp.where(plane & (column_of // 2 == wide_out % LANES // 4), 0.125, 0.0),
        ],
        axis=0,
    ).astype(jnp.bfloat16)


def kernel(dims, *refs):
    planes, columns, extent, owners, slabs_x = dims
    (u_ref, v_ref, u_out, v_out, gathered, spreading, loaded, state, edge, packed, folded, got, corner, middle, sums, outgoing,
     load_sem, send_sem, recv_sem, far) = refs
    tiles, pairs, last = extent // LANES, columns // 2, owners - 1
    half = extent // 2
    portion = half // owners
    widths = (LANES, extent) if tiles > 1 else (extent,)
    dealt_to = [(width - 2) // (2 * portion) for width in widths[:-1]] + [owners]
    spans = list(zip((0,) + widths[:-1], widths))
    shares = list(zip([0] + dealt_to[:-1], dealt_to))
    parts = range(len(widths))
    gx, gy = lax.axis_index("gx"), lax.axis_index("gy")
    at_top, at_bottom = gy // last, (last - gy) // last

    barrier = pltpu.get_barrier_semaphore()
    across_of = [lax.rem(gx + shift, slabs_x) for shift in (1, slabs_x - 1)]
    along_of = [lax.rem(gy + shift, owners) for shift in (1, owners - 1)]

    def greet(semaphore, x, y):
        pl.semaphore_signal(semaphore, inc=1, device_id=(x, y), device_id_type=MESH)

    for x in across_of:
        greet(barrier, x, gy)
        greet(barrier, x, along_of[1])

    @pl.when(gy < last)
    def _():
        for x in across_of:
            greet(barrier, x, gy + 1)

    for peer in range(owners):

        @pl.when((peer > gy) | (peer == gy - 1))
        def _():
            greet(barrier, gx, peer)

    near_count = 4 + gy + (1 - at_top) + 2 * (1 - at_bottom)
    far_count = last - gy - 1 + 2 * at_bottom

    loads = [
        pltpu.make_async_copy(source, loaded.at[field], load_sem)
        for field, source in enumerate((u_ref, v_ref))
    ]
    for load in loads:
        load.start()
    pltpu.make_async_copy(loaded, loaded, load_sem).wait()

    low = 2
    high = low + columns
    def lay_out(column):
        for field in range(2):
            state[field, low + column] = jnp.concatenate(
                [
                    loaded[field, pl.ds(tile * columns + column, planes, stride=tiles * columns), :]
                    for tile in range(tiles)
                ],
                axis=1,
            )

    outer_columns = (0, 1, columns - 2, columns - 1)
    for column in outer_columns:
        lay_out(column)

    pl.semaphore_wait(barrier, near_count)

    def send(sender, receiver, source, target, x, y):
        return pltpu.make_async_remote_copy(
            src_ref=source,
            dst_ref=target,
            send_sem=send_sem.at[sender],
            recv_sem=recv_sem.at[receiver],
            device_id=(x, y),
            device_id_type=MESH,
        )

    def wait_sent(sender, ref):
        send(sender, 0, ref, ref, gx, gy).wait_send()

    def wait_got(receiver, ref):
        send(0, receiver, ref, ref, gx, gy).wait_recv()

    def columns_of(first_column, count, part):
        return state.at[:, first_column : first_column + count, :, slice(*spans[part])]

    across = [send(0, 0, packed, got.at[side], across_of[side], gy) for side in range(2)]
    corners_up = [send(0, 1, folded, corner.at[0, side], across_of[side], along_of[0]) for side in range(2)]
    corners_down = [send(0, 2, folded, corner.at[1, side], across_of[side], along_of[1]) for side in range(2)]
    up, down = [
        [
            send(0, receiver + 2 * part, columns_of(source, 2, part), columns_of(target, 2, part), gx, along_of[way])
            for part in parts
        ]
        for receiver, source, target, way in ((1, high - 2, low - 2, 0), (2, low, high, 1))
    ]
    dealt_recv = 1 + 2 * len(widths)

    @pl.when(gy == last)
    def _():
        for x in across_of:
            greet(far, x, 0)

    for peer in range(owners - 2):

        @pl.when(peer < gy - 1)
        def _():
            greet(far, gx, peer)

    up[0].start()

    @pl.when(gy > 0)
    def _():
        down[0].start()

    for column in range(columns):
        if column not in outer_columns:
            lay_out(column)
    lane = lax.broadcasted_iota(jnp.int32, (planes, LANES), 1)
    group = lax.rem(lane + 2, LANES) // 4
    pack = jnp.zeros((planes, LANES), jnp.float32)
    for field in range(2):
        for column in range(columns):
            at = field * columns + column
            tips = jnp.where(
                lane < LANES // 2,
                state[field, low + column, :, :LANES],
                state[field, low + column, :, extent - LANES :],
            )
            tips = pltpu.roll(tips, 4 * at, 1) if at else tips
            pack = jnp.where(group == at, tips, pack)
    packed[...] = pack
    fold = planes // 2
    narrow = lax.broadcasted_iota(jnp.int32, (fold, LANES), 1)
    near_half = lax.rem(narrow + 2, LANES) < LANES // 2
    folded[...] = jnp.where(near_half, pack[:fold], pltpu.roll(pack[fold:], LANES // 2, 1))

    for copy in across + corners_up:
        copy.start()

    @pl.when(gy > 0)
    def _():
        for copy in corners_down:
            copy.start()

    @pl.when((gy > 0) & (gy < last))
    def _():
        for part in parts[1:]:
            down[part].start()

    @pl.when(gy == last)
    def _():
        for part in parts[1:]:
            up[part].start()

    row = lax.broadcasted_iota(jnp.int32, (half, extent), 0)
    fine = lax.broadcasted_iota(jnp.int32, (half, extent), 1)
    to_level = jnp.where(fine // 2 == row, 0.25, 0.0).astype(jnp.bfloat16)

    spreading[...] = spreading_of()

    wait_got(0, got)
    for part in parts[1:]:

        @pl.when(gy < last)
        def _():
            up[part].start()

        @pl.when(gy == last)
        def _():
            down[part].start()


    def merged(below, above):
        return jnp.where(lax.rem(lane[: below.shape[0]], 4) < 2, above, below)

    def unfolded(way):
        tips = merged(corner[way, 0], corner[way, 1])
        return jnp.concatenate([tips, pltpu.roll(tips, LANES // 2, 1)], axis=0)

    def place(c, tips, column):
        for field in range(2):
            at = field * columns + column
            edge[field, c] = pltpu.roll(tips, LANES - 4 * at, 1) if at else tips

    both = merged(got[0], got[1])
    for column in range(columns):
        place(low + column, both, column)

    def wide(field, c, width, outer=()):
        tail = jnp.zeros((planes, LANES), jnp.float32) if c in outer else edge[field, c]
        return jnp.concatenate([state[field, c, :, :width], tail], axis=1)

    def first(c, width, outer=()):
        u, v = wide(0, c, width), wide(1, c, width)
        su = spread_of(wide(0, c - 1, width, outer), u, wide(0, c + 1, width, outer))
        sv = spread_of(wide(1, c - 1, width, outer), v, wide(1, c + 1, width, outer))
        for field, new in enumerate(react(u, v, su, sv)):
            middle[field, c, :, :width] = new[:, :width]
            middle[field, c, :, extent:] = new[:, width:]

    def half_way(field, c, width):
        return jnp.concatenate([middle[field, c, :, :width], middle[field, c, :, extent:]], axis=1)

    def second(c, width):
        u, v = half_way(0, c, width), half_way(1, c, width)
        su = spread_of(half_way(0, c - 1, width), u, half_way(0, c + 1, width))
        sv = spread_of(half_way(1, c - 1, width), v, half_way(1, c + 1, width))
        return react(u[:, :width], v[:, :width], su[:, :width], sv[:, :width])

    def pair(k, c, width=extent, own=True, slot=0):
        new = [second(c, width), second(c + 1, width)]
        for field, out in enumerate((u_out, v_out)):
            for tile in range(width // LANES):
                lanes = slice(tile * LANES, (tile + 1) * LANES)
                both_of = [new[i][field][:, lanes] for i in range(2)]
                if own:
                    for i in range(2):
                        rows = pl.ds(tile * columns + c - low + i, planes, stride=tiles * columns)
                        out[rows, :] = both_of[i]
                rows = pl.ds(field * planes * pairs + k, planes, stride=pairs)
                sums[slot, tile, rows, :] = both_of[0] + both_of[1]

    def side_of_pair(c, before, after, width, slot):
        here, near = [], []
        for field in range(2):
            here.append(half_way(field, c, width))
            near.append([None if at is None else half_way(field, at, width) for at in (before, after)])
        spread = [spread_of(near[field][0], here[field], near[field][1])[:, :width] for field in range(2)]
        inner = [here[field][:, :width] for field in range(2)]
        new = react(inner[0], inner[1], spread[0], spread[1])
        for field, diffusion in enumerate((substrate_diffusion, catalyst_diffusion)):
            total = new[field] + diffusion * inner[field]
            for tile in range(width // LANES):
                rows = pl.ds(field * planes * pairs + pairs - 1, planes, stride=pairs)
                sums[slot, tile, rows, :] = total[:, tile * LANES : (tile + 1) * LANES]

    final = len(widths) - 1

    def wait_side(way, part):
        if part == 0:
            wait_got(1 + way, state.at[:, 0:5, :fold, :LANES])
        else:
            up[part].wait_recv() if way == 0 else down[part].wait_recv()

    def sides(part, below=True, above=True, wrapped=False):
        width = widths[part]
        if below:
            wait_side(0, part)
            if part == 0:
                beyond = unfolded(0)
                for step in range(1, 3 if wrapped else 2):
                    place(low - step, beyond, columns - step)
        if above:
            wait_side(1, part)
            if part == 0:
                place(high, unfolded(1), 0)
        if below:
            first(low, width)
            first(low - 1, width, () if wrapped else (low - 2,))
        if above:
            first(high - 1, width)
            first(high, width, (high + 1,))
        if below:
            pair(0, low, width, own=part == final, slot=1 if wrapped else 0)
        if above:
            pair(pairs - 1, high - 2, width, own=part == final)

    def level_of(part, slot):
        width = widths[part]
        contract = (((1,), (1,)), ((), ()))
        taking = to_level[: width // 2, :width]
        upper, lower = split(jnp.concatenate([sums[slot, tile] for tile in range(width // LANES)], axis=1))
        level = lax.dot_general(
            jnp.concatenate([taking, taking], axis=1),
            jnp.concatenate([upper, lower], axis=1),
            contract,
            preferred_element_type=jnp.float32,
        )
        for owner in range(*shares[part]):
            outgoing[slot, owner] = level[owner * portion : (owner + 1) * portion]

    def deal(slot, owner):
        target = owners if slot else gy
        return send(1 + slot, dealt_recv, outgoing.at[slot, owner], gathered.at[target], gx, owner)

    for c in range(low + 1, high - 1):
        first(c, extent)
    for k in range(1, pairs - 1):
        pair(k, low + 2 * k)

    @pl.when(gy == last)
    def _():
        side_of_pair(high - 2, high - 3, None, extent, 0)

    for part in parts:

        @pl.when((gy > 0) & (gy < last))
        def _():
            sides(part)

        @pl.when(gy == last)
        def _():
            sides(part, above=False)

        @pl.when(gy == 0)
        def _():
            sides(part, below=False)

        if part == 0:

            @pl.when(gy < last - 1)
            def _():
                pl.semaphore_wait(far, far_count)

        if part == 0:

            @pl.when(gy == 0)
            def _():
                for copy in corners_down + down:
                    copy.start()

        level_of(part, 0)
        for owner in range(*shares[part]):

            @pl.when(owner != gy)
            def _():
                deal(0, owner).start()

    @pl.when(gy == 0)
    def _():
        for part in parts:
            sides(part, above=False, wrapped=True)
            side_of_pair(low - 1, None, low, widths[part], 1)
            level_of(part, 1)
            for owner in range(*shares[part]):
                if owner:
                    deal(1, owner).start()

    gathered[gy] = outgoing[0, gy]

    @pl.when(gy == last)
    def _():
        for part in parts[:-1]:
            wait_side(1, part)
            if part == 0:
                place(high, unfolded(1), 0)
        wait_side(1, final)
        if final == 0:
            place(high, unfolded(1), 0)
        first(high - 1, extent)
        first(high, extent, (high + 1,))
        pair(pairs - 1, high - 2)

    @pl.when(gy == 0)
    def _():
        gathered[owners] = outgoing[1, 0]
        wait_got(dealt_recv, gathered.at[1:owners])
        wait_sent(2, outgoing.at[1, 1:])

    @pl.when(gy > 0)
    def _():
        wait_got(dealt_recv, gathered.at[:owners])

    wait_sent(0, state.at[:, 0 : 2 + 4 * tiles, :, :LANES])
    wait_sent(1, outgoing.at[0, 1:])


def finish(u_ref, v_ref, dealt, spreading, u_out, v_out, rebuilt_out, doubled, paired, rebuilt, sems):
    copies = [
        pltpu.make_async_copy(u_ref, u_out, sems.at[0]),
        pltpu.make_async_copy(v_ref, v_out, sems.at[1]),
    ]
    for copy in copies:
        copy.start()

    owners, portion = dealt.shape[0] - 1, dealt.shape[1]
    lane = lax.broadcasted_iota(jnp.int32, (portion, LANES), 1)
    even = lax.broadcasted_iota(jnp.int32, (portion, LANES), 0) % 2 == 0
    blocks = [dealt[owner] for owner in range(owners)]
    blocks[0] = jnp.where(lane % 4 == 0, dealt[owners], blocks[0])
    blocks[-1] = jnp.where(lane % 4 == 3, blocks[-1] + dealt[owners], blocks[-1])
    width, rows = rebuilt.shape[1], 2 * portion
    groups, quarters = 8, 4
    for h in range(groups):
        part = jnp.zeros((portion, LANES), jnp.float32)
        for owner in range(8):
            shift = (16 * (owner - h)) % LANES
            moved = pltpu.roll(blocks[owner], shift, 1) if shift else blocks[owner]
            part = jnp.where(lane // 16 == owner, moved, part)
        other = jnp.where(even, pltpu.roll(part, portion - 1, 0), pltpu.roll(part, 1, 0))
        total = part + other
        for twin in range(2):
            doubled[pl.ds(h * rows + twin, portion, stride=2), :] = part
            paired[pl.ds(h * rows + twin, portion, stride=2), :] = total
    high, low = split(jnp.concatenate([doubled[...], paired[...]], axis=1))
    whole = jnp.dot(
        jnp.concatenate([high, low], axis=1),
        jnp.concatenate([spreading[...], spreading[...]], axis=0),
        preferred_element_type=jnp.float32,
    )
    size = groups // quarters * 4 * rows
    for quarter in range(quarters):
        for h in range(quarter * groups // quarters, (quarter + 1) * groups // quarters):
            for z in range(4):
                base = (h * 4 + z) * rows
                rebuilt[base : base + rows, :] = whole[
                    h * rows : (h + 1) * rows, z * LANES : z * LANES + width
                ]
        copies.append(
            pltpu.make_async_copy(
                rebuilt.at[quarter * size : (quarter + 1) * size],
                rebuilt_out.at[quarter * size : (quarter + 1) * size],
                sems.at[2],
            )
        )
        copies[-1].start()
    for copy in copies[:2] + [pltpu.make_async_copy(rebuilt, rebuilt_out, sems.at[2])]:
        copy.wait()


def tiled(field):
    planes, columns, extent = field.shape
    field = field.reshape(planes, columns, extent // LANES, LANES)
    return jnp.transpose(field, (0, 2, 1, 3)).reshape(-1, LANES)


def untiled(field, shape):
    planes, columns, extent = shape
    field = field.reshape(planes, extent // LANES, columns, LANES)
    return jnp.transpose(field, (0, 2, 1, 3)).reshape(shape)


def body(substrate, catalyst):
    planes, columns, extent = substrate.shape
    slabs_x, owners = lax.axis_size("gx"), lax.axis_size("gy")
    half, pairs, tiles = extent // 2, columns // 2, extent // LANES
    portion = half // owners
    values = 2 * planes * pairs
    fused = (
        planes == 16 and pairs == 4 and owners == 8 and values == LANES and portion % 8 == 0
    )
    dims = (planes, columns, extent, owners, slabs_x)
    f32 = jnp.float32
    flat = (planes * tiles * columns, LANES)
    vmem = pl.BlockSpec(memory_space=pltpu.VMEM)
    anywhere = pl.BlockSpec(memory_space=pl.ANY)
    u, v, dealt, spreading = pl.pallas_call(
        functools.partial(kernel, dims),
        out_shape=(
            pltpu.VMEM(flat, f32),
            pltpu.VMEM(flat, f32),
            pltpu.VMEM((owners + 1, portion, values), f32),
            pltpu.VMEM((2 * LANES, 4 * LANES), jnp.bfloat16),
        ),
        in_specs=[anywhere] * 2,
        out_specs=(vmem,) * 4,
        scratch_shapes=[
            pltpu.VMEM((2,) + flat, f32),
            pltpu.VMEM((2, columns + 4, planes, extent), f32),
            pltpu.VMEM((2, columns + 4, planes, LANES), f32),
            pltpu.VMEM((planes, LANES), f32),
            pltpu.VMEM((planes // 2, LANES), f32),
            pltpu.VMEM((2, planes, LANES), f32),
            pltpu.VMEM((2, 2, planes // 2, LANES), f32),
            pltpu.VMEM((2, columns + 4, planes, extent + LANES), f32),
            pltpu.VMEM((2, tiles, values, LANES), f32),
            pltpu.VMEM((2, owners, portion, values), f32),
            pltpu.SemaphoreType.DMA,
            pltpu.SemaphoreType.DMA((3,)),
            pltpu.SemaphoreType.DMA((6 if tiles > 1 else 4,)),
            pltpu.SemaphoreType.REGULAR,
        ],
        compiler_params=pltpu.CompilerParams(collective_id=0, has_side_effects=True),
    )(tiled(substrate), tiled(catalyst))
    rows, width = 2 * portion, columns * owners
    if fused:
        u, v, dealt, spreading = (
            pltpu.with_memory_space_constraint(x, pltpu.VMEM) for x in (u, v, dealt, spreading)
        )
        u, v, rebuilt = pl.pallas_call(
            finish,
            out_shape=(
                jax.ShapeDtypeStruct(flat, f32),
                jax.ShapeDtypeStruct(flat, f32),
                jax.ShapeDtypeStruct((2 * planes * rows, width), f32),
            ),
            in_specs=[vmem] * 4,
            out_specs=(anywhere,) * 3,
            scratch_shapes=[
                pltpu.VMEM((8 * rows, LANES), f32),
                pltpu.VMEM((8 * rows, LANES), f32),
                pltpu.VMEM((2 * planes * rows, width), f32),
                pltpu.SemaphoreType.DMA((3,)),
            ],
        )(u, v, dealt, spreading)
        rebuilt = rebuilt.reshape(2, planes, rows, width)
    else:
        level = dealt.reshape(owners + 1, portion, 2, planes, pairs)
        outer = level[owners]
        lowest = jnp.concatenate([outer[..., :1], level[0, ..., 1:]], axis=-1)
        highest = level[owners - 1]
        highest = jnp.concatenate([highest[..., :-1], highest[..., -1:] + outer[..., -1:]], axis=-1)
        level = jnp.concatenate([lowest[None], level[1 : owners - 1], highest[None]], axis=0)
        level = jnp.transpose(level, (2, 3, 1, 0, 4)).reshape(2, planes, portion // 2, 2, columns * owners // 4, 2)
        coarse = 0.25 * jnp.sum(level, axis=(3, 5), keepdims=True)
        blend = (coarse + 0.5 * (level - coarse)).reshape(2, planes, portion, columns * owners // 2)
        rebuilt = jnp.repeat(jnp.repeat(blend, 2, axis=2), 2, axis=3)
    return untiled(u, substrate.shape), untiled(v, substrate.shape), rebuilt


def solution(mesh):
    in_specs = (P(None, "gy", "gx"), P(None, "gy", "gx"))
    out_specs = (P(None, "gy", "gx"), P(None, "gy", "gx"), P(None, None, ("gx", "gy"), None))
    return jax.shard_map(body, mesh=mesh, in_specs=in_specs, out_specs=out_specs, check_vma=False)
```
